128 devices in a mesh: dp: 1, ey: 16 (over z, y), ex: 8 (over x, core).
Axes of the slice: x: 4, y: 4, z: 4, core: 2. Of those that a mesh axis runs over, the one named last changes fastest.
Arguments:
- x: bfloat16 [32768, 2048], P(('dp', 'ey', 'ex'))
- ids: int32 [32768, 8], P(('dp', 'ey', 'ex'))
- gates: float32 [32768, 8], P(('dp', 'ey', 'ex'))
- w1: bfloat16 [128, 2048, 768], P(('ey', 'ex'))
- w3: bfloat16 [128, 2048, 768], P(('ey', 'ex'))
- w2: bfloat16 [128, 768, 2048], P(('ey', 'ex'))
Outputs:
- output: bfloat16 [32768, 2048], P(('dp', 'ey', 'ex'))
All inputs are finite; a program needn't handle non-finite values.
Results may differ from the reference program's by a relative error of at most 0.001.
Values are sent between devices in bfloat16 or wider.
A program may use at most 1 GiB of HBM per device.

```python
import jax
import jax.numpy as jnp
from jax import lax

H = 2048
F = 768
E = 128
TOP = 8
NG = 1
TG = 1
T = 256
P = 128

EL = E // P
N = P * T
GN = max(NG, 8)
GT = TG + (GN // 2 - TG) * (1 // NG)
EG = E // GN
CAP = min(T, 2 * T * TOP // P)


def setup_inputs(seed: int = 0, part: int = 0) -> dict:
    kw1, kw3, kw2 = jax.random.split(jax.random.key(seed), 3)
    kb1, kb2 = jax.random.split(jax.random.fold_in(jax.random.key(seed), 7), 2)
    kpart = jax.random.fold_in(jax.random.key(seed + 1), part)
    kx, _, _, ka = jax.random.split(kpart, 4)
    kg, ke = jax.random.split(jax.random.fold_in(kpart, 7), 2)
    x = jax.random.normal(kx, (N, H), jnp.float32)
    group_bias = jax.random.randint(kb1, (GN,), 0, 2 ** 21, jnp.int32)
    bias_draw = jax.random.randint(kb2, (E,), 0, 2 ** 10, jnp.int32)
    expert_bias = (3 * bias_draw * bias_draw) >> 1
    group_draw = jax.random.randint(kg, (N, GN), 0, 2 ** 20, jnp.int32)
    group_score = (group_draw + group_bias[None, :]) * GN + jnp.arange(GN, dtype=jnp.int32)[None, :]
    gtop = lax.top_k(group_score, GT)[1]
    gmask = jnp.any(gtop[:, :, None] == jnp.arange(GN)[None, None, :], axis=1)
    emask = jnp.repeat(gmask, EG, axis=1).astype(jnp.int32)
    expert_draw = jax.random.randint(ke, (N, E), 0, 2 ** 20, jnp.int32)
    expert_score = (expert_draw + expert_bias[None, :] + (4 << 20) * emask) * E + jnp.arange(E, dtype=jnp.int32)[None, :]
    ids = lax.top_k(expert_score, TOP)[1].astype(jnp.int32)
    a = jax.random.uniform(ka, (N, TOP), jnp.float32, 0.5, 1.5)
    gates = 2.5 * a / jnp.sum(a, axis=1, keepdims=True)
    w1 = jax.random.normal(kw1, (E, H, F), jnp.float32) * H ** -0.5
    w3 = jax.random.normal(kw3, (E, H, F), jnp.float32) * H ** -0.5
    w2 = jax.random.normal(kw2, (E, F, H), jnp.float32) * F ** -0.5
    return {"x": x.astype(jnp.bfloat16), "ids": ids, "gates": gates,
            "w1": w1.astype(jnp.bfloat16), "w3": w3.astype(jnp.bfloat16),
            "w2": w2.astype(jnp.bfloat16)}


def keep_mask(ids):
    dev = ids // EL
    hit = jnp.any(dev[:, :, None] == jnp.arange(P)[None, None, :], axis=1)
    hit3 = hit.reshape(P, T, P)
    rank = jnp.cumsum(hit3.astype(jnp.int32), axis=1) - 1
    kept = (hit3 & (rank < CAP)).reshape(N, P)
    return jnp.take_along_axis(kept, dev, axis=1)


def reference(x, ids, gates, w1, w3, w2):
    wk = gates * keep_mask(ids).astype(jnp.float32)

    def body(acc, e):
        c = jnp.sum(jnp.where(ids == e, wk, 0.0), axis=1)
        a1 = jnp.dot(x, w1[e], preferred_element_type=jnp.float32)
        a3 = jnp.dot(x, w3[e], preferred_element_type=jnp.float32)
        h = (jax.nn.silu(a1) * a3).astype(jnp.bfloat16)
        o = jnp.dot(h, w2[e], preferred_element_type=jnp.float32).astype(jnp.bfloat16)
        return acc + c[:, None] * o.astype(jnp.float32), None

    acc, _ = lax.scan(body, jnp.zeros((N, H), jnp.float32), jnp.arange(E))
    return (x.astype(jnp.float32) + acc).astype(jnp.bfloat16)
```

```python
import jax
import jax.numpy as jnp
from jax import lax
from jax.sharding import PartitionSpec as P

CAPF = 2
FULL = 16384.0


def solution(mesh):
    nx = mesh.shape["ex"]
    nd = mesh.shape["ey"] * nx
    axes = ("ey", "ex")
    tok = P(("dp", "ey", "ex"), None)
    wsp = P(("ey", "ex"), None, None)
    bf16, f16, f32 = jnp.bfloat16, jnp.float16, jnp.float32

    def top8(v):
        return lax.reduce_precision(jnp.minimum(v, float(jnp.finfo(bf16).max)), 8, 7)

    def split3(v):
        a = top8(v)
        b = top8(v - a)
        c = top8(v - a - b)
        return a.astype(bf16), b.astype(bf16), c.astype(bf16)

    def local(x, ids, gates, w1, w3, w2):
        t, hd = x.shape
        top = ids.shape[1]
        cap = min(t, CAPF * t * top // nd)
        match = ids[:, :, None] == jnp.arange(nd)[None, None, :]
        hit = jnp.any(match, axis=1)
        gate = jnp.sum(jnp.where(match, gates[:, :, None], 0.0), axis=1)
        lower = (jnp.arange(t)[:, None] >= jnp.arange(t)[None, :]).astype(bf16)
        rank = jnp.dot(lower, hit.astype(bf16), preferred_element_type=f32).astype(jnp.int32) - 1
        slot = jnp.where(hit & (rank < cap), rank, cap)

        sel = slot.T[:, None, :] == jnp.arange(cap)[None, :, None]
        send = jnp.dot(sel.astype(bf16).reshape(nd * cap, t), x,
                       preferred_element_type=f32).astype(bf16)
        rx = lax.all_to_all(send.reshape(nd, cap, hd), axes, 0, 0, tiled=True).reshape(nd * cap, hd)

        a1 = jnp.dot(rx, w1[0], preferred_element_type=f32)
        a3 = jnp.dot(rx, w3[0], preferred_element_type=f32)
        hh = (jax.nn.silu(a1) * a3).astype(bf16)
        o = jnp.dot(hh, w2[0], preferred_element_type=f32)
        peak = jnp.maximum(jnp.max(jnp.abs(o), axis=1), 1e-34)
        o = (o * (FULL / peak)[:, None]).astype(f16)
        back = lax.all_to_all(o.reshape(nd, cap, hd), axes, 0, 0, tiled=True).reshape(nd * cap, hd)
        peak = lax.all_to_all(peak.reshape(nd, cap), axes, 0, 0, tiled=True).reshape(1, nd * cap)

        grow = (jnp.arange(nd)[:, None] == (jnp.arange(nd * cap) // cap)[None, :]).astype(bf16)
        wide = lambda v: jnp.dot(v, grow, preferred_element_type=f32)
        mine = wide(slot.astype(bf16)) == (jnp.arange(nd * cap) % cap).astype(f32)[None, :]
        g = sum(wide(part) for part in split3(gate))
        wt = jnp.concatenate(split3(jnp.where(mine, g * (peak * (1.0 / FULL)), 0.0)), axis=0)
        wt = lax.optimization_barrier(wt)
        back = back.astype(f32)
        hi = top8(back)
        hi, lo = hi.astype(bf16), (back - hi).astype(bf16)
        acc = jnp.dot(wt, hi, preferred_element_type=f32) + jnp.dot(wt, lo, preferred_element_type=f32)
        moe = acc[:t] + acc[t:2 * t] + acc[2 * t:]
        return (x.astype(f32) + moe).astype(bf16)

    return jax.shard_map(local, mesh=mesh, in_specs=(tok, tok, tok, wsp, wsp, wsp),
                         out_specs=tok, check_vma=False)
```

```python
import functools

import jax
import jax.numpy as jnp
from jax import lax
from jax.experimental import pallas as pl
from jax.experimental.pallas import tpu as pltpu
from jax.sharding import PartitionSpec as P

CAPF = 2
FULL = 16384.0
RING = 4
CORES = 2
PARTS = 2
IDROWS = 8
ORDERS = ((0, 1, 2), (2, 0, 1), (1, 2, 0))
bf16, f16, f32 = jnp.bfloat16, jnp.float16, jnp.float32


def column_groups(hd):
    tiles = hd // 128
    first = -(-tiles // 3)
    second = -(-(tiles - first) // 2)
    widths = [first * 128, second * 128, (tiles - first - second) * 128]
    starts = [0, widths[0], widths[0] + widths[1]]
    return list(zip(starts, widths))


def dispatch_kernel(t, cap, groups, x_ref, rx_ref, got, out, upper, pick, load_sem, gsend, grecv, rsend, rrecv, self_sem):
    ey, ex, dp = lax.axis_index("ey"), lax.axis_index("ex"), lax.axis_index("dp")
    me = [ey // RING, ey % RING, ex // CORES]
    core = ex % CORES
    half = cap // PARTS
    rows = t + IDROWS
    split = (rows // 2 + 7) // 8 * 8

    def device(coords, c):
        return (dp, coords[0] * RING + coords[1], coords[2] * CORES + c)

    def shifted(axis, by, c=None):
        coords = list(me)
        coords[axis] = (coords[axis] + by) % RING
        return device(coords, core if c is None else c)

    loads = []
    for g, (start, width) in enumerate(groups):
        loads.append(pltpu.make_async_copy(
            x_ref.at[:, pl.ds(start, width)], got.at[g, 0, 0, :, pl.ds(0, width)], load_sem.at[g]))
        loads[-1].start()

    barrier = pltpu.get_barrier_semaphore()
    peers = [(axis, by, dc) for axis in range(3) for by in range(1, RING) for dc in range(CORES)] + [(0, 0, 1)]
    for axis, by, dc in peers:
        pl.semaphore_signal(barrier, inc=1, device_id=shifted(axis, by, (core + dc) % CORES),
                            device_id_type=pl.DeviceIdType.MESH)
    row = lax.broadcasted_iota(jnp.int32, (t, t), 0)
    col = lax.broadcasted_iota(jnp.int32, (t, t), 1)
    upper[...] = jnp.where(row <= col, 1.0, 0.0).astype(bf16)
    pl.semaphore_wait(barrier, len(peers))
    for load in loads:
        load.wait()

    def hop(g, index, block, to, axis, by, part=None):
        width = groups[g][1]
        at = pl.ds(0, rows) if part is None else part
        copy = pltpu.make_async_remote_copy(
            src_ref=got.at[g, block[0], block[1], at, pl.ds(0, width)],
            dst_ref=got.at[g, to[0], to[1], at, pl.ds(0, width)],
            send_sem=gsend.at[g, index], recv_sem=grecv.at[g, index],
            device_id=shifted(axis, by), device_id_type=pl.DeviceIdType.MESH)
        copy.start()
        hops[g, index] = copy

    hops = {}
    low, high = pl.ds(0, split), pl.ds(split, rows - split)

    def first(g):
        p = ORDERS[g][0]
        hop(g, 0, (0, 0), (3, 0), p, 1)
        hop(g, 1, (0, 0), (1, 0), p, 3)

    def second(g, i):
        q = ORDERS[g][1]
        hop(g, 4 + 4 * i, (i, 0), (i, 3), q, 1)
        hop(g, 5 + 4 * i, (i, 0), (i, 1), q, 3)

    def second_on(g, i):
        q = ORDERS[g][1]
        hops[g, 4 + 4 * i].wait_recv()
        hop(g, 6 + 4 * i, (i, 3), (i, 2), q, 1, low)
        hops[g, 5 + 4 * i].wait_recv()
        hop(g, 7 + 4 * i, (i, 1), (i, 2), q, 3, high)

    everyone = range(len(groups))
    for g in everyone:
        first(g)
        second(g, 0)
    for g in everyone:
        p = ORDERS[g][0]
        hops[g, 0].wait_recv()
        hop(g, 2, (3, 0), (2, 0), p, 1, low)
        second(g, 3)
        hops[g, 1].wait_recv()
        hop(g, 3, (1, 0), (2, 0), p, 3, high)
        second(g, 1)
    for g in everyone:
        second_on(g, 0)
    for g in everyone:
        hops[g, 2].wait_recv()
        hops[g, 3].wait_recv()
        second(g, 2)

    def choose(g, j):
        p, _, r = ORDERS[g]
        width = groups[g][1]
        stride = (RING * RING * CORES, RING * CORES, CORES)[r]
        base = ey * (RING * CORES) + ex - core - me[r] * stride

        def one(i, _):
            ids = got[g, i, j, pl.ds(t, IDROWS), pl.ds(0, t)].astype(f32)
            lines = []
            for k in range(RING * CORES):
                expert = (base + (k // CORES) * stride + k % CORES).astype(f32)
                lines.append(jnp.sum(jnp.where(ids == expert, 1.0, 0.0), axis=0, keepdims=True))
            hit = jnp.concatenate(lines, axis=0)
            rank = jnp.dot(hit.astype(bf16), upper[...], preferred_element_type=f32)
            slot = jnp.where((hit > 0.5) & (rank < cap + 0.5), rank - 1.0, -1.0)
            wanted = lax.broadcasted_iota(jnp.int32, (cap, t), 0).astype(f32)
            for k in range(RING * CORES):
                pick[pl.ds(k * cap, cap), :] = jnp.where(slot[k:k + 1, :] == wanted, 1.0, 0.0).astype(bf16)
            place = (me[p] + i) % RING

            def tile(n, _):
                at = pl.ds(pl.multiple_of(n * 128, 128), 128)
                val = jnp.dot(pick[...], got[g, i, j, pl.ds(0, t), at], preferred_element_type=f32).astype(bf16)
                for k in range(RING * CORES):
                    for h in range(PARTS):
                        begin = k * cap + h * half
                        out[g, j, k, h, place, :, at] = val[begin:begin + half]
                return 0

            return lax.fori_loop(0, width // 128, tile, 0)

        lax.fori_loop(0, RING, one, 0)

    def place_in(ref, g, j):
        start, width = groups[g]
        p, q, r = ORDERS[g]
        at = [None, None, None]
        at[p] = slice(None)
        at[q] = (me[q] + j) % RING
        at[r] = me[r]
        return ref.at[:, at[0], at[1], at[2], core, :, pl.ds(start, width)]

    sends, keeps = [], []

    def exchange(g, j):
        _, _, r = ORDERS[g]
        width = groups[g][1]
        for dr in range(RING):
            for dc in range(CORES):
                to, c = (me[r] + dr) % RING, (core + dc) % CORES
                src = out.at[g, j, to * CORES + c, :, :, :, pl.ds(0, width)]
                if dr == 0 and dc == 0:
                    copy = pltpu.make_async_copy(src, place_in(rx_ref, g, j), self_sem.at[g, j])
                    keeps.append(copy)
                else:
                    n = dr * CORES + dc
                    copy = pltpu.make_async_remote_copy(
                        src_ref=src, dst_ref=place_in(rx_ref, g, j),
                        send_sem=rsend.at[g, j, n], recv_sem=rrecv.at[g, j, n],
                        device_id=shifted(r, dr, c), device_id_type=pl.DeviceIdType.MESH)
                    sends.append(copy)
                copy.start()

    for g in everyone:
        choose(g, 0)
        exchange(g, 0)
    for i in (3, 1):
        for g in everyone:
            second_on(g, i)
    for g in everyone:
        second_on(g, 2)
    for j in (3, 1):
        for g in everyone:
            choose(g, j)
            exchange(g, j)
    for g in everyone:
        for i in range(RING):
            hops[g, 6 + 4 * i].wait_recv()
            hops[g, 7 + 4 * i].wait_recv()
        choose(g, 2)
        exchange(g, 2)

    for copy in sends:
        copy.wait_recv()
    for copy in keeps:
        copy.wait()
    for copy in hops.values():
        copy.wait_send()
    for copy in sends:
        copy.wait_send()


def dispatch(x, ids, cap):
    t, hd = x.shape
    groups = column_groups(hd)
    wide = max(w for _, w in groups)
    tail = jnp.full((IDROWS, hd), -1.0, bf16)
    for start, _ in groups:
        tail = lax.dynamic_update_slice(tail, ids.T.astype(bf16), (0, start))
    block = jnp.concatenate([x, tail], axis=0)
    n = len(groups)
    peers = RING * CORES
    return pl.pallas_call(
        functools.partial(dispatch_kernel, t, cap, groups),
        out_shape=jax.ShapeDtypeStruct((PARTS, RING, RING, RING, CORES, cap // PARTS, hd), bf16),
        in_specs=[pl.BlockSpec(memory_space=pl.ANY)],
        out_specs=pl.BlockSpec(memory_space=pl.ANY),
        scratch_shapes=[
            pltpu.VMEM((n, RING, RING, t + IDROWS, wide), bf16),
            pltpu.VMEM((n, RING, peers, PARTS, RING, cap // PARTS, wide), bf16),
            pltpu.VMEM((t, t), bf16),
            pltpu.VMEM((peers * cap, t), bf16),
            pltpu.SemaphoreType.DMA((n,)),
            pltpu.SemaphoreType.DMA((n, 4 + 4 * RING)),
            pltpu.SemaphoreType.DMA((n, 4 + 4 * RING)),
            pltpu.SemaphoreType.DMA((n, RING, peers)),
            pltpu.SemaphoreType.DMA((n, RING, peers)),
            pltpu.SemaphoreType.DMA((n, RING)),
        ],
        compiler_params=pltpu.CompilerParams(collective_id=0, has_side_effects=True, vmem_limit_bytes=60 * 2 ** 20),
        name="dispatch",
    )(block)


def solution(mesh):
    nx = mesh.shape["ex"]
    nd = mesh.shape["ey"] * nx
    axes = ("ey", "ex")
    tok = P(("dp", "ey", "ex"), None)
    wsp = P(("ey", "ex"), None, None)

    def top8(v):
        return lax.reduce_precision(jnp.minimum(v, float(jnp.finfo(bf16).max)), 8, 7)

    def split3(v):
        a = top8(v)
        b = top8(v - a)
        c = top8(v - a - b)
        return a.astype(bf16), b.astype(bf16), c.astype(bf16)

    def local(x, ids, gates, w1, w3, w2):
        t, hd = x.shape
        top = ids.shape[1]
        cap = min(t, CAPF * t * top // nd)
        half = cap // PARTS
        rx = dispatch(x, ids, cap)

        match = ids[:, :, None] == jnp.arange(nd)[None, None, :]
        hit = jnp.any(match, axis=1)
        gate = jnp.sum(jnp.where(match, gates[:, :, None], 0.0), axis=1)
        lower = (jnp.arange(t)[:, None] >= jnp.arange(t)[None, :]).astype(bf16)
        rank = jnp.dot(lower, hit.astype(bf16), preferred_element_type=f32).astype(jnp.int32) - 1
        slot = jnp.where(hit & (rank < cap), rank, cap)
        grow = (jnp.arange(nd)[:, None] == (jnp.arange(nd * half) // half)[None, :]).astype(bf16)
        wide = lambda v: jnp.dot(v, grow, preferred_element_type=f32)
        slots = wide(slot.astype(bf16))
        g = sum(wide(part) for part in split3(gate))

        moe = x.astype(f32)
        for h in range(PARTS):
            r = rx[h].reshape(nd * half, hd)
            a1 = jnp.dot(r, w1[0], preferred_element_type=f32)
            a3 = jnp.dot(r, w3[0], preferred_element_type=f32)
            hh = (jax.nn.silu(a1) * a3).astype(bf16)
            o = jnp.dot(hh, w2[0], preferred_element_type=f32)
            peak = jnp.maximum(jnp.max(jnp.abs(o), axis=1), 1e-34)
            o = (o * (FULL / peak)[:, None]).astype(f16)
            back = lax.all_to_all(o.reshape(nd, half, hd), axes, 0, 0, tiled=True).reshape(nd * half, hd)
            peak = lax.all_to_all(peak.reshape(nd, half), axes, 0, 0, tiled=True).reshape(1, nd * half)
            mine = slots == (jnp.arange(nd * half) % half + h * half).astype(f32)[None, :]
            wt = jnp.concatenate(split3(jnp.where(mine, g * (peak * (1.0 / FULL)), 0.0)), axis=0)
            wt = lax.optimization_barrier(wt)
            back = back.astype(f32)
            hi = top8(back)
            hi, lo = hi.astype(bf16), (back - hi).astype(bf16)
            acc = jnp.dot(wt, hi, preferred_element_type=f32) + jnp.dot(wt, lo, preferred_element_type=f32)
            moe = moe + (acc[:t] + acc[t:2 * t] + acc[2 * t:])
        return moe.astype(bf16)

    return jax.shard_map(local, mesh=mesh, in_specs=(tok, tok, tok, wsp, wsp, wsp),
                         out_specs=tok, check_vma=False)
```

```python
import functools

import jax
import jax.numpy as jnp
from jax import lax
from jax.experimental import pallas as pl
from jax.experimental.pallas import tpu as pltpu
from jax.sharding import PartitionSpec as P

CAPF = 2
FULL = 32000.0
RING = 4
CORES = 2
IDROWS = 8
ORDERS = ((0, 1, 2), (2, 0, 1), (1, 2, 0))
LINE = RING * CORES
STRIDES = (RING * RING * CORES, RING * CORES, CORES)
RETURNS = ((2, 1, 0), (1, 0, 2), (0, 2, 1))
TILE = 256
SLOTS = 4
MESH = pl.DeviceIdType.MESH
bf16, i16, f32 = jnp.bfloat16, jnp.int16, jnp.float32


def column_groups(hd, tile):
    tiles = hd // tile
    first = -(-tiles // 3)
    second = -(-(tiles - first) // 2)
    widths = [first * tile, second * tile, (tiles - first - second) * tile]
    starts = [0, widths[0], widths[0] + widths[1]]
    return list(zip(starts, widths))


def dispatch_kernel(t, cap, groups, x_ref, rx_ref, got, out, upper, pick, load_sem, gsend, grecv, rsend, rrecv, self_sem):
    ey, ex, dp = lax.axis_index("ey"), lax.axis_index("ex"), lax.axis_index("dp")
    me = [ey // RING, ey % RING, ex // CORES]
    core = ex % CORES
    rows = t + IDROWS
    split = (rows // 2 + 7) // 8 * 8

    def device(coords, c):
        return (dp, coords[0] * RING + coords[1], coords[2] * CORES + c)

    def shifted(axis, by, c=None):
        coords = list(me)
        coords[axis] = (coords[axis] + by) % RING
        return device(coords, core if c is None else c)

    loads = []
    for g, (start, width) in enumerate(groups):
        loads.append(pltpu.make_async_copy(
            x_ref.at[:, pl.ds(start, width)], got.at[g, 0, 0, :, pl.ds(0, width)], load_sem.at[g]))
        loads[-1].start()

    barrier = pltpu.get_barrier_semaphore()
    peers = [(axis, by, dc) for axis in range(3) for by in range(1, RING) for dc in range(CORES)] + [(0, 0, 1)]
    for axis, by, dc in peers:
        pl.semaphore_signal(barrier, inc=1, device_id=shifted(axis, by, (core + dc) % CORES),
                            device_id_type=MESH)
    row = lax.broadcasted_iota(jnp.int32, (t, t), 0)
    col = lax.broadcasted_iota(jnp.int32, (t, t), 1)
    upper[...] = jnp.where(row <= col, 1.0, 0.0).astype(bf16)
    pl.semaphore_wait(barrier, len(peers))
    for load in loads:
        load.wait()

    def hop(g, index, block, to, axis, by, part=None):
        width = groups[g][1]
        at = pl.ds(0, rows) if part is None else part
        copy = pltpu.make_async_remote_copy(
            src_ref=got.at[g, block[0], block[1], at, pl.ds(0, width)],
            dst_ref=got.at[g, to[0], to[1], at, pl.ds(0, width)],
            send_sem=gsend.at[g, index], recv_sem=grecv.at[g, index],
            device_id=shifted(axis, by), device_id_type=MESH)
        copy.start()
        hops[g, index] = copy

    hops = {}
    low, high = pl.ds(0, split), pl.ds(split, rows - split)

    def first(g):
        p = ORDERS[g][0]
        hop(g, 0, (0, 0), (3, 0), p, 1)
        hop(g, 1, (0, 0), (1, 0), p, 3)

    def second(g, i):
        q = ORDERS[g][1]
        hop(g, 4 + 4 * i, (i, 0), (i, 3), q, 1)
        hop(g, 5 + 4 * i, (i, 0), (i, 1), q, 3)

    def second_on(g, i):
        q = ORDERS[g][1]
        hops[g, 4 + 4 * i].wait_recv()
        hop(g, 6 + 4 * i, (i, 3), (i, 2), q, 1, low)
        hops[g, 5 + 4 * i].wait_recv()
        hop(g, 7 + 4 * i, (i, 1), (i, 2), q, 3, high)

    everyone = range(len(groups))
    for g in everyone:
        first(g)
        second(g, 0)
    for g in everyone:
        p = ORDERS[g][0]
        hops[g, 0].wait_recv()
        hop(g, 2, (3, 0), (2, 0), p, 1, low)
        second(g, 3)
        hops[g, 1].wait_recv()
        hop(g, 3, (1, 0), (2, 0), p, 3, high)
        second(g, 1)
    for g in everyone:
        second_on(g, 0)
    for g in everyone:
        hops[g, 2].wait_recv()
        hops[g, 3].wait_recv()
        second(g, 2)

    def choose(g, j):
        p, _, r = ORDERS[g]
        width = groups[g][1]
        stride = (RING * RING * CORES, RING * CORES, CORES)[r]
        base = ey * (RING * CORES) + ex - core - me[r] * stride

        def one(i, _):
            ids = got[g, i, j, pl.ds(t, IDROWS), pl.ds(0, t)].astype(f32)
            lines = []
            for k in range(RING * CORES):
                expert = (base + (k // CORES) * stride + k % CORES).astype(f32)
                lines.append(jnp.sum(jnp.where(ids == expert, 1.0, 0.0), axis=0, keepdims=True))
            hit = jnp.concatenate(lines, axis=0)
            rank = jnp.dot(hit.astype(bf16), upper[...], preferred_element_type=f32)
            slot = jnp.where((hit > 0.5) & (rank < cap + 0.5), rank - 1.0, -1.0)
            wanted = lax.broadcasted_iota(jnp.int32, (cap, t), 0).astype(f32)
            for k in range(RING * CORES):
                pick[pl.ds(k * cap, cap), :] = jnp.where(slot[k:k + 1, :] == wanted, 1.0, 0.0).astype(bf16)
            place = (me[p] + i) % RING

            def tile(n, _):
                at = pl.ds(pl.multiple_of(n * 128, 128), 128)
                val = jnp.dot(pick[...], got[g, i, j, pl.ds(0, t), at], preferred_element_type=f32).astype(bf16)
                for k in range(RING * CORES):
                    out[g, j, k, place, :, at] = val[k * cap:(k + 1) * cap]
                return 0

            return lax.fori_loop(0, width // 128, tile, 0)

        lax.fori_loop(0, RING, one, 0)

    def place_in(ref, g, j):
        start, width = groups[g]
        p, q, r = ORDERS[g]
        at = [None, None, None]
        at[p] = slice(None)
        at[q] = (me[q] + j) % RING
        at[r] = me[r]
        return ref.at[at[0], at[1], at[2], core, :, pl.ds(start, width)]

    sends, keeps = [], []

    def exchange(g, j):
        _, _, r = ORDERS[g]
        width = groups[g][1]
        for dr in range(RING):
            for dc in range(CORES):
                to, c = (me[r] + dr) % RING, (core + dc) % CORES
                src = out.at[g, j, to * CORES + c, :, :, pl.ds(0, width)]
                if dr == 0 and dc == 0:
                    copy = pltpu.make_async_copy(src, place_in(rx_ref, g, j), self_sem.at[g, j])
                    keeps.append(copy)
                else:
                    n = dr * CORES + dc
                    copy = pltpu.make_async_remote_copy(
                        src_ref=src, dst_ref=place_in(rx_ref, g, j),
                        send_sem=rsend.at[g, j, n], recv_sem=rrecv.at[g, j, n],
                        device_id=shifted(r, dr, c), device_id_type=MESH)
                    sends.append(copy)
                copy.start()

    for g in everyone:
        choose(g, 0)
        exchange(g, 0)
    for i in (3, 1):
        for g in everyone:
            second_on(g, i)
    for g in everyone:
        second_on(g, 2)
    for j in (3, 1):
        for g in everyone:
            choose(g, j)
            exchange(g, j)
    for g in everyone:
        for i in range(RING):
            hops[g, 6 + 4 * i].wait_recv()
            hops[g, 7 + 4 * i].wait_recv()
        choose(g, 2)
        exchange(g, 2)

    for copy in sends:
        copy.wait_recv()
    for copy in keeps:
        copy.wait()
    for copy in hops.values():
        copy.wait_send()
    for copy in sends:
        copy.wait_send()


def dispatch(x, ids, cap):
    t, hd = x.shape
    groups = column_groups(hd, 128)
    wide = max(w for _, w in groups)
    tail = jnp.full((IDROWS, hd), -1.0, bf16)
    for start, _ in groups:
        tail = lax.dynamic_update_slice(tail, ids.T.astype(bf16), (0, start))
    block = jnp.concatenate([x, tail], axis=0)
    n = len(groups)
    peers = RING * CORES
    return pl.pallas_call(
        functools.partial(dispatch_kernel, t, cap, groups),
        out_shape=jax.ShapeDtypeStruct((RING, RING, RING, CORES, cap, hd), bf16),
        in_specs=[pl.BlockSpec(memory_space=pl.ANY)],
        out_specs=pl.BlockSpec(memory_space=pl.ANY),
        scratch_shapes=[
            pltpu.VMEM((n, RING, RING, t + IDROWS, wide), bf16),
            pltpu.VMEM((n, RING, peers, RING, cap, wide), bf16),
            pltpu.VMEM((t, t), bf16),
            pltpu.VMEM((peers * cap, t), bf16),
            pltpu.SemaphoreType.DMA((n,)),
            pltpu.SemaphoreType.DMA((n, 4 + 4 * RING)),
            pltpu.SemaphoreType.DMA((n, 4 + 4 * RING)),
            pltpu.SemaphoreType.DMA((n, RING, peers)),
            pltpu.SemaphoreType.DMA((n, RING, peers)),
            pltpu.SemaphoreType.DMA((n, RING)),
        ],
        compiler_params=pltpu.CompilerParams(collective_id=0, has_side_effects=True, vmem_limit_bytes=60 * 2 ** 20),
        name="dispatch",
    )(block)


def experts_kernel(t, cap, groups, info_ref, x_ref, rx_ref, w1_ref, w3_ref, w2_ref, y_ref, r2,
                   w1, w3, w2, xb, hh, res, ob, so, r1, s1, s2, acc, planes, info, db, wt, upper,
                   wsem, xsem, isend, irecv, p1s, p1r, q1s, q1r, p2s, p2r, q2s, q2r, p3s, p3r, dsem):
    ey, ex, dp = lax.axis_index("ey"), lax.axis_index("ex"), lax.axis_index("dp")
    me = [ey // RING, ey % RING, ex // CORES]
    core = ex % CORES
    rows = LINE * cap
    hd, ff = w1.shape
    everyone = range(len(groups))
    col0 = [start for start, _ in groups]
    width = [w for _, w in groups]
    own = [me[RETURNS[g][0]] * CORES + core for g in everyone]

    def shifted(axis, by, c=None):
        coords = list(me)
        coords[axis] = (coords[axis] + by) % RING
        return (dp, coords[0] * RING + coords[1], coords[2] * CORES + (core if c is None else c))

    def remote(src, dst, send, recv, to):
        return pltpu.make_async_remote_copy(src_ref=src, dst_ref=dst, send_sem=send, recv_sem=recv,
                                            device_id=to, device_id_type=MESH)

    loads = [pltpu.make_async_copy(a, b, wsem.at[n])
             for n, (a, b) in enumerate(((w1_ref, w1), (w3_ref, w3), (w2_ref, w2)))]
    for load in loads:
        load.start()

    def homes(step):
        return (step + step // RING) % RING, step % RING

    def tile_load(step):
        dz, dy = homes(step)
        return pltpu.make_async_copy(rx_ref.at[(me[0] + dz) % RING, (me[1] + dy) % RING], xb.at[step % 2], xsem.at[step % 2])

    tile_load(0).start()

    barrier = pltpu.get_barrier_semaphore()
    peers = [(axis, by, dc) for axis in range(3) for by in range(1, RING) for dc in range(CORES)] + [(0, 0, 1)]
    for axis, by, dc in peers:
        pl.semaphore_signal(barrier, inc=1, device_id=shifted(axis, by, (core + dc) % CORES), device_id_type=MESH)
    row = lax.broadcasted_iota(jnp.int32, (t, t), 0)
    col = lax.broadcasted_iota(jnp.int32, (t, t), 1)
    upper[...] = jnp.where(row <= col, 1.0, 0.0).astype(bf16)
    for axis in range(3):
        info[axis, me[axis]] = info_ref[...]
    pl.semaphore_wait(barrier, len(peers))

    told = []
    for axis in range(3):
        for by in range(1, RING):
            told.append(remote(info_ref, info.at[axis, me[axis]], isend.at[axis, by], irecv.at[axis, by], shifted(axis, by)))
            told[-1].start()

    for load in loads:
        load.wait()

    def first(step):
        dz, dy = homes(step)
        zh, yh = (me[0] + dz) % RING, (me[1] + dy) % RING
        slot = step % SLOTS
        found = []
        for n in range(1, LINE):
            d, dc = n // CORES, n % CORES
            c = (core + dc) % CORES
            found.append((None, remote(
                ob.at[slot, (me[2] + d) % RING, c, :, pl.ds(col0[0], width[0])],
                r1.at[0, own[0], zh, yh, :, pl.ds(0, width[0])],
                p1s.at[slot, n], p1r.at[0, n], shifted(2, d, c))))
        for g, axis, d, lead in ((1, 1, dy, zh), (2, 0, dz, yh)):
            for dc in range(CORES):
                c = (core + dc) % CORES
                found.append((None if dc else d != 0, remote(
                    ob.at[slot, :, c, :, pl.ds(col0[g], width[g])],
                    r1.at[g, own[g], lead, :, :, pl.ds(0, width[g])],
                    p1s.at[slot, LINE + 2 * (g - 1) + dc], p1r.at[g, d * CORES + dc], shifted(axis, d, c))))
        return found

    def each(found, act):
        for whether, copy in found:
            if whether is None:
                act(copy)
            else:
                @pl.when(whether)
                def _():
                    act(copy)

    eye = lax.broadcasted_iota(jnp.int32, (cap, 128), 0) == lax.broadcasted_iota(jnp.int32, (cap, 128), 1)

    def tile(step, _):
        dz, dy = homes(step)
        zh, yh = (me[0] + dz) % RING, (me[1] + dy) % RING
        slot = step % SLOTS

        @pl.when(step + 1 < RING * RING)
        def _():
            tile_load(step + 1).start()

        tile_load(step).wait()

        def up(n, _):
            at = pl.ds(pl.multiple_of(n * TILE, TILE), TILE)
            xt = xb[step % 2].reshape(rows, hd)
            a1 = jnp.dot(xt, w1[:, at], preferred_element_type=f32)
            a3 = jnp.dot(xt, w3[:, at], preferred_element_type=f32)
            hh[:, at] = (a1 * (1.0 / (1.0 + jnp.exp(-a1))) * a3).astype(bf16)
            return 0

        lax.fori_loop(0, ff // TILE, up, 0)

        def down(n, peak):
            at = pl.ds(pl.multiple_of(n * TILE, TILE), TILE)
            o = jnp.dot(hh[...], w2[:, at], preferred_element_type=f32)
            res[:, at] = o
            return jnp.maximum(peak, jnp.max(jnp.abs(o), axis=1, keepdims=True))

        peak = lax.fori_loop(0, hd // TILE, down, jnp.full((rows, 1), 1e-30, f32))
        for k in range(LINE):
            part = jnp.where(eye, peak[k * cap:(k + 1) * cap], 0.0)
            so[zh, yh, k // CORES, k % CORES] = jnp.sum(part, axis=0, keepdims=True) * (1.0 / FULL)

        @pl.when(step >= SLOTS)
        def _():
            each(first(step - SLOTS), lambda copy: copy.wait_send())

        factor = FULL / peak

        def code(n, _):
            at = pl.ds(pl.multiple_of(n * TILE, TILE), TILE)
            v = jnp.round(res[:, at] * factor).astype(jnp.int32).astype(i16)
            ob[slot, :, :, :, at] = v.reshape(RING, CORES, cap, TILE)
            return 0

        lax.fori_loop(0, hd // TILE, code, 0)
        each(first(step), lambda copy: copy.start())

        r1[0, own[0], zh, yh, :, pl.ds(0, width[0])] = ob[slot, me[2], core, :, pl.ds(col0[0], width[0])]
        for g, d, lead in ((1, dy, zh), (2, dz, yh)):
            @pl.when(d == 0)
            def _():
                for xh in range(RING):
                    r1[g, own[g], lead, xh, :, pl.ds(0, width[g])] = ob[slot, xh, core, :, pl.ds(col0[g], width[g])]
        return 0

    lax.fori_loop(0, RING * RING, tile, 0)

    def scales(g, coord, c):
        return (so.at[:, :, coord, c], so.at[:, coord, :, c], so.at[coord, :, :, c])[g]

    hints = []
    for g in everyone:
        axis = RETURNS[g][0]
        s1[g, own[g]] = (so[:, :, me[2], core], so[:, me[1], :, core], so[me[0], :, :, core])[g]
        for n in range(1, LINE):
            d, dc = n // CORES, n % CORES
            c = (core + dc) % CORES
            hints.append(remote(scales(g, (me[axis] + d) % RING, c), s1.at[g, own[g]],
                                q1s.at[g, n], q1r.at[g, n], shifted(axis, d, c)))
            hints[-1].start()

    for g in everyone:
        axis = RETURNS[g][0]
        for n in range(1, LINE):
            d, dc = n // CORES, n % CORES
            src = (me[axis] - d) % RING * CORES + (core + dc) % CORES
            ref = r1.at[g, src, :, :, :, pl.ds(0, width[g])]
            pltpu.make_async_copy(ref, ref, p1r.at[g, n]).wait()
    for copy in hints:
        copy.wait_recv()

    def lane(ref, g, h2, h3):
        return (ref.at[0, :, h3, h2], ref.at[1, :, h2, h3], ref.at[2, :, h3, h2])[g]

    moved = []
    for g in everyone:
        axis = RETURNS[g][1]
        s2[g, me[axis]] = (s1[0, :, :, me[1]], s1[1, :, me[0]], s1[2, :, :, me[2]])[g]
        for d in (1, 3, 2):
            moved.append(remote(lane(s1, g, (me[axis] + d) % RING, slice(None)), s2.at[g, me[axis]],
                                q2s.at[g, d], q2r.at[g, d], shifted(axis, d)))
            moved[-1].start()

    def second(g, k3, d):
        _, axis, third = RETURNS[g]
        h3 = (me[third] + k3) % RING
        src = (r1.at[0, :, h3, (me[axis] + d) % RING, :, pl.ds(0, width[0])] if g == 0 else
               r1.at[1, :, (me[axis] + d) % RING, h3, :, pl.ds(0, width[1])] if g == 1 else
               r1.at[2, :, h3, (me[axis] + d) % RING, :, pl.ds(0, width[2])])
        return remote(src, r2.at[g, h3, me[axis], :, :, pl.ds(0, width[g])],
                      p2s.at[g, k3, d], p2r.at[g, k3, d], shifted(axis, d))

    for k3 in (1, 2, 3, 0):
        for d in (1, 3, 2):
            for g in everyone:
                second(g, k3, d).start()

    for copy in told:
        copy.wait_recv()
    for copy in moved:
        copy.wait_recv()

    wanted = lax.broadcasted_iota(jnp.int32, (cap, t), 0).astype(f32)

    def weights(g, h3, src):
        first_axis, axis, third = RETURNS[g]
        ids = info[third, h3, 0:8, :]
        gates = info[third, h3, 8:16, :]
        base = src * STRIDES[axis] + me[third] * STRIDES[third]
        hits, gate = [], []
        for k in range(LINE):
            same = ids == (base + (k // CORES) * STRIDES[first_axis] + k % CORES).astype(f32)
            hits.append(jnp.sum(jnp.where(same, 1.0, 0.0), axis=0, keepdims=True))
            gate.append(jnp.sum(jnp.where(same, gates, 0.0), axis=0, keepdims=True))
        hit = jnp.concatenate(hits, axis=0)
        rank = jnp.dot(hit.astype(bf16), upper[...], preferred_element_type=f32)
        slot = jnp.where((hit > 0.5) & (rank < cap + 0.5), rank - 1.0, -1.0)
        for k in range(LINE):
            scale = jnp.sum(jnp.where(eye, s2[g, src, k, h3], 0.0), axis=1, keepdims=True)
            w = jnp.where(slot[k:k + 1, :] == wanted, gate[k], 0.0) * scale
            a = w.astype(bf16)
            w = w - a.astype(f32)
            b = w.astype(bf16)
            w = w - b.astype(f32)
            at = pl.ds(k * cap, cap)
            wt[at, pl.ds(0, t)] = a
            wt[at, pl.ds(t, t)] = b
            wt[at, pl.ds(2 * t, t)] = w.astype(bf16)

    def line(index, _):
        k3 = (index + 1) % RING

        def plane(turn, _):
            d = turn + turn // 2 - 2 * (turn // 3)

            def fetch(g):
                third = RETURNS[g][2]
                src = (me[RETURNS[g][1]] - d) % RING
                return pltpu.make_async_copy(r2.at[g, (me[third] + k3) % RING, src, :, :, pl.ds(0, width[g])],
                                             db.at[g, :, :, pl.ds(0, width[g])], dsem.at[g])

            for g in everyone:
                _, axis, third = RETURNS[g]
                h3 = (me[third] + k3) % RING

                @pl.when(turn == 0)
                def _():
                    at = pl.ds(0, width[g])
                    if g == 1:
                        db[g, :, :, at] = r1[g, :, me[axis], h3, :, at]
                    else:
                        db[g, :, :, at] = r1[g, :, h3, me[axis], :, at]
                    acc[g, index] = jnp.zeros(acc.shape[2:], f32)

                @pl.when(turn > 0)
                def _():
                    second(g, k3, d).wait_recv()
                    fetch(g).start()

            for g in everyone:
                _, axis, third = RETURNS[g]
                weights(g, (me[third] + k3) % RING, (me[axis] - d) % RING)

                @pl.when(turn > 0)
                def _():
                    fetch(g).wait()

                def piece(n, _):
                    at = pl.ds(pl.multiple_of(n * TILE, TILE), TILE)
                    q = db[g, :, :, at].reshape(rows, TILE).astype(f32)
                    high = q.astype(bf16)
                    low = (q - high.astype(f32)).astype(bf16)
                    dims = (((0,), (0,)), ((), ()))
                    p = (lax.dot_general(wt[...], high, dims, preferred_element_type=f32)
                         + lax.dot_general(wt[...], low, dims, preferred_element_type=f32))
                    acc[g, index, :, at] += p[0:t] + p[t:2 * t] + p[2 * t:]
                    return 0

                lax.fori_loop(0, width[g] // TILE, piece, 0)
            return 0

        lax.fori_loop(0, RING, plane, 0)

        @pl.when(index < RING - 1)
        def _():
            for g in everyone:
                home(g, index).start()
        return 0

    def home(g, index):
        at = pl.ds(0, width[g])
        return remote(acc.at[g, index, :, at], planes.at[g, index, :, at],
                      p3s.at[g, index], p3r.at[g, index], shifted(RETURNS[g][2], (index + 1) % RING))

    lax.fori_loop(0, RING, line, 0)

    for g in everyone:
        for index in range(RING - 1):
            home(g, index).wait_recv()
        for n in range(width[g] // TILE):
            at = pl.ds(n * TILE, TILE)
            to = pl.ds(col0[g] + n * TILE, TILE)
            total = acc[g, RING - 1, :, at] + planes[g, 0, :, at] + planes[g, 1, :, at] + planes[g, 2, :, at]
            y_ref[:, to] = (x_ref[:, to].astype(f32) + total).astype(bf16)

    for copy in told + hints + moved:
        copy.wait_send()

    def last(step, _):
        each(first(step), lambda copy: copy.wait_send())
        return 0

    lax.fori_loop(RING * RING - SLOTS, RING * RING, last, 0)
    for g in everyone:
        for k3 in range(RING):
            for d in (1, 3, 2):
                second(g, k3, d).wait_send()
        for index in range(RING - 1):
            home(g, index).wait_send()


def experts(x, ids, gates, rx, w1, w3, w2):
    t, hd = x.shape
    ff = w1.shape[1]
    cap = rx.shape[4]
    groups = column_groups(hd, TILE)
    wide = max(w for _, w in groups)
    n = len(groups)
    info = jnp.concatenate([ids.T.astype(f32), gates.T], axis=0)
    dma = pltpu.SemaphoreType.DMA
    anywhere = pl.BlockSpec(memory_space=pl.ANY)
    vmem = pl.BlockSpec(memory_space=pltpu.VMEM)
    y, _ = pl.pallas_call(
        functools.partial(experts_kernel, t, cap, groups),
        out_shape=(jax.ShapeDtypeStruct((t, hd), bf16),
                   jax.ShapeDtypeStruct((n, RING, RING, LINE, cap, wide), i16)),
        in_specs=[vmem, vmem] + [anywhere] * 4,
        out_specs=(vmem, anywhere),
        scratch_shapes=[
            pltpu.VMEM((hd, ff), bf16), pltpu.VMEM((hd, ff), bf16), pltpu.VMEM((ff, hd), bf16),
            pltpu.VMEM((2, RING, CORES, cap, hd), bf16),
            pltpu.VMEM((LINE * cap, ff), bf16),
            pltpu.VMEM((LINE * cap, hd), f32),
            pltpu.VMEM((SLOTS, RING, CORES, cap, hd), i16),
            pltpu.VMEM((RING, RING, RING, CORES, 1, 128), f32),
            pltpu.VMEM((n, LINE, RING, RING, cap, wide), i16),
            pltpu.VMEM((n, LINE, RING, RING, 1, 128), f32),
            pltpu.VMEM((n, RING, LINE, RING, 1, 128), f32),
            pltpu.VMEM((n, RING, t, wide), f32),
            pltpu.VMEM((n, RING - 1, t, wide), f32),
            pltpu.VMEM((3, RING, 16, t), f32),
            pltpu.VMEM((n, LINE, cap, wide), i16),
            pltpu.VMEM((LINE * cap, 3 * t), bf16),
            pltpu.VMEM((t, t), bf16),
            dma((3,)), dma((2,)), dma((3, RING)), dma((3, RING)),
            dma((SLOTS, LINE + 4)), dma((n, LINE)), dma((n, LINE)), dma((n, LINE)),
            dma((n, RING, RING)), dma((n, RING, RING)), dma((n, RING)), dma((n, RING)),
            dma((n, RING)), dma((n, RING)), dma((n,)),
        ],
        compiler_params=pltpu.CompilerParams(collective_id=1, has_side_effects=True, vmem_limit_bytes=67043328),
        name="experts",
    )(info, x, rx, w1, w3, w2)
    return y


def solution(mesh):
    nd = mesh.shape["ey"] * mesh.shape["ex"]
    tok = P(("dp", "ey", "ex"), None)
    wsp = P(("ey", "ex"), None, None)

    def local(x, ids, gates, w1, w3, w2):
        t = x.shape[0]
        cap = min(t, CAPF * t * ids.shape[1] // nd)
        rx = dispatch(x, ids, cap)
        return experts(x, ids, gates, rx, w1[0], w3[0], w2[0])

    return jax.shard_map(local, mesh=mesh, in_specs=(tok, tok, tok, wsp, wsp, wsp),
                         out_specs=tok, check_vma=False)
```

```python
import functools

import jax
import jax.numpy as jnp
from jax import lax
from jax.experimental import pallas as pl
from jax.experimental.pallas import tpu as pltpu
from jax.sharding import PartitionSpec as P

CAPF = 2
FULL = 32000.0
RING = 4
CORES = 2
IDROWS = 8
ORDERS = ((0, 1, 2), (2, 0, 1), (1, 2, 0))
LINE = RING * CORES
STRIDES = (RING * RING * CORES, RING * CORES, CORES)
RETURNS = ((2, 1, 0), (1, 0, 2), (0, 2, 1))
TILE = 256
WIDE = 512
SLOTS = 5
MESH = pl.DeviceIdType.MESH
bf16, i16, f32 = jnp.bfloat16, jnp.int16, jnp.float32


def column_groups(hd, tile):
    tiles = hd // tile
    first = -(-tiles // 3)
    second = -(-(tiles - first) // 2)
    widths = [first * tile, second * tile, (tiles - first - second) * tile]
    starts = [0, widths[0], widths[0] + widths[1]]
    return list(zip(starts, widths))


def dispatch_kernel(t, cap, groups, x_ref, ids_ref, rx_ref, got, out, upper, pick, load_sem, gsend, grecv, rsend, rrecv, self_sem):
    ey, ex, dp = lax.axis_index("ey"), lax.axis_index("ex"), lax.axis_index("dp")
    me = [ey // RING, ey % RING, ex // CORES]
    core = ex % CORES
    rows = t + IDROWS
    split = (rows // 2 + 7) // 8 * 8

    def device(coords, c):
        return (dp, coords[0] * RING + coords[1], coords[2] * CORES + c)

    def shifted(axis, by, c=None):
        coords = list(me)
        coords[axis] = (coords[axis] + by) % RING
        return device(coords, core if c is None else c)

    loads = []
    for g, (start, width) in enumerate(groups):
        loads.append(pltpu.make_async_copy(
            x_ref.at[:, pl.ds(start, width)], got.at[g, 0, 0, pl.ds(0, t), pl.ds(0, width)], load_sem.at[g, 0]))
        loads.append(pltpu.make_async_copy(
            ids_ref, got.at[g, 0, 0, pl.ds(t, IDROWS), pl.ds(0, t)], load_sem.at[g, 1]))
    for load in loads:
        load.start()

    barrier = pltpu.get_barrier_semaphore()
    peers = [(axis, by, dc) for axis in range(3) for by in range(1, RING) for dc in range(CORES)] + [(0, 0, 1)]
    for axis, by, dc in peers:
        pl.semaphore_signal(barrier, inc=1, device_id=shifted(axis, by, (core + dc) % CORES),
                            device_id_type=MESH)
    row = lax.broadcasted_iota(jnp.int32, (t, t), 0)
    col = lax.broadcasted_iota(jnp.int32, (t, t), 1)
    upper[...] = jnp.where(row <= col, 1.0, 0.0).astype(bf16)
    pl.semaphore_wait(barrier, len(peers))
    for load in loads:
        load.wait()

    def hop(g, index, block, to, axis, by, part=None):
        width = groups[g][1]
        at = pl.ds(0, rows) if part is None else part
        copy = pltpu.make_async_remote_copy(
            src_ref=got.at[g, block[0], block[1], at, pl.ds(0, width)],
            dst_ref=got.at[g, to[0], to[1], at, pl.ds(0, width)],
            send_sem=gsend.at[g, index], recv_sem=grecv.at[g, index],
            device_id=shifted(axis, by), device_id_type=MESH)
        copy.start()
        hops[g, index] = copy

    hops = {}
    low, high = pl.ds(0, split), pl.ds(split, rows - split)

    def first(g):
        p = ORDERS[g][0]
        hop(g, 0, (0, 0), (3, 0), p, 1)
        hop(g, 1, (0, 0), (1, 0), p, 3)

    def second(g, i):
        q = ORDERS[g][1]
        hop(g, 4 + 4 * i, (i, 0), (i, 3), q, 1)
        hop(g, 5 + 4 * i, (i, 0), (i, 1), q, 3)

    def second_on(g, i):
        q = ORDERS[g][1]
        hops[g, 4 + 4 * i].wait_recv()
        hop(g, 6 + 4 * i, (i, 3), (i, 2), q, 1, low)
        hops[g, 5 + 4 * i].wait_recv()
        hop(g, 7 + 4 * i, (i, 1), (i, 2), q, 3, high)

    everyone = range(len(groups))
    for g in everyone:
        first(g)
        second(g, 0)
    for g in everyone:
        p = ORDERS[g][0]
        hops[g, 0].wait_recv()
        hop(g, 2, (3, 0), (2, 0), p, 1, low)
        second(g, 3)
        hops[g, 1].wait_recv()
        hop(g, 3, (1, 0), (2, 0), p, 3, high)
        second(g, 1)
    for g in everyone:
        second_on(g, 0)
    for g in everyone:
        hops[g, 2].wait_recv()
        hops[g, 3].wait_recv()
        second(g, 2)

    def choose(g, j):
        p, _, r = ORDERS[g]
        width = groups[g][1]
        stride = (RING * RING * CORES, RING * CORES, CORES)[r]
        base = ey * (RING * CORES) + ex - core - me[r] * stride

        def one(i, _):
            ids = got[g, i, j, pl.ds(t, IDROWS), pl.ds(0, t)].astype(f32)
            lines = []
            for k in range(RING * CORES):
                expert = (base + (k // CORES) * stride + k % CORES).astype(f32)
                lines.append(jnp.sum(jnp.where(ids == expert, 1.0, 0.0), axis=0, keepdims=True))
            hit = jnp.concatenate(lines, axis=0)
            rank = jnp.dot(hit.astype(bf16), upper[...], preferred_element_type=f32)
            slot = jnp.where((hit > 0.5) & (rank < cap + 0.5), rank - 1.0, -1.0)
            wanted = lax.broadcasted_iota(jnp.int32, (cap, t), 0).astype(f32)
            for k in range(RING * CORES):
                pick[pl.ds(k * cap, cap), :] = jnp.where(slot[k:k + 1, :] == wanted, 1.0, 0.0).astype(bf16)
            place = (me[p] + i) % RING

            def tile(n, _):
                at = pl.ds(pl.multiple_of(n * 128, 128), 128)
                val = jnp.dot(pick[...], got[g, i, j, pl.ds(0, t), at], preferred_element_type=f32).astype(bf16)
                for k in range(RING * CORES):
                    out[g, j, k, place, :, at] = val[k * cap:(k + 1) * cap]
                return 0

            return lax.fori_loop(0, width // 128, tile, 0)

        lax.fori_loop(0, RING, one, 0)

    def place_in(ref, g, j):
        start, width = groups[g]
        p, q, r = ORDERS[g]
        at = [None, None, None]
        at[p] = slice(None)
        at[q] = (me[q] + j) % RING
        at[r] = me[r]
        return ref.at[at[0], at[1], at[2], core, :, pl.ds(start, width)]

    sends, keeps = [], []

    def exchange(g, j):
        _, _, r = ORDERS[g]
        width = groups[g][1]
        for dr in range(RING):
            for dc in range(CORES):
                to, c = (me[r] + dr) % RING, (core + dc) % CORES
                src = out.at[g, j, to * CORES + c, :, :, pl.ds(0, width)]
                if dr == 0 and dc == 0:
                    copy = pltpu.make_async_copy(src, place_in(rx_ref, g, j), self_sem.at[g, j])
                    keeps.append(copy)
                else:
                    n = dr * CORES + dc
                    copy = pltpu.make_async_remote_copy(
                        src_ref=src, dst_ref=place_in(rx_ref, g, j),
                        send_sem=rsend.at[g, j, n], recv_sem=rrecv.at[g, j, n],
                        device_id=shifted(r, dr, c), device_id_type=MESH)
                    sends.append(copy)
                copy.start()

    for g in everyone:
        choose(g, 0)
        exchange(g, 0)
    for i in (3, 1):
        for g in everyone:
            second_on(g, i)
    for g in everyone:
        second_on(g, 2)
    for j in (3, 1):
        for g in everyone:
            choose(g, j)
            exchange(g, j)
    for g in everyone:
        for i in range(RING):
            hops[g, 6 + 4 * i].wait_recv()
            hops[g, 7 + 4 * i].wait_recv()
        choose(g, 2)
        exchange(g, 2)

    for copy in sends:
        copy.wait_recv()
    for copy in keeps:
        copy.wait()
    for copy in hops.values():
        copy.wait_send()
    for copy in sends:
        copy.wait_send()


def dispatch(x, ids, cap):
    t, hd = x.shape
    groups = column_groups(hd, 128)
    wide = max(w for _, w in groups)
    n = len(groups)
    peers = RING * CORES
    return pl.pallas_call(
        functools.partial(dispatch_kernel, t, cap, groups),
        out_shape=jax.ShapeDtypeStruct((RING, RING, RING, CORES, cap, hd), bf16),
        in_specs=[pl.BlockSpec(memory_space=pl.ANY)] * 2,
        out_specs=pl.BlockSpec(memory_space=pl.ANY),
        scratch_shapes=[
            pltpu.VMEM((n, RING, RING, t + IDROWS, wide), bf16),
            pltpu.VMEM((n, RING, peers, RING, cap, wide), bf16),
            pltpu.VMEM((t, t), bf16),
            pltpu.VMEM((peers * cap, t), bf16),
            pltpu.SemaphoreType.DMA((n, 2)),
            pltpu.SemaphoreType.DMA((n, 4 + 4 * RING)),
            pltpu.SemaphoreType.DMA((n, 4 + 4 * RING)),
            pltpu.SemaphoreType.DMA((n, RING, peers)),
            pltpu.SemaphoreType.DMA((n, RING, peers)),
            pltpu.SemaphoreType.DMA((n, RING)),
        ],
        compiler_params=pltpu.CompilerParams(collective_id=0, has_side_effects=True, vmem_limit_bytes=60 * 2 ** 20),
        name="dispatch",
    )(x, ids.T.astype(bf16))


def experts_kernel(t, cap, groups, info_ref, x_ref, rx_ref, w1_ref, w3_ref, w2_ref, y_ref, r2,
                   w1, w3, w2, xb, hh, res, top, ob, rest, so, r1, s1, s2, acc, planes, info, db, wt, upper, xv,
                   wsem, xsem, isend, irecv, p1s, p1r, q1s, q1r, p2s, p2r, q2s, q2r, p3s, p3r, e1s, e1r, e2s, e2r, dsem):
    ey, ex, dp = lax.axis_index("ey"), lax.axis_index("ex"), lax.axis_index("dp")
    me = [ey // RING, ey % RING, ex // CORES]
    core = ex % CORES
    rows = LINE * cap
    hd, ff = w1.shape
    everyone = range(len(groups))
    col0 = [start for start, _ in groups]
    width = [w for _, w in groups]
    main = min(width)
    more = width[0] - main
    own = [me[RETURNS[g][0]] * CORES + core for g in everyone]

    def shifted(axis, by, c=None):
        coords = list(me)
        coords[axis] = (coords[axis] + by) % RING
        return (dp, coords[0] * RING + coords[1], coords[2] * CORES + (core if c is None else c))

    def remote(src, dst, send, recv, to):
        return pltpu.make_async_remote_copy(src_ref=src, dst_ref=dst, send_sem=send, recv_sem=recv,
                                            device_id=to, device_id_type=MESH)

    loads = [pltpu.make_async_copy(a, b, wsem.at[n])
             for n, (a, b) in enumerate(((w1_ref, w1), (w3_ref, w3), (w2_ref, w2), (x_ref, xv)))]
    mine = [pltpu.make_async_copy(info_ref, info.at[axis, me[axis]], isend.at[axis, 0]) for axis in range(3)]
    for load in mine + loads:
        load.start()

    def homes(step):
        left = RING * RING - 1 - step
        return (left + left // RING) % RING, left % RING

    def tile_load(step):
        dz, dy = homes(step)
        return pltpu.make_async_copy(rx_ref.at[(me[0] + dz) % RING, (me[1] + dy) % RING], xb.at[step % 2], xsem.at[step % 2])

    tile_load(0).start()

    barrier = pltpu.get_barrier_semaphore()
    peers = [(axis, by, dc) for axis in range(3) for by in range(1, RING) for dc in range(CORES)] + [(0, 0, 1)]
    for axis, by, dc in peers:
        pl.semaphore_signal(barrier, inc=1, device_id=shifted(axis, by, (core + dc) % CORES), device_id_type=MESH)
    row = lax.broadcasted_iota(jnp.int32, (t, t), 0)
    col = lax.broadcasted_iota(jnp.int32, (t, t), 1)
    upper[...] = jnp.where(row <= col, 1.0, 0.0).astype(bf16)
    pl.semaphore_wait(barrier, len(peers))

    told = []
    for axis in range(3):
        for by in range(1, RING):
            told.append(remote(info_ref, info.at[axis, me[axis]], isend.at[axis, by], irecv.at[axis, by], shifted(axis, by)))
            told[-1].start()

    for load in mine + loads[:3]:
        load.wait()

    def first(step):
        dz, dy = homes(step)
        zh, yh = (me[0] + dz) % RING, (me[1] + dy) % RING
        slot = step % SLOTS
        found = []
        for n in range(1, LINE):
            d, dc = n // CORES, n % CORES
            c = (core + dc) % CORES
            found.append((None, remote(
                ob.at[slot, (me[2] + d) % RING, c, :, pl.ds(col0[0], main)],
                r1.at[0, own[0], zh, yh, :, pl.ds(0, main)],
                p1s.at[slot, n], p1r.at[0, n], shifted(2, d, c))))
        for g, axis, d, lead in ((1, 1, dy, zh), (2, 0, dz, yh)):
            for dc in range(CORES):
                c = (core + dc) % CORES
                found.append((None if dc else d != 0, remote(
                    ob.at[slot, :, c, :, pl.ds(col0[g], width[g])],
                    r1.at[g, own[g], lead, :, :, pl.ds(0, width[g])],
                    p1s.at[slot, LINE + 2 * (g - 1) + dc], p1r.at[g, d * CORES + dc], shifted(axis, d, c))))
        return found

    def each(found, act):
        for whether, copy in found:
            if whether is None:
                act(copy)
            else:
                @pl.when(whether)
                def _():
                    act(copy)

    eye = lax.broadcasted_iota(jnp.int32, (cap, 128), 0) == lax.broadcasted_iota(jnp.int32, (cap, 128), 1)

    def tile(step, _):
        dz, dy = homes(step)
        zh, yh = (me[0] + dz) % RING, (me[1] + dy) % RING
        slot = step % SLOTS

        @pl.when(step + 1 < RING * RING)
        def _():
            tile_load(step + 1).start()

        tile_load(step).wait()

        top[...] = jnp.zeros(top.shape, f32)

        def up(n, _):
            at = pl.ds(pl.multiple_of(n * TILE, TILE), TILE)
            xt = xb[step % 2].reshape(rows, hd)
            a1 = jnp.dot(xt, w1[:, at], preferred_element_type=f32)
            a3 = jnp.dot(xt, w3[:, at], preferred_element_type=f32)
            hh[:, at] = (a1 * (1.0 / (1.0 + jnp.exp(-a1))) * a3).astype(bf16)
            return 0

        lax.fori_loop(0, ff // TILE, up, 0)

        def down(n, _):
            at = pl.ds(pl.multiple_of(n * WIDE, WIDE), WIDE)
            o = jnp.dot(hh[...], w2[:, at], preferred_element_type=f32)
            res[:, at] = o
            o = jnp.abs(o)
            most = o[:, 0:128]
            for k in range(1, WIDE // 128):
                most = jnp.maximum(most, o[:, k * 128:(k + 1) * 128])
            top[...] = jnp.maximum(top[...], most)
            return 0

        lax.fori_loop(0, hd // WIDE, down, 0)
        peak = jnp.maximum(jnp.max(top[...], axis=1, keepdims=True), 1e-30)
        for k in range(LINE):
            part = jnp.where(eye, peak[k * cap:(k + 1) * cap], 0.0)
            so[zh, yh, k // CORES, k % CORES] = jnp.sum(part, axis=0, keepdims=True) * (1.0 / FULL)

        @pl.when(step >= SLOTS)
        def _():
            each(first(step - SLOTS), lambda copy: copy.wait_send())

        top[...] = jnp.broadcast_to(FULL / peak, top.shape)

        def code(n, _):
            at = pl.ds(pl.multiple_of(n * 128, 128), 128)
            v = jnp.round(res[:, at] * top[...]).astype(jnp.int32).astype(i16)
            ob[slot, :, :, :, at] = v.reshape(RING, CORES, cap, 128)
            return 0

        lax.fori_loop(0, hd // 128, code, 0)
        each(first(step), lambda copy: copy.start())

        r1[0, own[0], zh, yh, :, pl.ds(0, width[0])] = ob[slot, me[2], core, :, pl.ds(col0[0], width[0])]
        if more:
            rest[zh, yh] = ob[slot, :, :, :, pl.ds(col0[0] + main, more)]
        for g, d, lead in ((1, dy, zh), (2, dz, yh)):
            @pl.when(d == 0)
            def _():
                for xh in range(RING):
                    r1[g, own[g], lead, xh, :, pl.ds(0, width[g])] = ob[slot, xh, core, :, pl.ds(col0[g], width[g])]
        return 0

    lax.fori_loop(0, RING * RING, tile, 0)

    later = []
    if more:
        for n in range(1, LINE):
            d, dc = n // CORES, n % CORES
            c = (core + dc) % CORES
            later.append(remote(rest.at[:, :, (me[2] + d) % RING, c], r1.at[0, own[0], :, :, :, pl.ds(main, more)],
                                e1s.at[n], e1r.at[n], shifted(2, d, c)))
            later[-1].start()

    def scales(g, coord, c):
        return (so.at[:, :, coord, c], so.at[:, coord, :, c], so.at[coord, :, :, c])[g]

    hints = []
    for g in everyone:
        axis = RETURNS[g][0]
        s1[g, own[g]] = (so[:, :, me[2], core], so[:, me[1], :, core], so[me[0], :, :, core])[g]
        for n in range(1, LINE):
            d, dc = n // CORES, n % CORES
            c = (core + dc) % CORES
            hints.append(remote(scales(g, (me[axis] + d) % RING, c), s1.at[g, own[g]],
                                q1s.at[g, n], q1r.at[g, n], shifted(axis, d, c)))
            hints[-1].start()

    for g in everyone:
        axis = RETURNS[g][0]
        for n in range(1, LINE):
            d, dc = n // CORES, n % CORES
            src = (me[axis] - d) % RING * CORES + (core + dc) % CORES
            ref = r1.at[g, src, :, :, :, pl.ds(0, main)]
            pltpu.make_async_copy(ref, ref, p1r.at[g, n]).wait()
    for copy in hints:
        copy.wait_recv()

    def lane(ref, g, h2, h3):
        return (ref.at[0, :, h3, h2], ref.at[1, :, h2, h3], ref.at[2, :, h3, h2])[g]

    moved = []
    for g in everyone:
        axis = RETURNS[g][1]
        s2[g, me[axis]] = (s1[0, :, :, me[1]], s1[1, :, me[0]], s1[2, :, :, me[2]])[g]
        for d in (1, 3, 2):
            moved.append(remote(lane(s1, g, (me[axis] + d) % RING, slice(None)), s2.at[g, me[axis]],
                                q2s.at[g, d], q2r.at[g, d], shifted(axis, d)))
            moved[-1].start()

    def second(g, k3, d):
        _, axis, third = RETURNS[g]
        h3 = (me[third] + k3) % RING
        at = pl.ds(0, main)
        src = (r1.at[0, :, h3, (me[axis] + d) % RING, :, at] if g == 0 else
               r1.at[1, :, (me[axis] + d) % RING, h3, :, at] if g == 1 else
               r1.at[2, :, h3, (me[axis] + d) % RING, :, at])
        return remote(src, r2.at[g, h3, me[axis], :, :, at], p2s.at[g, k3, d], p2r.at[g, k3, d], shifted(axis, d))

    def second_more(k3, d):
        _, axis, third = RETURNS[0]
        h3 = (me[third] + k3) % RING
        at = pl.ds(main, more)
        return remote(r1.at[0, :, h3, (me[axis] + d) % RING, :, at], r2.at[0, h3, me[axis], :, :, at],
                      e2s.at[k3, d], e2r.at[k3, d], shifted(axis, d))

    for k3 in (1, 2, 3, 0):
        for d in (1, 3, 2):
            for g in everyone:
                second(g, k3, d).start()
        if more and k3 == 1:
            for copy in later:
                copy.wait_recv()
            for each_k3 in (1, 2, 3, 0):
                for d in (1, 3, 2):
                    second_more(each_k3, d).start()

    for copy in told:
        copy.wait_recv()
    for copy in moved:
        copy.wait_recv()

    wanted = lax.broadcasted_iota(jnp.int32, (cap, t), 0).astype(f32)

    def weights(g, h3, src):
        first_axis, axis, third = RETURNS[g]
        ids = info[third, h3, 0:8, :]
        gates = info[third, h3, 8:16, :]
        base = src * STRIDES[axis] + me[third] * STRIDES[third]
        hits, gate = [], []
        for k in range(LINE):
            same = ids == (base + (k // CORES) * STRIDES[first_axis] + k % CORES).astype(f32)
            hits.append(jnp.sum(jnp.where(same, 1.0, 0.0), axis=0, keepdims=True))
            gate.append(jnp.sum(jnp.where(same, gates, 0.0), axis=0, keepdims=True))
        hit = jnp.concatenate(hits, axis=0)
        rank = jnp.dot(hit.astype(bf16), upper[...], preferred_element_type=f32)
        slot = jnp.where((hit > 0.5) & (rank < cap + 0.5), rank - 1.0, -1.0)
        for k in range(LINE):
            scale = jnp.sum(jnp.where(eye, s2[g, src, k, h3], 0.0), axis=1, keepdims=True)
            w = jnp.where(slot[k:k + 1, :] == wanted, gate[k], 0.0) * scale
            a = w.astype(bf16)
            w = w - a.astype(f32)
            b = w.astype(bf16)
            w = w - b.astype(f32)
            at = pl.ds(k * cap, cap)
            wt[at, pl.ds(0, t)] = a
            wt[at, pl.ds(t, t)] = b
            wt[at, pl.ds(2 * t, t)] = w.astype(bf16)

    def line(index, _):
        k3 = (index + 1) % RING

        def plane(turn, _):
            d = turn + turn // 2 - 2 * (turn // 3)

            def fetch(g):
                third = RETURNS[g][2]
                src = (me[RETURNS[g][1]] - d) % RING
                return pltpu.make_async_copy(r2.at[g, (me[third] + k3) % RING, src, :, :, pl.ds(0, width[g])],
                                             db.at[g, :, :, pl.ds(0, width[g])], dsem.at[g])

            for g in everyone:
                _, axis, third = RETURNS[g]
                h3 = (me[third] + k3) % RING

                @pl.when(turn == 0)
                def _():
                    at = pl.ds(0, width[g])
                    if g == 1:
                        db[g, :, :, at] = r1[g, :, me[axis], h3, :, at]
                    else:
                        db[g, :, :, at] = r1[g, :, h3, me[axis], :, at]
                    acc[g, index] = jnp.zeros(acc.shape[2:], f32)

                @pl.when(turn > 0)
                def _():
                    second(g, k3, d).wait_recv()
                    if more and g == 0:
                        second_more(k3, d).wait_recv()
                    fetch(g).start()

            for g in everyone:
                _, axis, third = RETURNS[g]
                weights(g, (me[third] + k3) % RING, (me[axis] - d) % RING)

                @pl.when(turn > 0)
                def _():
                    fetch(g).wait()

                def piece(at, size):
                    q = db[g, :, :, at].reshape(rows, size).astype(f32)
                    high = q.astype(bf16)
                    low = (q - high.astype(f32)).astype(bf16)
                    dims = (((0,), (0,)), ((), ()))
                    p = (lax.dot_general(wt[...], high, dims, preferred_element_type=f32)
                         + lax.dot_general(wt[...], low, dims, preferred_element_type=f32))
                    acc[g, index, :, at] += p[0:t] + p[t:2 * t] + p[2 * t:]

                begin = 0
                while begin < width[g]:
                    size = min(WIDE, width[g] - begin)
                    piece(pl.ds(begin, size), size)
                    begin += size
            return 0

        lax.fori_loop(0, RING, plane, 0)

        @pl.when(index < RING - 1)
        def _():
            for g in everyone:
                home(g, index).start()
        return 0

    def home(g, index):
        at = pl.ds(0, width[g])
        return remote(acc.at[g, index, :, at], planes.at[g, index, :, at],
                      p3s.at[g, index], p3r.at[g, index], shifted(RETURNS[g][2], (index + 1) % RING))

    lax.fori_loop(0, RING, line, 0)

    loads[3].wait()
    for g in everyone:
        for index in range(RING - 1):
            home(g, index).wait_recv()

        def finish(n, _):
            at = pl.ds(pl.multiple_of(n * 128, 128), 128)
            to = pl.ds(pl.multiple_of(col0[g] + n * 128, 128), 128)
            total = acc[g, RING - 1, :, at] + planes[g, 0, :, at] + planes[g, 1, :, at] + planes[g, 2, :, at]
            y_ref[:, to] = (xv[:, to].astype(f32) + total).astype(bf16)
            return 0

        lax.fori_loop(0, width[g] // 128, finish, 0)

    for copy in told + hints + moved + later:
        copy.wait_send()

    def last(step, _):
        each(first(step), lambda copy: copy.wait_send())
        return 0

    lax.fori_loop(RING * RING - SLOTS, RING * RING, last, 0)
    for g in everyone:
        for k3 in range(RING):
            for d in (1, 3, 2):
                second(g, k3, d).wait_send()
                if more and g == 0:
                    second_more(k3, d).wait_send()
        for index in range(RING - 1):
            home(g, index).wait_send()


def experts(x, ids, gates, rx, w1, w3, w2):
    t, hd = x.shape
    ff = w1.shape[1]
    cap = rx.shape[4]
    groups = column_groups(hd, 128)
    wide = max(w for _, w in groups)
    n = len(groups)
    more = max(wide - min(w for _, w in groups), 128)
    info = jnp.concatenate([ids.T.astype(f32), gates.T], axis=0)
    dma = pltpu.SemaphoreType.DMA
    anywhere = pl.BlockSpec(memory_space=pl.ANY)
    vmem = pl.BlockSpec(memory_space=pltpu.VMEM)
    y, _ = pl.pallas_call(
        functools.partial(experts_kernel, t, cap, groups),
        out_shape=(jax.ShapeDtypeStruct((t, hd), bf16),
                   jax.ShapeDtypeStruct((n, RING, RING, LINE, cap, wide), i16)),
        in_specs=[anywhere] * 6,
        out_specs=(vmem, anywhere),
        scratch_shapes=[
            pltpu.VMEM((hd, ff), bf16), pltpu.VMEM((hd, ff), bf16), pltpu.VMEM((ff, hd), bf16),
            pltpu.VMEM((2, RING, CORES, cap, hd), bf16),
            pltpu.VMEM((LINE * cap, ff), bf16),
            pltpu.VMEM((LINE * cap, hd), f32),
            pltpu.VMEM((LINE * cap, 128), f32),
            pltpu.VMEM((SLOTS, RING, CORES, cap, hd), i16),
            pltpu.VMEM((RING, RING, RING, CORES, cap, more), i16),
            pltpu.VMEM((RING, RING, RING, CORES, 1, 128), f32),
            pltpu.VMEM((n, LINE, RING, RING, cap, wide), i16),
            pltpu.VMEM((n, LINE, RING, RING, 1, 128), f32),
            pltpu.VMEM((n, RING, LINE, RING, 1, 128), f32),
            pltpu.VMEM((n, RING, t, wide), f32),
            pltpu.VMEM((n, RING - 1, t, wide), f32),
            pltpu.VMEM((3, RING, 16, t), f32),
            pltpu.VMEM((n, LINE, cap, wide), i16),
            pltpu.VMEM((LINE * cap, 3 * t), bf16),
            pltpu.VMEM((t, t), bf16),
            pltpu.VMEM((t, hd), bf16),
            dma((4,)), dma((2,)), dma((3, RING)), dma((3, RING)),
            dma((SLOTS, LINE + 4)), dma((n, LINE)), dma((n, LINE)), dma((n, LINE)),
            dma((n, RING, RING)), dma((n, RING, RING)), dma((n, RING)), dma((n, RING)),
            dma((n, RING)), dma((n, RING)), dma((LINE,)), dma((LINE,)), dma((RING, RING)), dma((RING, RING)), dma((n,)),
        ],
        compiler_params=pltpu.CompilerParams(collective_id=1, has_side_effects=True, vmem_limit_bytes=67043328),
        name="experts",
    )(info, x, rx, w1, w3, w2)
    return y


def solution(mesh):
    nd = mesh.shape["ey"] * mesh.shape["ex"]
    tok = P(("dp", "ey", "ex"), None)
    wsp = P(("ey", "ex"), None, None)

    def local(x, ids, gates, w1, w3, w2):
        t = x.shape[0]
        cap = min(t, CAPF * t * ids.shape[1] // nd)
        rx = dispatch(x, ids, cap)
        return experts(x, ids, gates, rx, w1[0], w3[0], w2[0])

    return jax.shard_map(local, mesh=mesh, in_specs=(tok, tok, tok, wsp, wsp, wsp),
                         out_specs=tok, check_vma=False)
```

```python
import functools

import jax
import jax.numpy as jnp
from jax import lax
from jax.experimental import pallas as pl
from jax.experimental.pallas import tpu as pltpu
from jax.sharding import PartitionSpec as P

CAPF = 2
FULL = 32000.0
RING = 4
CORES = 2
IDROWS = 8
ORDERS = ((0, 1, 2), (2, 0, 1), (1, 2, 0))
LINE = RING * CORES
STRIDES = (RING * RING * CORES, RING * CORES, CORES)
RETURNS = ((2, 1, 0), (1, 0, 2), (0, 2, 1))
TILE = 256
WIDE = 512
SLOTS = 5
MESH = pl.DeviceIdType.MESH
bf16, i16, f32 = jnp.bfloat16, jnp.int16, jnp.float32


def column_groups(hd, tile):
    tiles = hd // tile
    first = -(-tiles // 3)
    second = -(-(tiles - first) // 2)
    widths = [first * tile, second * tile, (tiles - first - second) * tile]
    starts = [0, widths[0], widths[0] + widths[1]]
    return list(zip(starts, widths))


def dispatch_kernel(t, cap, groups, x_ref, ids_ref, rx_ref, got, out, upper, pick, load_sem, gsend, grecv, rsend, rrecv, self_sem):
    ey, ex, dp = lax.axis_index("ey"), lax.axis_index("ex"), lax.axis_index("dp")
    me = [ey // RING, ey % RING, ex // CORES]
    core = ex % CORES
    rows = t + IDROWS
    split = (rows // 2 + 7) // 8 * 8

    def device(coords, c):
        return (dp, coords[0] * RING + coords[1], coords[2] * CORES + c)

    def shifted(axis, by, c=None):
        coords = list(me)
        coords[axis] = (coords[axis] + by) % RING
        return device(coords, core if c is None else c)

    loads = []
    for g, (start, width) in enumerate(groups):
        loads.append(pltpu.make_async_copy(
            x_ref.at[:, pl.ds(start, width)], got.at[g, 0, 0, pl.ds(0, t), pl.ds(0, width)], load_sem.at[g, 0]))
        loads.append(pltpu.make_async_copy(
            ids_ref, got.at[g, 0, 0, pl.ds(t, IDROWS), pl.ds(0, t)], load_sem.at[g, 1]))
    for load in loads:
        load.start()

    barrier = pltpu.get_barrier_semaphore()
    peers = [(axis, by, dc) for axis in range(3) for by in range(1, RING) for dc in range(CORES)] + [(0, 0, 1)]
    for axis, by, dc in peers:
        pl.semaphore_signal(barrier, inc=1, device_id=shifted(axis, by, (core + dc) % CORES),
                            device_id_type=MESH)
    row = lax.broadcasted_iota(jnp.int32, (t, t), 0)
    col = lax.broadcasted_iota(jnp.int32, (t, t), 1)
    upper[...] = jnp.where(row <= col, 1.0, 0.0).astype(bf16)
    pl.semaphore_wait(barrier, len(peers))
    for load in loads:
        load.wait()

    def hop(g, index, block, to, axis, by, part=None):
        width = groups[g][1]
        at = pl.ds(0, rows) if part is None else part
        copy = pltpu.make_async_remote_copy(
            src_ref=got.at[g, block[0], block[1], at, pl.ds(0, width)],
            dst_ref=got.at[g, to[0], to[1], at, pl.ds(0, width)],
            send_sem=gsend.at[g, index], recv_sem=grecv.at[g, index],
            device_id=shifted(axis, by), device_id_type=MESH)
        copy.start()
        hops[g, index] = copy

    hops = {}
    low, high = pl.ds(0, split), pl.ds(split, rows - split)

    def first(g):
        p = ORDERS[g][0]
        hop(g, 0, (0, 0), (3, 0), p, 1)
        hop(g, 1, (0, 0), (1, 0), p, 3)

    def second(g, i):
        q = ORDERS[g][1]
        hop(g, 4 + 4 * i, (i, 0), (i, 3), q, 1)
        hop(g, 5 + 4 * i, (i, 0), (i, 1), q, 3)

    def second_on(g, i):
        q = ORDERS[g][1]
        hops[g, 4 + 4 * i].wait_recv()
        hop(g, 6 + 4 * i, (i, 3), (i, 2), q, 1, low)
        hops[g, 5 + 4 * i].wait_recv()
        hop(g, 7 + 4 * i, (i, 1), (i, 2), q, 3, high)

    everyone = range(len(groups))
    for g in everyone:
        first(g)
        second(g, 0)
    for g in everyone:
        p = ORDERS[g][0]
        hops[g, 0].wait_recv()
        hop(g, 2, (3, 0), (2, 0), p, 1, low)
        second(g, 3)
        hops[g, 1].wait_recv()
        hop(g, 3, (1, 0), (2, 0), p, 3, high)
        second(g, 1)
    for g in everyone:
        second_on(g, 0)
    for g in everyone:
        hops[g, 2].wait_recv()
        hops[g, 3].wait_recv()
        second(g, 2)

    def choose(g, j):
        p, _, r = ORDERS[g]
        width = groups[g][1]
        stride = (RING * RING * CORES, RING * CORES, CORES)[r]
        base = ey * (RING * CORES) + ex - core - me[r] * stride

        def one(i, _):
            ids = got[g, i, j, pl.ds(t, IDROWS), pl.ds(0, t)].astype(f32)
            lines = []
            for k in range(RING * CORES):
                expert = (base + (k // CORES) * stride + k % CORES).astype(f32)
                lines.append(jnp.sum(jnp.where(ids == expert, 1.0, 0.0), axis=0, keepdims=True))
            hit = jnp.concatenate(lines, axis=0)
            rank = jnp.dot(hit.astype(bf16), upper[...], preferred_element_type=f32)
            slot = jnp.where((hit > 0.5) & (rank < cap + 0.5), rank - 1.0, -1.0)
            wanted = lax.broadcasted_iota(jnp.int32, (cap, t), 0).astype(f32)
            for k in range(RING * CORES):
                pick[pl.ds(k * cap, cap), :] = jnp.where(slot[k:k + 1, :] == wanted, 1.0, 0.0).astype(bf16)
            place = (me[p] + i) % RING

            def tile(n, _):
                at = pl.ds(pl.multiple_of(n * 128, 128), 128)
                val = jnp.dot(pick[...], got[g, i, j, pl.ds(0, t), at], preferred_element_type=f32).astype(bf16)
                for k in range(RING * CORES):
                    out[g, j, k, place, :, at] = val[k * cap:(k + 1) * cap]
                return 0

            return lax.fori_loop(0, width // 128, tile, 0)

        lax.fori_loop(0, RING, one, 0)

    def place_in(ref, g, j):
        start, width = groups[g]
        p, q, r = ORDERS[g]
        at = [None, None, None]
        at[p] = slice(None)
        at[q] = (me[q] + j) % RING
        at[r] = me[r]
        return ref.at[at[0], at[1], at[2], core, :, pl.ds(start, width)]

    sends, keeps = [], []

    def exchange(g, j):
        _, _, r = ORDERS[g]
        width = groups[g][1]
        for dr in range(RING):
            for dc in range(CORES):
                to, c = (me[r] + dr) % RING, (core + dc) % CORES
                src = out.at[g, j, to * CORES + c, :, :, pl.ds(0, width)]
                if dr == 0 and dc == 0:
                    copy = pltpu.make_async_copy(src, place_in(rx_ref, g, j), self_sem.at[g, j])
                    keeps.append(copy)
                else:
                    n = dr * CORES + dc
                    copy = pltpu.make_async_remote_copy(
                        src_ref=src, dst_ref=place_in(rx_ref, g, j),
                        send_sem=rsend.at[g, j, n], recv_sem=rrecv.at[g, j, n],
                        device_id=shifted(r, dr, c), device_id_type=MESH)
                    sends.append(copy)
                copy.start()

    for g in everyone:
        choose(g, 0)
        exchange(g, 0)
    for i in (3, 1):
        for g in everyone:
            second_on(g, i)
    for g in everyone:
        second_on(g, 2)
    for j in (3, 1):
        for g in everyone:
            choose(g, j)
            exchange(g, j)
    for g in everyone:
        for i in range(RING):
            hops[g, 6 + 4 * i].wait_recv()
            hops[g, 7 + 4 * i].wait_recv()
        choose(g, 2)
        exchange(g, 2)

    for copy in sends:
        copy.wait_recv()
    for copy in keeps:
        copy.wait()
    for copy in hops.values():
        copy.wait_send()
    for copy in sends:
        copy.wait_send()


def dispatch(x, ids, cap):
    t, hd = x.shape
    groups = column_groups(hd, 128)
    wide = max(w for _, w in groups)
    n = len(groups)
    peers = RING * CORES
    return pl.pallas_call(
        functools.partial(dispatch_kernel, t, cap, groups),
        out_shape=jax.ShapeDtypeStruct((RING, RING, RING, CORES, cap, hd), bf16),
        in_specs=[pl.BlockSpec(memory_space=pl.ANY)] * 2,
        out_specs=pl.BlockSpec(memory_space=pl.ANY),
        scratch_shapes=[
            pltpu.VMEM((n, RING, RING, t + IDROWS, wide), bf16),
            pltpu.VMEM((n, RING, peers, RING, cap, wide), bf16),
            pltpu.VMEM((t, t), bf16),
            pltpu.VMEM((peers * cap, t), bf16),
            pltpu.SemaphoreType.DMA((n, 2)),
            pltpu.SemaphoreType.DMA((n, 4 + 4 * RING)),
            pltpu.SemaphoreType.DMA((n, 4 + 4 * RING)),
            pltpu.SemaphoreType.DMA((n, RING, peers)),
            pltpu.SemaphoreType.DMA((n, RING, peers)),
            pltpu.SemaphoreType.DMA((n, RING)),
        ],
        compiler_params=pltpu.CompilerParams(collective_id=0, has_side_effects=True, vmem_limit_bytes=60 * 2 ** 20),
        name="dispatch",
    )(x, ids.T.astype(bf16))


def experts_kernel(t, cap, groups, info_ref, x_ref, rx_ref, w1_ref, w3_ref, w2_ref, y_ref, r2,
                   w1, w3, w2, xb, hh, res, top, ob, rest, so, r1, s1, s2, acc, planes, info, db, wt, upper, xv,
                   wsem, xsem, isend, irecv, p1s, p1r, q1s, q1r, p2s, p2r, q2s, q2r, p3s, p3r, e1s, e1r, e2s, e2r, dsem):
    ey, ex, dp = lax.axis_index("ey"), lax.axis_index("ex"), lax.axis_index("dp")
    me = [ey // RING, ey % RING, ex // CORES]
    core = ex % CORES
    rows = LINE * cap
    hd, ff = w1.shape
    everyone = range(len(groups))
    col0 = [start for start, _ in groups]
    width = [w for _, w in groups]
    main = min(width)
    more = width[0] - main
    own = [me[RETURNS[g][0]] * CORES + core for g in everyone]

    def shifted(axis, by, c=None):
        coords = list(me)
        coords[axis] = (coords[axis] + by) % RING
        return (dp, coords[0] * RING + coords[1], coords[2] * CORES + (core if c is None else c))

    def remote(src, dst, send, recv, to):
        return pltpu.make_async_remote_copy(src_ref=src, dst_ref=dst, send_sem=send, recv_sem=recv,
                                            device_id=to, device_id_type=MESH)

    loads = [pltpu.make_async_copy(a, b, wsem.at[n])
             for n, (a, b) in enumerate(((w1_ref, w1), (w3_ref, w3), (w2_ref, w2), (x_ref, xv)))]
    mine = [pltpu.make_async_copy(info_ref, info.at[axis, me[axis]], isend.at[axis, 0]) for axis in range(3)]
    for load in mine + loads:
        load.start()

    def homes(step):
        left = RING * RING - 1 - step
        return (left + left // RING) % RING, left % RING

    def tile_load(step):
        dz, dy = homes(step)
        return pltpu.make_async_copy(rx_ref.at[(me[0] + dz) % RING, (me[1] + dy) % RING], xb.at[step % 2], xsem.at[step % 2])

    tile_load(0).start()

    barrier = pltpu.get_barrier_semaphore()
    peers = [(axis, by, dc) for axis in range(3) for by in range(1, RING) for dc in range(CORES)] + [(0, 0, 1)]
    for axis, by, dc in peers:
        pl.semaphore_signal(barrier, inc=1, device_id=shifted(axis, by, (core + dc) % CORES), device_id_type=MESH)
    row = lax.broadcasted_iota(jnp.int32, (t, t), 0)
    col = lax.broadcasted_iota(jnp.int32, (t, t), 1)
    upper[...] = jnp.where(row <= col, 1.0, 0.0).astype(bf16)
    pl.semaphore_wait(barrier, len(peers))

    told = []
    for axis in range(3):
        for by in range(1, RING):
            told.append(remote(info_ref, info.at[axis, me[axis]], isend.at[axis, by], irecv.at[axis, by], shifted(axis, by)))
            told[-1].start()

    for load in mine + loads[:3]:
        load.wait()

    def first(step):
        dz, dy = homes(step)
        zh, yh = (me[0] + dz) % RING, (me[1] + dy) % RING
        slot = step % SLOTS
        found = []
        for n in range(1, LINE):
            d, dc = n // CORES, n % CORES
            c = (core + dc) % CORES
            found.append((None, remote(
                ob.at[slot, (me[2] + d) % RING, c, :, pl.ds(col0[0], main)],
                r1.at[0, own[0], zh, yh, :, pl.ds(0, main)],
                p1s.at[slot, n], p1r.at[0, n], shifted(2, d, c))))
        for g, axis, d, lead in ((1, 1, dy, zh), (2, 0, dz, yh)):
            for dc in range(CORES):
                c = (core + dc) % CORES
                found.append((None if dc else d != 0, remote(
                    ob.at[slot, :, c, :, pl.ds(col0[g], width[g])],
                    r1.at[g, own[g], lead, :, :, pl.ds(0, width[g])],
                    p1s.at[slot, LINE + 2 * (g - 1) + dc], p1r.at[g, d * CORES + dc], shifted(axis, d, c))))
        return found

    def each(found, act):
        for whether, copy in found:
            if whether is None:
                act(copy)
            else:
                @pl.when(whether)
                def _():
                    act(copy)

    eye = lax.broadcasted_iota(jnp.int32, (cap, 128), 0) == lax.broadcasted_iota(jnp.int32, (cap, 128), 1)

    def tile(step, _):
        dz, dy = homes(step)
        zh, yh = (me[0] + dz) % RING, (me[1] + dy) % RING
        slot = step % SLOTS

        @pl.when(step + 1 < RING * RING)
        def _():
            tile_load(step + 1).start()

        tile_load(step).wait()

        top[...] = jnp.zeros(top.shape, f32)

        def up(n, _):
            at = pl.ds(pl.multiple_of(n * TILE, TILE), TILE)
            xt = xb[step % 2].reshape(rows, hd)
            a1 = jnp.dot(xt, w1[:, at], preferred_element_type=f32)
            a3 = jnp.dot(xt, w3[:, at], preferred_element_type=f32)
            hh[:, at] = (a1 * (1.0 / (1.0 + jnp.exp(-a1))) * a3).astype(bf16)
            return 0

        lax.fori_loop(0, ff // TILE, up, 0)

        def down(n, _):
            at = pl.ds(pl.multiple_of(n * WIDE, WIDE), WIDE)
            o = jnp.dot(hh[...], w2[:, at], preferred_element_type=f32)
            res[:, at] = o
            o = jnp.abs(o)
            most = o[:, 0:128]
            for k in range(1, WIDE // 128):
                most = jnp.maximum(most, o[:, k * 128:(k + 1) * 128])
            top[...] = jnp.maximum(top[...], most)
            return 0

        lax.fori_loop(0, hd // WIDE, down, 0)
        peak = jnp.maximum(jnp.max(top[...], axis=1, keepdims=True), 1e-30)
        for k in range(LINE):
            part = jnp.where(eye, peak[k * cap:(k + 1) * cap], 0.0)
            so[zh, yh, k // CORES, k % CORES] = jnp.sum(part, axis=0, keepdims=True) * (1.0 / FULL)

        @pl.when(step >= SLOTS)
        def _():
            each(first(step - SLOTS), lambda copy: copy.wait_send())

        top[...] = jnp.broadcast_to(FULL / peak, top.shape)

        def code(n, _):
            at = pl.ds(pl.multiple_of(n * 128, 128), 128)
            v = jnp.round(res[:, at] * top[...]).astype(jnp.int32).astype(i16)
            ob[slot, :, :, :, at] = v.reshape(RING, CORES, cap, 128)
            return 0

        lax.fori_loop(0, hd // 128, code, 0)
        each(first(step), lambda copy: copy.start())

        r1[0, own[0], zh, yh, :, pl.ds(0, width[0])] = ob[slot, me[2], core, :, pl.ds(col0[0], width[0])]
        if more:
            rest[zh, yh] = ob[slot, :, :, :, pl.ds(col0[0] + main, more)]
        for g, d, lead in ((1, dy, zh), (2, dz, yh)):
            @pl.when(d == 0)
            def _():
                for xh in range(RING):
                    r1[g, own[g], lead, xh, :, pl.ds(0, width[g])] = ob[slot, xh, core, :, pl.ds(col0[g], width[g])]
        return 0

    lax.fori_loop(0, RING * RING, tile, 0)

    def scales(g, coord, c):
        return (so.at[:, :, coord, c], so.at[:, coord, :, c], so.at[coord, :, :, c])[g]

    hints = []
    for g in everyone:
        axis = RETURNS[g][0]
        s1[g, own[g]] = (so[:, :, me[2], core], so[:, me[1], :, core], so[me[0], :, :, core])[g]
        for n in range(1, LINE):
            d, dc = n // CORES, n % CORES
            c = (core + dc) % CORES
            hints.append(remote(scales(g, (me[axis] + d) % RING, c), s1.at[g, own[g]],
                                q1s.at[g, n], q1r.at[g, n], shifted(axis, d, c)))
            hints[-1].start()

    later = []
    if more:
        for n in range(1, LINE):
            d, dc = n // CORES, n % CORES
            c = (core + dc) % CORES
            later.append(remote(rest.at[:, :, (me[2] + d) % RING, c], r1.at[0, own[0], :, :, :, pl.ds(main, more)],
                                e1s.at[n], e1r.at[n], shifted(2, d, c)))
            later[-1].start()

    def lane(ref, g, h2, h3):
        return (ref.at[0, :, h3, h2], ref.at[1, :, h2, h3], ref.at[2, :, h3, h2])[g]

    def second(g, k3, d):
        _, axis, third = RETURNS[g]
        h3 = (me[third] + k3) % RING
        at = pl.ds(0, main)
        src = (r1.at[0, :, h3, (me[axis] + d) % RING, :, at] if g == 0 else
               r1.at[1, :, (me[axis] + d) % RING, h3, :, at] if g == 1 else
               r1.at[2, :, h3, (me[axis] + d) % RING, :, at])
        return remote(src, r2.at[g, h3, me[axis], :, :, at], p2s.at[g, k3, d], p2r.at[g, k3, d], shifted(axis, d))

    def second_more(k3, d):
        _, axis, third = RETURNS[0]
        h3 = (me[third] + k3) % RING
        at = pl.ds(main, more)
        return remote(r1.at[0, :, h3, (me[axis] + d) % RING, :, at], r2.at[0, h3, me[axis], :, :, at],
                      e2s.at[k3, d], e2r.at[k3, d], shifted(axis, d))

    for g in everyone:
        axis = RETURNS[g][0]
        for n in range(1, LINE):
            d, dc = n // CORES, n % CORES
            src = (me[axis] - d) % RING * CORES + (core + dc) % CORES
            ref = r1.at[g, src, :, :, :, pl.ds(0, main)]
            pltpu.make_async_copy(ref, ref, p1r.at[g, n]).wait()
        for d in (1, 3, 2):
            second(g, 1, d).start()

    for copy in hints:
        copy.wait_recv()
    moved = []
    for g in everyone:
        axis = RETURNS[g][1]
        s2[g, me[axis]] = (s1[0, :, :, me[1]], s1[1, :, me[0]], s1[2, :, :, me[2]])[g]
        for d in (1, 3, 2):
            moved.append(remote(lane(s1, g, (me[axis] + d) % RING, slice(None)), s2.at[g, me[axis]],
                                q2s.at[g, d], q2r.at[g, d], shifted(axis, d)))
            moved[-1].start()

    for copy in later:
        copy.wait_recv()
    for k3 in (1, 2, 3, 0):
        for d in (1, 3, 2):
            if more:
                second_more(k3, d).start()
            for g in everyone:
                if k3 != 1:
                    second(g, k3, d).start()

    for copy in told:
        copy.wait_recv()
    for copy in moved:
        copy.wait_recv()

    wanted = lax.broadcasted_iota(jnp.int32, (cap, t), 0).astype(f32)

    def weights(g, h3, src):
        first_axis, axis, third = RETURNS[g]
        ids = info[third, h3, 0:8, :]
        gates = info[third, h3, 8:16, :]
        base = src * STRIDES[axis] + me[third] * STRIDES[third]
        hits, gate = [], []
        for k in range(LINE):
            same = ids == (base + (k // CORES) * STRIDES[first_axis] + k % CORES).astype(f32)
            hits.append(jnp.sum(jnp.where(same, 1.0, 0.0), axis=0, keepdims=True))
            gate.append(jnp.sum(jnp.where(same, gates, 0.0), axis=0, keepdims=True))
        hit = jnp.concatenate(hits, axis=0)
        rank = jnp.dot(hit.astype(bf16), upper[...], preferred_element_type=f32)
        slot = jnp.where((hit > 0.5) & (rank < cap + 0.5), rank - 1.0, -1.0)
        for k in range(LINE):
            scale = jnp.sum(jnp.where(eye, s2[g, src, k, h3], 0.0), axis=1, keepdims=True)
            w = jnp.where(slot[k:k + 1, :] == wanted, gate[k], 0.0) * scale
            a = w.astype(bf16)
            w = w - a.astype(f32)
            b = w.astype(bf16)
            w = w - b.astype(f32)
            at = pl.ds(k * cap, cap)
            wt[at, pl.ds(0, t)] = a
            wt[at, pl.ds(t, t)] = b
            wt[at, pl.ds(2 * t, t)] = w.astype(bf16)

    def line(index, _):
        k3 = (index + 1) % RING

        def plane(turn, _):
            d = turn + turn // 2 - 2 * (turn // 3)

            def fetch(g):
                third = RETURNS[g][2]
                src = (me[RETURNS[g][1]] - d) % RING
                return pltpu.make_async_copy(r2.at[g, (me[third] + k3) % RING, src, :, :, pl.ds(0, width[g])],
                                             db.at[g, :, :, pl.ds(0, width[g])], dsem.at[g])

            for g in everyone:
                _, axis, third = RETURNS[g]
                h3 = (me[third] + k3) % RING

                @pl.when(turn == 0)
                def _():
                    at = pl.ds(0, width[g])
                    if g == 1:
                        db[g, :, :, at] = r1[g, :, me[axis], h3, :, at]
                    else:
                        db[g, :, :, at] = r1[g, :, h3, me[axis], :, at]
                    acc[g, index] = jnp.zeros(acc.shape[2:], f32)

                @pl.when(turn > 0)
                def _():
                    second(g, k3, d).wait_recv()
                    if more and g == 0:
                        second_more(k3, d).wait_recv()
                    fetch(g).start()

            for g in everyone:
                _, axis, third = RETURNS[g]
                weights(g, (me[third] + k3) % RING, (me[axis] - d) % RING)

                @pl.when(turn > 0)
                def _():
                    fetch(g).wait()

                def piece(at, size):
                    q = db[g, :, :, at].reshape(rows, size).astype(f32)
                    high = q.astype(bf16)
                    low = (q - high.astype(f32)).astype(bf16)
                    dims = (((0,), (0,)), ((), ()))
                    p = (lax.dot_general(wt[...], high, dims, preferred_element_type=f32)
                         + lax.dot_general(wt[...], low, dims, preferred_element_type=f32))
                    acc[g, index, :, at] += p[0:t] + p[t:2 * t] + p[2 * t:]

                begin = 0
                while begin < width[g]:
                    size = min(WIDE, width[g] - begin)
                    piece(pl.ds(begin, size), size)
                    begin += size

                @pl.when((turn == RING - 1) & (index < RING - 1))
                def _():
                    home(g, index).start()
            return 0

        lax.fori_loop(0, RING, plane, 0)

        return 0

    def home(g, index):
        at = pl.ds(0, width[g])
        return remote(acc.at[g, index, :, at], planes.at[g, index, :, at],
                      p3s.at[g, index], p3r.at[g, index], shifted(RETURNS[g][2], (index + 1) % RING))

    lax.fori_loop(0, RING, line, 0)

    loads[3].wait()
    for g in everyone:
        for index in range(RING - 1):
            home(g, index).wait_recv()

        def finish(n, _):
            at = pl.ds(pl.multiple_of(n * 128, 128), 128)
            to = pl.ds(pl.multiple_of(col0[g] + n * 128, 128), 128)
            total = acc[g, RING - 1, :, at] + planes[g, 0, :, at] + planes[g, 1, :, at] + planes[g, 2, :, at]
            y_ref[:, to] = (xv[:, to].astype(f32) + total).astype(bf16)
            return 0

        lax.fori_loop(0, width[g] // 128, finish, 0)

    for copy in told + hints + moved + later:
        copy.wait_send()

    def last(step, _):
        each(first(step), lambda copy: copy.wait_send())
        return 0

    lax.fori_loop(RING * RING - SLOTS, RING * RING, last, 0)
    for g in everyone:
        for k3 in range(RING):
            for d in (1, 3, 2):
                second(g, k3, d).wait_send()
                if more and g == 0:
                    second_more(k3, d).wait_send()
        for index in range(RING - 1):
            home(g, index).wait_send()


def experts(x, ids, gates, rx, w1, w3, w2):
    t, hd = x.shape
    ff = w1.shape[1]
    cap = rx.shape[4]
    groups = column_groups(hd, 128)
    wide = max(w for _, w in groups)
    n = len(groups)
    more = max(wide - min(w for _, w in groups), 128)
    info = jnp.concatenate([ids.T.astype(f32), gates.T], axis=0)
    dma = pltpu.SemaphoreType.DMA
    anywhere = pl.BlockSpec(memory_space=pl.ANY)
    vmem = pl.BlockSpec(memory_space=pltpu.VMEM)
    y, _ = pl.pallas_call(
        functools.partial(experts_kernel, t, cap, groups),
        out_shape=(jax.ShapeDtypeStruct((t, hd), bf16),
                   jax.ShapeDtypeStruct((n, RING, RING, LINE, cap, wide), i16)),
        in_specs=[anywhere] * 6,
        out_specs=(vmem, anywhere),
        scratch_shapes=[
            pltpu.VMEM((hd, ff), bf16), pltpu.VMEM((hd, ff), bf16), pltpu.VMEM((ff, hd), bf16),
            pltpu.VMEM((2, RING, CORES, cap, hd), bf16),
            pltpu.VMEM((LINE * cap, ff), bf16),
            pltpu.VMEM((LINE * cap, hd), f32),
            pltpu.VMEM((LINE * cap, 128), f32),
            pltpu.VMEM((SLOTS, RING, CORES, cap, hd), i16),
            pltpu.VMEM((RING, RING, RING, CORES, cap, more), i16),
            pltpu.VMEM((RING, RING, RING, CORES, 1, 128), f32),
            pltpu.VMEM((n, LINE, RING, RING, cap, wide), i16),
            pltpu.VMEM((n, LINE, RING, RING, 1, 128), f32),
            pltpu.VMEM((n, RING, LINE, RING, 1, 128), f32),
            pltpu.VMEM((n, RING, t, wide), f32),
            pltpu.VMEM((n, RING - 1, t, wide), f32),
            pltpu.VMEM((3, RING, 16, t), f32),
            pltpu.VMEM((n, LINE, cap, wide), i16),
            pltpu.VMEM((LINE * cap, 3 * t), bf16),
            pltpu.VMEM((t, t), bf16),
            pltpu.VMEM((t, hd), bf16),
            dma((4,)), dma((2,)), dma((3, RING)), dma((3, RING)),
            dma((SLOTS, LINE + 4)), dma((n, LINE)), dma((n, LINE)), dma((n, LINE)),
            dma((n, RING, RING)), dma((n, RING, RING)), dma((n, RING)), dma((n, RING)),
            dma((n, RING)), dma((n, RING)), dma((LINE,)), dma((LINE,)), dma((RING, RING)), dma((RING, RING)), dma((n,)),
        ],
        compiler_params=pltpu.CompilerParams(collective_id=1, has_side_effects=True, vmem_limit_bytes=67043328),
        name="experts",
    )(info, x, rx, w1, w3, w2)
    return y


def solution(mesh):
    nd = mesh.shape["ey"] * mesh.shape["ex"]
    tok = P(("dp", "ey", "ex"), None)
    wsp = P(("ey", "ex"), None, None)

    def local(x, ids, gates, w1, w3, w2):
        t = x.shape[0]
        cap = min(t, CAPF * t * ids.shape[1] // nd)
        rx = dispatch(x, ids, cap)
        return experts(x, ids, gates, rx, w1[0], w3[0], w2[0])

    return jax.shard_map(local, mesh=mesh, in_specs=(tok, tok, tok, wsp, wsp, wsp),
                         out_specs=tok, check_vma=False)
```

```python
import functools

import jax
import jax.numpy as jnp
from jax import lax
from jax.experimental import pallas as pl
from jax.experimental.pallas import tpu as pltpu
from jax.sharding import PartitionSpec as P

CAPF = 2
FULL = 32000.0
RING = 4
CORES = 2
IDROWS = 8
ORDERS = ((0, 1, 2), (2, 0, 1), (1, 2, 0))
LINE = RING * CORES
STRIDES = (RING * RING * CORES, RING * CORES, CORES)
RETURNS = ((2, 1, 0), (1, 0, 2), (0, 2, 1))
TILE = 256
LINES = (2, 1, 3, 0)
WIDE = 512
SLOTS = 5
MESH = pl.DeviceIdType.MESH
bf16, i16, f32 = jnp.bfloat16, jnp.int16, jnp.float32


def column_groups(hd, tile):
    tiles = hd // tile
    first = -(-tiles // 3)
    second = -(-(tiles - first) // 2)
    widths = [first * tile, second * tile, (tiles - first - second) * tile]
    starts = [0, widths[0], widths[0] + widths[1]]
    return list(zip(starts, widths))


def dispatch_kernel(t, cap, groups, x_ref, ids_ref, rx_ref, got, out, upper, pick, load_sem, gsend, grecv, rsend, rrecv, self_sem):
    ey, ex, dp = lax.axis_index("ey"), lax.axis_index("ex"), lax.axis_index("dp")
    me = [ey // RING, ey % RING, ex // CORES]
    core = ex % CORES
    rows = t + IDROWS
    split = (rows // 2 + 7) // 8 * 8

    def device(coords, c):
        return (dp, coords[0] * RING + coords[1], coords[2] * CORES + c)

    def shifted(axis, by, c=None):
        coords = list(me)
        coords[axis] = (coords[axis] + by) % RING
        return device(coords, core if c is None else c)

    loads = []
    for g, (start, width) in enumerate(groups):
        loads.append(pltpu.make_async_copy(
            x_ref.at[:, pl.ds(start, width)], got.at[g, 0, 0, pl.ds(0, t), pl.ds(0, width)], load_sem.at[g, 0]))
        loads.append(pltpu.make_async_copy(
            ids_ref, got.at[g, 0, 0, pl.ds(t, IDROWS), pl.ds(0, t)], load_sem.at[g, 1]))
    for load in loads:
        load.start()

    barrier = pltpu.get_barrier_semaphore()
    peers = [(axis, by, dc) for axis in range(3) for by in range(1, RING) for dc in range(CORES)] + [(0, 0, 1)]
    for axis, by, dc in peers:
        pl.semaphore_signal(barrier, inc=1, device_id=shifted(axis, by, (core + dc) % CORES),
                            device_id_type=MESH)
    row = lax.broadcasted_iota(jnp.int32, (t, t), 0)
    col = lax.broadcasted_iota(jnp.int32, (t, t), 1)
    upper[...] = jnp.where(row <= col, 1.0, 0.0).astype(bf16)
    pl.semaphore_wait(barrier, len(peers))
    for load in loads:
        load.wait()

    def hop(g, index, block, to, axis, by, part=None):
        width = groups[g][1]
        at = pl.ds(0, rows) if part is None else part
        copy = pltpu.make_async_remote_copy(
            src_ref=got.at[g, block[0], block[1], at, pl.ds(0, width)],
            dst_ref=got.at[g, to[0], to[1], at, pl.ds(0, width)],
            send_sem=gsend.at[g, index], recv_sem=grecv.at[g, index],
            device_id=shifted(axis, by), device_id_type=MESH)
        copy.start()
        hops[g, index] = copy

    hops = {}
    low, high = pl.ds(0, split), pl.ds(split, rows - split)

    def first(g):
        p = ORDERS[g][0]
        hop(g, 0, (0, 0), (3, 0), p, 1)
        hop(g, 1, (0, 0), (1, 0), p, 3)

    def second(g, i):
        q = ORDERS[g][1]
        hop(g, 4 + 4 * i, (i, 0), (i, 3), q, 1)
        hop(g, 5 + 4 * i, (i, 0), (i, 1), q, 3)

    def second_on(g, i):
        q = ORDERS[g][1]
        hops[g, 4 + 4 * i].wait_recv()
        hop(g, 6 + 4 * i, (i, 3), (i, 2), q, 1, low)
        hops[g, 5 + 4 * i].wait_recv()
        hop(g, 7 + 4 * i, (i, 1), (i, 2), q, 3, high)

    everyone = range(len(groups))
    for g in everyone:
        first(g)
        second(g, 0)
    for g in everyone:
        p = ORDERS[g][0]
        hops[g, 0].wait_recv()
        hop(g, 2, (3, 0), (2, 0), p, 1, low)
        second(g, 3)
        hops[g, 1].wait_recv()
        hop(g, 3, (1, 0), (2, 0), p, 3, high)
        second(g, 1)
    for g in everyone:
        second_on(g, 0)
    for g in everyone:
        hops[g, 2].wait_recv()
        hops[g, 3].wait_recv()
        second(g, 2)

    def choose(g, j):
        p, _, r = ORDERS[g]
        width = groups[g][1]
        stride = (RING * RING * CORES, RING * CORES, CORES)[r]
        base = ey * (RING * CORES) + ex - core - me[r] * stride

        def one(i, _):
            ids = got[g, i, j, pl.ds(t, IDROWS), pl.ds(0, t)].astype(f32)
            lines = []
            for k in range(RING * CORES):
                expert = (base + (k // CORES) * stride + k % CORES).astype(f32)
                lines.append(jnp.sum(jnp.where(ids == expert, 1.0, 0.0), axis=0, keepdims=True))
            hit = jnp.concatenate(lines, axis=0)
            rank = jnp.dot(hit.astype(bf16), upper[...], preferred_element_type=f32)
            slot = jnp.where((hit > 0.5) & (rank < cap + 0.5), rank - 1.0, -1.0)
            wanted = lax.broadcasted_iota(jnp.int32, (cap, t), 0).astype(f32)
            for k in range(RING * CORES):
                pick[pl.ds(k * cap, cap), :] = jnp.where(slot[k:k + 1, :] == wanted, 1.0, 0.0).astype(bf16)
            place = (me[p] + i) % RING

            def tile(n, _):
                at = pl.ds(pl.multiple_of(n * 128, 128), 128)
                val = jnp.dot(pick[...], got[g, i, j, pl.ds(0, t), at], preferred_element_type=f32).astype(bf16)
                for k in range(RING * CORES):
                    out[g, j, k, place, :, at] = val[k * cap:(k + 1) * cap]
                return 0

            return lax.fori_loop(0, width // 128, tile, 0)

        lax.fori_loop(0, RING, one, 0)

    def place_in(ref, g, j):
        start, width = groups[g]
        p, q, r = ORDERS[g]
        at = [None, None, None]
        at[p] = slice(None)
        at[q] = (me[q] + j) % RING
        at[r] = me[r]
        return ref.at[at[0], at[1], at[2], core, :, pl.ds(start, width)]

    sends, keeps = [], []

    def exchange(g, j):
        _, _, r = ORDERS[g]
        width = groups[g][1]
        for dr in range(RING):
            for dc in range(CORES):
                to, c = (me[r] + dr) % RING, (core + dc) % CORES
                src = out.at[g, j, to * CORES + c, :, :, pl.ds(0, width)]
                if dr == 0 and dc == 0:
                    copy = pltpu.make_async_copy(src, place_in(rx_ref, g, j), self_sem.at[g, j])
                    keeps.append(copy)
                else:
                    n = dr * CORES + dc
                    copy = pltpu.make_async_remote_copy(
                        src_ref=src, dst_ref=place_in(rx_ref, g, j),
                        send_sem=rsend.at[g, j, n], recv_sem=rrecv.at[g, j, n],
                        device_id=shifted(r, dr, c), device_id_type=MESH)
                    sends.append(copy)
                copy.start()

    for g in everyone:
        choose(g, 0)
        exchange(g, 0)
    for i in (3, 1):
        for g in everyone:
            second_on(g, i)
    for g in everyone:
        second_on(g, 2)
    for j in (3, 1):
        for g in everyone:
            choose(g, j)
            exchange(g, j)
    for g in everyone:
        for i in range(RING):
            hops[g, 6 + 4 * i].wait_recv()
            hops[g, 7 + 4 * i].wait_recv()
        choose(g, 2)
        exchange(g, 2)

    for copy in sends:
        copy.wait_recv()
    for copy in keeps:
        copy.wait()
    for copy in hops.values():
        copy.wait_send()
    for copy in sends:
        copy.wait_send()


def dispatch(x, ids, cap):
    t, hd = x.shape
    groups = column_groups(hd, 128)
    wide = max(w for _, w in groups)
    n = len(groups)
    peers = RING * CORES
    return pl.pallas_call(
        functools.partial(dispatch_kernel, t, cap, groups),
        out_shape=jax.ShapeDtypeStruct((RING, RING, RING, CORES, cap, hd), bf16),
        in_specs=[pl.BlockSpec(memory_space=pl.ANY)] * 2,
        out_specs=pl.BlockSpec(memory_space=pl.ANY),
        scratch_shapes=[
            pltpu.VMEM((n, RING, RING, t + IDROWS, wide), bf16),
            pltpu.VMEM((n, RING, peers, RING, cap, wide), bf16),
            pltpu.VMEM((t, t), bf16),
            pltpu.VMEM((peers * cap, t), bf16),
            pltpu.SemaphoreType.DMA((n, 2)),
            pltpu.SemaphoreType.DMA((n, 4 + 4 * RING)),
            pltpu.SemaphoreType.DMA((n, 4 + 4 * RING)),
            pltpu.SemaphoreType.DMA((n, RING, peers)),
            pltpu.SemaphoreType.DMA((n, RING, peers)),
            pltpu.SemaphoreType.DMA((n, RING)),
        ],
        compiler_params=pltpu.CompilerParams(collective_id=0, has_side_effects=True, vmem_limit_bytes=60 * 2 ** 20),
        name="dispatch",
    )(x, ids.T.astype(bf16))


def experts_kernel(t, cap, groups, info_ref, x_ref, rx_ref, w1_ref, w3_ref, w2_ref, y_ref, r2,
                   w1, w3, w2, xb, hh, res, top, ob, rest, so, r1, s1, s2, acc, part, planes, info, db, wt, upper, xv,
                   wsem, xsem, isend, irecv, p1s, p1r, q1s, q1r, p2s, p2r, q2s, q2r, p3s, p3r, hs, hr, e1s, e1r, e2s, e2r, dsem):
    ey, ex, dp = lax.axis_index("ey"), lax.axis_index("ex"), lax.axis_index("dp")
    me = [ey // RING, ey % RING, ex // CORES]
    core = ex % CORES
    rows = LINE * cap
    hd, ff = w1.shape
    everyone = range(len(groups))
    col0 = [start for start, _ in groups]
    width = [w for _, w in groups]
    main = min(width)
    more = width[0] - main
    own = [me[RETURNS[g][0]] * CORES + core for g in everyone]

    def shifted(axis, by, c=None):
        coords = list(me)
        coords[axis] = (coords[axis] + by) % RING
        return (dp, coords[0] * RING + coords[1], coords[2] * CORES + (core if c is None else c))

    def remote(src, dst, send, recv, to):
        return pltpu.make_async_remote_copy(src_ref=src, dst_ref=dst, send_sem=send, recv_sem=recv,
                                            device_id=to, device_id_type=MESH)

    loads = [pltpu.make_async_copy(a, b, wsem.at[n])
             for n, (a, b) in enumerate(((w1_ref, w1), (w3_ref, w3), (w2_ref, w2), (x_ref, xv)))]
    mine = [pltpu.make_async_copy(info_ref, info.at[axis, me[axis]], isend.at[axis, 0]) for axis in range(3)]
    for load in mine + loads:
        load.start()

    def homes(step):
        left = RING * RING - 1 - step
        return (left + left // RING) % RING, left % RING

    def tile_load(step):
        dz, dy = homes(step)
        return pltpu.make_async_copy(rx_ref.at[(me[0] + dz) % RING, (me[1] + dy) % RING], xb.at[step % 2], xsem.at[step % 2])

    tile_load(0).start()

    barrier = pltpu.get_barrier_semaphore()
    peers = [(axis, by, dc) for axis in range(3) for by in range(1, RING) for dc in range(CORES)] + [(0, 0, 1)]
    for axis, by, dc in peers:
        pl.semaphore_signal(barrier, inc=1, device_id=shifted(axis, by, (core + dc) % CORES), device_id_type=MESH)
    row = lax.broadcasted_iota(jnp.int32, (t, t), 0)
    col = lax.broadcasted_iota(jnp.int32, (t, t), 1)
    upper[...] = jnp.where(row <= col, 1.0, 0.0).astype(bf16)
    pl.semaphore_wait(barrier, len(peers))

    told = []
    for axis in range(3):
        for by in range(1, RING):
            told.append(remote(info_ref, info.at[axis, me[axis]], isend.at[axis, by], irecv.at[axis, by], shifted(axis, by)))
            told[-1].start()

    for load in mine + loads[:3]:
        load.wait()

    def first(step):
        dz, dy = homes(step)
        zh, yh = (me[0] + dz) % RING, (me[1] + dy) % RING
        slot = step % SLOTS
        found = []
        for n in range(1, LINE):
            d, dc = n // CORES, n % CORES
            c = (core + dc) % CORES
            found.append((None, remote(
                ob.at[slot, (me[2] + d) % RING, c, :, pl.ds(col0[0], main)],
                r1.at[0, own[0], zh, yh, :, pl.ds(0, main)],
                p1s.at[slot, n], p1r.at[0, n], shifted(2, d, c))))
        for g, axis, d, lead in ((1, 1, dy, zh), (2, 0, dz, yh)):
            for dc in range(CORES):
                c = (core + dc) % CORES
                found.append((None if dc else d != 0, remote(
                    ob.at[slot, :, c, :, pl.ds(col0[g], width[g])],
                    r1.at[g, own[g], lead, :, :, pl.ds(0, width[g])],
                    p1s.at[slot, LINE + 2 * (g - 1) + dc], p1r.at[g, d * CORES + dc], shifted(axis, d, c))))
        return found

    def each(found, act):
        for whether, copy in found:
            if whether is None:
                act(copy)
            else:
                @pl.when(whether)
                def _():
                    act(copy)

    eye = lax.broadcasted_iota(jnp.int32, (cap, 128), 0) == lax.broadcasted_iota(jnp.int32, (cap, 128), 1)

    def code(step, begin, end):
        slot = step % SLOTS
        for n in range(begin, end):
            at = pl.ds(n * 128, 128)
            v = jnp.round(res[:, at] * top[...]).astype(jnp.int32).astype(i16)
            ob[slot, :, :, :, at] = v.reshape(RING, CORES, cap, 128)

    def room(step):
        @pl.when(step >= SLOTS)
        def _():
            each(first(step - SLOTS), lambda copy: copy.wait_send())

    def leave(step):
        each(first(step), lambda copy: copy.start())
        dz, dy = homes(step)
        zh, yh = (me[0] + dz) % RING, (me[1] + dy) % RING
        slot = step % SLOTS
        r1[0, own[0], zh, yh, :, pl.ds(0, width[0])] = ob[slot, me[2], core, :, pl.ds(col0[0], width[0])]
        if more:
            rest[zh, yh] = ob[slot, :, :, :, pl.ds(col0[0] + main, more)]
        for g, d, lead in ((1, dy, zh), (2, dz, yh)):
            @pl.when(d == 0)
            def _():
                for xh in range(RING):
                    r1[g, own[g], lead, xh, :, pl.ds(0, width[g])] = ob[slot, xh, core, :, pl.ds(col0[g], width[g])]

    def tile(step, _):
        dz, dy = homes(step)
        zh, yh = (me[0] + dz) % RING, (me[1] + dy) % RING

        @pl.when(step + 1 < RING * RING)
        def _():
            tile_load(step + 1).start()

        room(step - 1)
        tile_load(step).wait()
        ups, codes = ff // TILE, hd // 128
        for n in range(ups):
            at = pl.ds(n * TILE, TILE)
            xt = xb[step % 2].reshape(rows, hd)
            a1 = jnp.dot(xt, w1[:, at], preferred_element_type=f32)
            a3 = jnp.dot(xt, w3[:, at], preferred_element_type=f32)
            hh[:, at] = (a1 * (1.0 / (1.0 + jnp.exp(-a1))) * a3).astype(bf16)
            code(step - 1, codes * n // ups, codes * (n + 1) // ups)

        @pl.when(step > 0)
        def _():
            leave(step - 1)

        most = jnp.zeros((rows, 128), f32)
        for n in range(hd // WIDE):
            o = jnp.dot(hh[...], w2[:, n * WIDE:(n + 1) * WIDE], preferred_element_type=f32)
            res[:, n * WIDE:(n + 1) * WIDE] = o
            o = jnp.abs(o)
            for k in range(WIDE // 128):
                most = jnp.maximum(most, o[:, k * 128:(k + 1) * 128])
        peak = jnp.maximum(jnp.max(most, axis=1, keepdims=True), 1e-30)
        top[...] = jnp.broadcast_to(FULL / peak, top.shape)
        for k in range(LINE):
            part = jnp.where(eye, peak[k * cap:(k + 1) * cap], 0.0)
            so[zh, yh, k // CORES, k % CORES] = jnp.sum(part, axis=0, keepdims=True) * (1.0 / FULL)
        return 0

    steps = RING * RING
    lax.fori_loop(0, steps, tile, 0)
    room(steps - 1)
    code(steps - 1, 0, hd // 128)
    leave(steps - 1)

    def scales(g, coord, c):
        return (so.at[:, :, coord, c], so.at[:, coord, :, c], so.at[coord, :, :, c])[g]

    hints = []
    for g in everyone:
        axis = RETURNS[g][0]
        s1[g, own[g]] = (so[:, :, me[2], core], so[:, me[1], :, core], so[me[0], :, :, core])[g]
        for n in range(1, LINE):
            d, dc = n // CORES, n % CORES
            c = (core + dc) % CORES
            hints.append(remote(scales(g, (me[axis] + d) % RING, c), s1.at[g, own[g]],
                                q1s.at[g, n], q1r.at[g, n], shifted(axis, d, c)))
            hints[-1].start()

    later = []
    if more:
        for n in range(1, LINE):
            d, dc = n // CORES, n % CORES
            c = (core + dc) % CORES
            later.append(remote(rest.at[:, :, (me[2] + d) % RING, c], r1.at[0, own[0], :, :, :, pl.ds(main, more)],
                                e1s.at[n], e1r.at[n], shifted(2, d, c)))
            later[-1].start()

    def lane(ref, g, h2, h3):
        return (ref.at[0, :, h3, h2], ref.at[1, :, h2, h3], ref.at[2, :, h3, h2])[g]

    def second(g, k3, d):
        _, axis, third = RETURNS[g]
        h3 = (me[third] + k3) % RING
        at = pl.ds(0, main)
        src = (r1.at[0, :, h3, (me[axis] + d) % RING, :, at] if g == 0 else
               r1.at[1, :, (me[axis] + d) % RING, h3, :, at] if g == 1 else
               r1.at[2, :, h3, (me[axis] + d) % RING, :, at])
        return remote(src, r2.at[g, h3, me[axis], :, :, at], p2s.at[g, k3, d], p2r.at[g, k3, d], shifted(axis, d))

    def second_more(k3, d):
        _, axis, third = RETURNS[0]
        h3 = (me[third] + k3) % RING
        at = pl.ds(main, more)
        return remote(r1.at[0, :, h3, (me[axis] + d) % RING, :, at], r2.at[0, h3, me[axis], :, :, at],
                      e2s.at[k3, d], e2r.at[k3, d], shifted(axis, d))

    for g in everyone:
        axis = RETURNS[g][0]
        for n in range(1, LINE):
            d, dc = n // CORES, n % CORES
            src = (me[axis] - d) % RING * CORES + (core + dc) % CORES
            ref = r1.at[g, src, :, :, :, pl.ds(0, main)]
            pltpu.make_async_copy(ref, ref, p1r.at[g, n]).wait()
        for d in (1, 3, 2):
            second(g, LINES[0], d).start()

    for copy in hints:
        copy.wait_recv()
    moved = []
    for g in everyone:
        axis = RETURNS[g][1]
        s2[g, me[axis]] = (s1[0, :, :, me[1]], s1[1, :, me[0]], s1[2, :, :, me[2]])[g]
        for d in (1, 3, 2):
            moved.append(remote(lane(s1, g, (me[axis] + d) % RING, slice(None)), s2.at[g, me[axis]],
                                q2s.at[g, d], q2r.at[g, d], shifted(axis, d)))
            moved[-1].start()

    for copy in later:
        copy.wait_recv()
    def rest_of(k3):
        for d in (1, 3, 2):
            if more:
                second_more(k3, d).start()
            for g in everyone:
                if k3 != LINES[0]:
                    second(g, k3, d).start()

    for k3 in LINES[:-1]:
        rest_of(k3)

    for copy in told:
        copy.wait_recv()
    for copy in moved:
        copy.wait_recv()

    wanted = lax.broadcasted_iota(jnp.int32, (cap, t), 0).astype(f32)

    def weights(g, h3, src):
        first_axis, axis, third = RETURNS[g]
        ids = info[third, h3, 0:8, :]
        gates = info[third, h3, 8:16, :]
        base = src * STRIDES[axis] + me[third] * STRIDES[third]
        hits, gate = [], []
        for k in range(LINE):
            same = ids == (base + (k // CORES) * STRIDES[first_axis] + k % CORES).astype(f32)
            hits.append(jnp.sum(jnp.where(same, 1.0, 0.0), axis=0, keepdims=True))
            gate.append(jnp.sum(jnp.where(same, gates, 0.0), axis=0, keepdims=True))
        hit = jnp.concatenate(hits, axis=0)
        rank = jnp.dot(hit.astype(bf16), upper[...], preferred_element_type=f32)
        slot = jnp.where((hit > 0.5) & (rank < cap + 0.5), rank - 1.0, -1.0)
        for k in range(LINE):
            scale = jnp.sum(jnp.where(eye, s2[g, src, k, h3], 0.0), axis=1, keepdims=True)
            w = jnp.where(slot[k:k + 1, :] == wanted, gate[k], 0.0) * scale
            a = w.astype(bf16)
            w = w - a.astype(f32)
            b = w.astype(bf16)
            w = w - b.astype(f32)
            at = pl.ds(k * cap, cap)
            wt[at, pl.ds(0, t)] = a
            wt[at, pl.ds(t, t)] = b
            wt[at, pl.ds(2 * t, t)] = w.astype(bf16)

    def line(index, _):
        k3 = 2 - index + 3 * (index // 2) - 2 * (index // 3)

        def plane(turn, _):
            d = turn + turn // 2 - 2 * (turn // 3)

            def fetch(g):
                third = RETURNS[g][2]
                src = (me[RETURNS[g][1]] - d) % RING
                return pltpu.make_async_copy(r2.at[g, (me[third] + k3) % RING, src, :, :, pl.ds(0, width[g])],
                                             db.at[g, :, :, pl.ds(0, width[g])], dsem.at[g])

            for g in everyone:
                _, axis, third = RETURNS[g]
                h3 = (me[third] + k3) % RING

                @pl.when(turn == 0)
                def _():
                    at = pl.ds(0, width[g])
                    if g == 1:
                        db[g, :, :, at] = r1[g, :, me[axis], h3, :, at]
                    else:
                        db[g, :, :, at] = r1[g, :, h3, me[axis], :, at]
                    acc[g, index] = jnp.zeros(acc.shape[2:], f32)

                @pl.when(turn > 0)
                def _():
                    second(g, k3, d).wait_recv()
                    if more and g == 0:
                        second_more(k3, d).wait_recv()
                    fetch(g).start()

            for g in everyone:
                _, axis, third = RETURNS[g]
                weights(g, (me[third] + k3) % RING, (me[axis] - d) % RING)

                @pl.when(turn > 0)
                def _():
                    fetch(g).wait()

                def piece(at, size):
                    q = db[g, :, :, at].reshape(rows, size).astype(f32)
                    high = q.astype(bf16)
                    low = (q - high.astype(f32)).astype(bf16)
                    dims = (((0,), (0,)), ((), ()))
                    p = (lax.dot_general(wt[...], high, dims, preferred_element_type=f32)
                         + lax.dot_general(wt[...], low, dims, preferred_element_type=f32))
                    acc[g, index, :, at] += p[0:t] + p[t:2 * t] + p[2 * t:]

                begin = 0
                while begin < width[g]:
                    size = min(WIDE, width[g] - begin)
                    piece(pl.ds(begin, size), size)
                    begin += size

                @pl.when((turn == RING - 1) & (index == 0))
                def _():
                    for way in range(2):
                        opposite(g, way).start()

                @pl.when((turn == RING - 1) & (index == 2))
                def _():
                    for way in range(2):
                        opposite(g, way).wait_recv()
                        rows_of = pl.ds(way * (t // 2), t // 2)
                        at = pl.ds(0, width[g])
                        acc[g, 1 + way, rows_of, at] += part[g, way, :, at]
                    for way in range(2):
                        home(g, way).start()
            return 0

        lax.fori_loop(0, RING, plane, 0)

        @pl.when(index == 0)
        def _():
            rest_of(LINES[-1])
        return 0

    def opposite(g, way):
        at = pl.ds(0, width[g])
        return remote(acc.at[g, 0, pl.ds(way * (t // 2), t // 2), at], part.at[g, way, :, at],
                      hs.at[g, way], hr.at[g, way], shifted(RETURNS[g][2], LINES[1 + way]))

    def home(g, way):
        at = pl.ds(0, width[g])
        return remote(acc.at[g, 1 + way, :, at], planes.at[g, way, :, at],
                      p3s.at[g, way], p3r.at[g, way], shifted(RETURNS[g][2], LINES[1 + way]))

    lax.fori_loop(0, RING, line, 0)

    loads[3].wait()
    for g in everyone:
        for way in range(2):
            home(g, way).wait_recv()

        def finish(n, _):
            at = pl.ds(pl.multiple_of(n * 128, 128), 128)
            to = pl.ds(pl.multiple_of(col0[g] + n * 128, 128), 128)
            total = acc[g, RING - 1, :, at] + planes[g, 0, :, at] + planes[g, 1, :, at]
            y_ref[:, to] = (xv[:, to].astype(f32) + total).astype(bf16)
            return 0

        lax.fori_loop(0, width[g] // 128, finish, 0)

    for copy in told + hints + moved + later:
        copy.wait_send()

    def last(step, _):
        each(first(step), lambda copy: copy.wait_send())
        return 0

    lax.fori_loop(RING * RING - SLOTS, RING * RING, last, 0)
    for g in everyone:
        for k3 in range(RING):
            for d in (1, 3, 2):
                second(g, k3, d).wait_send()
                if more and g == 0:
                    second_more(k3, d).wait_send()
        for way in range(2):
            opposite(g, way).wait_send()
            home(g, way).wait_send()


def experts(x, ids, gates, rx, w1, w3, w2):
    t, hd = x.shape
    ff = w1.shape[1]
    cap = rx.shape[4]
    groups = column_groups(hd, 128)
    wide = max(w for _, w in groups)
    n = len(groups)
    more = max(wide - min(w for _, w in groups), 128)
    info = jnp.concatenate([ids.T.astype(f32), gates.T], axis=0)
    dma = pltpu.SemaphoreType.DMA
    anywhere = pl.BlockSpec(memory_space=pl.ANY)
    vmem = pl.BlockSpec(memory_space=pltpu.VMEM)
    y, _ = pl.pallas_call(
        functools.partial(experts_kernel, t, cap, groups),
        out_shape=(jax.ShapeDtypeStruct((t, hd), bf16),
                   jax.ShapeDtypeStruct((n, RING, RING, LINE, cap, wide), i16)),
        in_specs=[anywhere] * 6,
        out_specs=(vmem, anywhere),
        scratch_shapes=[
            pltpu.VMEM((hd, ff), bf16), pltpu.VMEM((hd, ff), bf16), pltpu.VMEM((ff, hd), bf16),
            pltpu.VMEM((2, RING, CORES, cap, hd), bf16),
            pltpu.VMEM((LINE * cap, ff), bf16),
            pltpu.VMEM((LINE * cap, hd), f32),
            pltpu.VMEM((LINE * cap, 128), f32),
            pltpu.VMEM((SLOTS, RING, CORES, cap, hd), i16),
            pltpu.VMEM((RING, RING, RING, CORES, cap, more), i16),
            pltpu.VMEM((RING, RING, RING, CORES, 1, 128), f32),
            pltpu.VMEM((n, LINE, RING, RING, cap, wide), i16),
            pltpu.VMEM((n, LINE, RING, RING, 1, 128), f32),
            pltpu.VMEM((n, RING, LINE, RING, 1, 128), f32),
            pltpu.VMEM((n, RING, t, wide), f32),
            pltpu.VMEM((n, 2, t // 2, wide), f32),
            pltpu.VMEM((n, 2, t, wide), f32),
            pltpu.VMEM((3, RING, 16, t), f32),
            pltpu.VMEM((n, LINE, cap, wide), i16),
            pltpu.VMEM((LINE * cap, 3 * t), bf16),
            pltpu.VMEM((t, t), bf16),
            pltpu.VMEM((t, hd), bf16),
            dma((4,)), dma((2,)), dma((3, RING)), dma((3, RING)),
            dma((SLOTS, LINE + 4)), dma((n, LINE)), dma((n, LINE)), dma((n, LINE)),
            dma((n, RING, RING)), dma((n, RING, RING)), dma((n, RING)), dma((n, RING)),
            dma((n, 2)), dma((n, 2)), dma((n, 2)), dma((n, 2)), dma((LINE,)), dma((LINE,)), dma((RING, RING)), dma((RING, RING)), dma((n,)),
        ],
        compiler_params=pltpu.CompilerParams(collective_id=1, has_side_effects=True, vmem_limit_bytes=67043328),
        name="experts",
    )(info, x, rx, w1, w3, w2)
    return y


def solution(mesh):
    nd = mesh.shape["ey"] * mesh.shape["ex"]
    tok = P(("dp", "ey", "ex"), None)
    wsp = P(("ey", "ex"), None, None)

    def local(x, ids, gates, w1, w3, w2):
        t = x.shape[0]
        cap = min(t, CAPF * t * ids.shape[1] // nd)
        rx = dispatch(x, ids, cap)
        return experts(x, ids, gates, rx, w1[0], w3[0], w2[0])

    return jax.shard_map(local, mesh=mesh, in_specs=(tok, tok, tok, wsp, wsp, wsp),
                         out_specs=tok, check_vma=False)
```

```python
import functools

import jax
import jax.numpy as jnp
from jax import lax
from jax.experimental import pallas as pl
from jax.experimental.pallas import tpu as pltpu
from jax.sharding import PartitionSpec as P

CAPF = 2
FULL = 32000.0
RING = 4
CORES = 2
IDROWS = 8
ORDERS = ((0, 1, 2), (2, 0, 1), (1, 2, 0))
LINE = RING * CORES
STRIDES = (RING * RING * CORES, RING * CORES, CORES)
RETURNS = ((2, 1, 0), (1, 0, 2), (0, 2, 1))
TILE = 256
LINES = (2, 1, 3, 0)
WIDE = 512
SLOTS = 5
MESH = pl.DeviceIdType.MESH
PEERS = [(axis, by, dc) for axis in range(3) for by in range(1, RING) for dc in range(CORES)] + [(0, 0, 1)]
bf16, i16, f32 = jnp.bfloat16, jnp.int16, jnp.float32


def column_groups(hd, tile):
    tiles = hd // tile
    first = -(-tiles // 3)
    second = -(-(tiles - first) // 2)
    widths = [first * tile, second * tile, (tiles - first - second) * tile]
    starts = [0, widths[0], widths[0] + widths[1]]
    return list(zip(starts, widths))


def dispatch_part(t, cap, groups, x_ref, rx_ref, idv, gatev, upper, info, load_sem, gsend, grecv, rsend, rrecv, self_sem,
                  isend, irecv, weight_loads, got, out, pick):
    ey, ex, dp = lax.axis_index("ey"), lax.axis_index("ex"), lax.axis_index("dp")
    me = [ey // RING, ey % RING, ex // CORES]
    core = ex % CORES
    rows = t + IDROWS
    split = (rows // 2 + 7) // 8 * 8

    def device(coords, c):
        return (dp, coords[0] * RING + coords[1], coords[2] * CORES + c)

    def shifted(axis, by, c=None):
        coords = list(me)
        coords[axis] = (coords[axis] + by) % RING
        return device(coords, core if c is None else c)

    loads = [pltpu.make_async_copy(x_ref.at[:, pl.ds(start, width)], got.at[g, 0, 0, pl.ds(0, t), pl.ds(0, width)],
                                   load_sem.at[g]) for g, (start, width) in enumerate(groups)]
    for load in loads:
        load.start()

    barrier = pltpu.get_barrier_semaphore()
    for axis, by, dc in PEERS:
        pl.semaphore_signal(barrier, inc=1, device_id=shifted(axis, by, (core + dc) % CORES), device_id_type=MESH)
    row = lax.broadcasted_iota(jnp.int32, (t, t), 0)
    col = lax.broadcasted_iota(jnp.int32, (t, t), 1)
    upper[...] = jnp.where(row <= col, 1.0, 0.0).astype(bf16)
    ids = idv[...].astype(f32)
    for g in range(len(groups)):
        got[g, 0, 0, pl.ds(t, IDROWS), pl.ds(0, t)] = ids.astype(bf16)
    for axis in range(3):
        info[axis, me[axis], 0:8, :] = ids
        info[axis, me[axis], 8:16, :] = gatev[...]
    pl.semaphore_wait(barrier, len(PEERS))
    for load in loads:
        load.wait()

    def hop(g, index, block, to, axis, by, part=None):
        width = groups[g][1]
        at = pl.ds(0, rows) if part is None else part
        copy = pltpu.make_async_remote_copy(
            src_ref=got.at[g, block[0], block[1], at, pl.ds(0, width)],
            dst_ref=got.at[g, to[0], to[1], at, pl.ds(0, width)],
            send_sem=gsend.at[g, index], recv_sem=grecv.at[g, index],
            device_id=shifted(axis, by), device_id_type=MESH)
        copy.start()
        hops[g, index] = copy

    hops = {}
    low, high = pl.ds(0, split), pl.ds(split, rows - split)

    def first(g):
        p = ORDERS[g][0]
        hop(g, 0, (0, 0), (3, 0), p, 1)
        hop(g, 1, (0, 0), (1, 0), p, 3)

    def second(g, i):
        q = ORDERS[g][1]
        hop(g, 4 + 4 * i, (i, 0), (i, 3), q, 1)
        hop(g, 5 + 4 * i, (i, 0), (i, 1), q, 3)

    def second_on(g, i):
        q = ORDERS[g][1]
        hops[g, 4 + 4 * i].wait_recv()
        hop(g, 6 + 4 * i, (i, 3), (i, 2), q, 1, low)
        hops[g, 5 + 4 * i].wait_recv()
        hop(g, 7 + 4 * i, (i, 1), (i, 2), q, 3, high)

    everyone = range(len(groups))
    for g in everyone:
        first(g)
        second(g, 0)
    for load in weight_loads:
        load.start()
    for g in everyone:
        p = ORDERS[g][0]
        hops[g, 0].wait_recv()
        hop(g, 2, (3, 0), (2, 0), p, 1, low)
        second(g, 3)
        hops[g, 1].wait_recv()
        hop(g, 3, (1, 0), (2, 0), p, 3, high)
        second(g, 1)
    for g in everyone:
        second_on(g, 0)
    for g in everyone:
        hops[g, 2].wait_recv()
        hops[g, 3].wait_recv()
        second(g, 2)

    def choose(g, j):
        p, _, r = ORDERS[g]
        width = groups[g][1]
        stride = (RING * RING * CORES, RING * CORES, CORES)[r]
        base = ey * (RING * CORES) + ex - core - me[r] * stride

        def one(i, _):
            ids = got[g, i, j, pl.ds(t, IDROWS), pl.ds(0, t)].astype(f32)
            lines = []
            for k in range(RING * CORES):
                expert = (base + (k // CORES) * stride + k % CORES).astype(f32)
                lines.append(jnp.sum(jnp.where(ids == expert, 1.0, 0.0), axis=0, keepdims=True))
            hit = jnp.concatenate(lines, axis=0)
            rank = jnp.dot(hit.astype(bf16), upper[...], preferred_element_type=f32)
            slot = jnp.where((hit > 0.5) & (rank < cap + 0.5), rank - 1.0, -1.0)
            wanted = lax.broadcasted_iota(jnp.int32, (cap, t), 0).astype(f32)
            for k in range(RING * CORES):
                pick[pl.ds(k * cap, cap), :] = jnp.where(slot[k:k + 1, :] == wanted, 1.0, 0.0).astype(bf16)
            place = (me[p] + i) % RING

            def tile(n, _):
                at = pl.ds(pl.multiple_of(n * 128, 128), 128)
                val = jnp.dot(pick[...], got[g, i, j, pl.ds(0, t), at], preferred_element_type=f32).astype(bf16)
                for k in range(RING * CORES):
                    out[g, j, k, place, :, at] = val[k * cap:(k + 1) * cap]
                return 0

            return lax.fori_loop(0, width // 128, tile, 0)

        lax.fori_loop(0, RING, one, 0)

    def place_in(ref, g, j):
        start, width = groups[g]
        p, q, r = ORDERS[g]
        at = [None, None, None]
        at[p] = slice(None)
        at[q] = (me[q] + j) % RING
        at[r] = me[r]
        return ref.at[at[0], at[1], at[2], core, :, pl.ds(start, width)]

    sends, keeps = [], []

    def exchange(g, j):
        _, _, r = ORDERS[g]
        width = groups[g][1]
        for dr in range(RING):
            for dc in range(CORES):
                to, c = (me[r] + dr) % RING, (core + dc) % CORES
                src = out.at[g, j, to * CORES + c, :, :, pl.ds(0, width)]
                if dr == 0 and dc == 0:
                    copy = pltpu.make_async_copy(src, place_in(rx_ref, g, j), self_sem.at[g, j])
                    keeps.append(copy)
                else:
                    n = dr * CORES + dc
                    copy = pltpu.make_async_remote_copy(
                        src_ref=src, dst_ref=place_in(rx_ref, g, j),
                        send_sem=rsend.at[g, j, n], recv_sem=rrecv.at[g, j, n],
                        device_id=shifted(r, dr, c), device_id_type=MESH)
                    sends.append(copy)
                copy.start()

    for g in everyone:
        choose(g, 0)
        exchange(g, 0)
    for i in (3, 1):
        for g in everyone:
            second_on(g, i)
    for g in everyone:
        second_on(g, 2)
    for j in (3, 1):
        for g in everyone:
            choose(g, j)
            exchange(g, j)
    for g in everyone:
        for i in range(RING):
            hops[g, 6 + 4 * i].wait_recv()
            hops[g, 7 + 4 * i].wait_recv()
        choose(g, 2)
        exchange(g, 2)

    told = []
    for axis in range(3):
        for by in range(1, RING):
            told.append(pltpu.make_async_remote_copy(
                src_ref=info.at[axis, me[axis]], dst_ref=info.at[axis, me[axis]], send_sem=isend.at[axis, by],
                recv_sem=irecv.at[axis, by], device_id=shifted(axis, by), device_id_type=MESH))
            told[-1].start()

    for copy in sends:
        copy.wait_recv()
    for copy in keeps:
        copy.wait()
    for copy in hops.values():
        copy.wait_send()
    for copy in sends + told:
        copy.wait_send()
    for copy in told:
        copy.wait_recv()


def experts_part(t, cap, groups, x_ref, rx_ref, y_ref, r2, w1, w3, w2, info, upper, ready, weight_loads, xload_sem, sems,
                 xb, hh, res, top, ob, rest, so, r1, s1, s2, acc, part, planes, db, wt, xv):
    xsem, p1s, p1r, q1s, q1r, p2s, p2r, q2s, q2r, p3s, p3r, hs, hr, e1s, e1r, e2s, e2r, dsem = sems
    ey, ex, dp = lax.axis_index("ey"), lax.axis_index("ex"), lax.axis_index("dp")
    me = [ey // RING, ey % RING, ex // CORES]
    core = ex % CORES
    rows = LINE * cap
    hd, ff = w1.shape
    everyone = range(len(groups))
    col0 = [start for start, _ in groups]
    width = [w for _, w in groups]
    main = min(width)
    more = width[0] - main
    own = [me[RETURNS[g][0]] * CORES + core for g in everyone]

    def shifted(axis, by, c=None):
        coords = list(me)
        coords[axis] = (coords[axis] + by) % RING
        return (dp, coords[0] * RING + coords[1], coords[2] * CORES + (core if c is None else c))

    def remote(src, dst, send, recv, to):
        return pltpu.make_async_remote_copy(src_ref=src, dst_ref=dst, send_sem=send, recv_sem=recv,
                                            device_id=to, device_id_type=MESH)

    def homes(step):
        left = RING * RING - 1 - step
        return (left + left // RING) % RING, left % RING

    def tile_load(step):
        dz, dy = homes(step)
        return pltpu.make_async_copy(rx_ref.at[(me[0] + dz) % RING, (me[1] + dy) % RING], xb.at[step % 2], xsem.at[step % 2])

    tile_load(0).start()

    for axis, by, dc in PEERS:
        pl.semaphore_signal(ready, inc=1, device_id=shifted(axis, by, (core + dc) % CORES), device_id_type=MESH)
    xload = pltpu.make_async_copy(x_ref, xv, xload_sem)
    xload.start()
    for load in weight_loads:
        load.wait()

    def first(step):
        dz, dy = homes(step)
        zh, yh = (me[0] + dz) % RING, (me[1] + dy) % RING
        slot = step % SLOTS
        found = []
        for n in range(1, LINE):
            d, dc = n // CORES, n % CORES
            c = (core + dc) % CORES
            found.append((None, remote(
                ob.at[slot, (me[2] + d) % RING, c, :, pl.ds(col0[0], main)],
                r1.at[0, own[0], zh, yh, :, pl.ds(0, main)],
                p1s.at[slot, n], p1r.at[0, n], shifted(2, d, c))))
        for g, axis, d, lead in ((1, 1, dy, zh), (2, 0, dz, yh)):
            for dc in range(CORES):
                c = (core + dc) % CORES
                found.append((None if dc else d != 0, remote(
                    ob.at[slot, :, c, :, pl.ds(col0[g], width[g])],
                    r1.at[g, own[g], lead, :, :, pl.ds(0, width[g])],
                    p1s.at[slot, LINE + 2 * (g - 1) + dc], p1r.at[g, d * CORES + dc], shifted(axis, d, c))))
        return found

    def each(found, act):
        for whether, copy in found:
            if whether is None:
                act(copy)
            else:
                @pl.when(whether)
                def _():
                    act(copy)

    eye = lax.broadcasted_iota(jnp.int32, (cap, 128), 0) == lax.broadcasted_iota(jnp.int32, (cap, 128), 1)

    def code(step, begin, end):
        slot = step % SLOTS
        for n in range(begin, end):
            at = pl.ds(n * 128, 128)
            v = jnp.round(res[:, at] * top[...]).astype(jnp.int32).astype(i16)
            ob[slot, :, :, :, at] = v.reshape(RING, CORES, cap, 128)

    def room(step):
        @pl.when(step >= SLOTS)
        def _():
            each(first(step - SLOTS), lambda copy: copy.wait_send())

    def leave(step):
        each(first(step), lambda copy: copy.start())
        dz, dy = homes(step)
        zh, yh = (me[0] + dz) % RING, (me[1] + dy) % RING
        slot = step % SLOTS
        r1[0, own[0], zh, yh, :, pl.ds(0, width[0])] = ob[slot, me[2], core, :, pl.ds(col0[0], width[0])]
        if more:
            rest[zh, yh] = ob[slot, :, :, :, pl.ds(col0[0] + main, more)]
        for g, d, lead in ((1, dy, zh), (2, dz, yh)):
            @pl.when(d == 0)
            def _():
                for xh in range(RING):
                    r1[g, own[g], lead, xh, :, pl.ds(0, width[g])] = ob[slot, xh, core, :, pl.ds(col0[g], width[g])]

    def tile(step, _):
        dz, dy = homes(step)
        zh, yh = (me[0] + dz) % RING, (me[1] + dy) % RING

        @pl.when(step + 1 < RING * RING)
        def _():
            tile_load(step + 1).start()

        room(step - 1)
        tile_load(step).wait()
        ups, codes = ff // TILE, hd // 128
        for n in range(ups):
            at = pl.ds(n * TILE, TILE)
            xt = xb[step % 2].reshape(rows, hd)
            a1 = jnp.dot(xt, w1[:, at], preferred_element_type=f32)
            a3 = jnp.dot(xt, w3[:, at], preferred_element_type=f32)
            hh[:, at] = (a1 * (1.0 / (1.0 + jnp.exp(-a1))) * a3).astype(bf16)
            code(step - 1, codes * n // ups, codes * (n + 1) // ups)

        @pl.when(step == 1)
        def _():
            pl.semaphore_wait(ready, len(PEERS))

        @pl.when(step > 0)
        def _():
            leave(step - 1)

        most = jnp.zeros((rows, 128), f32)
        for n in range(hd // WIDE):
            o = jnp.dot(hh[...], w2[:, n * WIDE:(n + 1) * WIDE], preferred_element_type=f32)
            res[:, n * WIDE:(n + 1) * WIDE] = o
            o = jnp.abs(o)
            for k in range(WIDE // 128):
                most = jnp.maximum(most, o[:, k * 128:(k + 1) * 128])
        peak = jnp.maximum(jnp.max(most, axis=1, keepdims=True), 1e-30)
        top[...] = jnp.broadcast_to(FULL / peak, top.shape)
        for k in range(LINE):
            part = jnp.where(eye, peak[k * cap:(k + 1) * cap], 0.0)
            so[zh, yh, k // CORES, k % CORES] = jnp.sum(part, axis=0, keepdims=True) * (1.0 / FULL)
        return 0

    steps = RING * RING
    lax.fori_loop(0, steps, tile, 0)
    room(steps - 1)
    code(steps - 1, 0, hd // 128)
    leave(steps - 1)

    def scales(g, coord, c):
        return (so.at[:, :, coord, c], so.at[:, coord, :, c], so.at[coord, :, :, c])[g]

    hints = []
    for g in everyone:
        axis = RETURNS[g][0]
        s1[g, own[g]] = (so[:, :, me[2], core], so[:, me[1], :, core], so[me[0], :, :, core])[g]
        for n in range(1, LINE):
            d, dc = n // CORES, n % CORES
            c = (core + dc) % CORES
            hints.append(remote(scales(g, (me[axis] + d) % RING, c), s1.at[g, own[g]],
                                q1s.at[g, n], q1r.at[g, n], shifted(axis, d, c)))
            hints[-1].start()

    later = []
    if more:
        for n in range(1, LINE):
            d, dc = n // CORES, n % CORES
            c = (core + dc) % CORES
            later.append(remote(rest.at[:, :, (me[2] + d) % RING, c], r1.at[0, own[0], :, :, :, pl.ds(main, more)],
                                e1s.at[n], e1r.at[n], shifted(2, d, c)))
            later[-1].start()

    def lane(ref, g, h2, h3):
        return (ref.at[0, :, h3, h2], ref.at[1, :, h2, h3], ref.at[2, :, h3, h2])[g]

    def second(g, k3, d):
        _, axis, third = RETURNS[g]
        h3 = (me[third] + k3) % RING
        at = pl.ds(0, main)
        src = (r1.at[0, :, h3, (me[axis] + d) % RING, :, at] if g == 0 else
               r1.at[1, :, (me[axis] + d) % RING, h3, :, at] if g == 1 else
               r1.at[2, :, h3, (me[axis] + d) % RING, :, at])
        return remote(src, r2.at[g, h3, me[axis], :, :, at], p2s.at[g, k3, d], p2r.at[g, k3, d], shifted(axis, d))

    def second_more(k3, d):
        _, axis, third = RETURNS[0]
        h3 = (me[third] + k3) % RING
        at = pl.ds(main, more)
        return remote(r1.at[0, :, h3, (me[axis] + d) % RING, :, at], r2.at[0, h3, me[axis], :, :, at],
                      e2s.at[k3, d], e2r.at[k3, d], shifted(axis, d))

    for g in everyone:
        axis = RETURNS[g][0]
        for n in range(1, LINE):
            d, dc = n // CORES, n % CORES
            src = (me[axis] - d) % RING * CORES + (core + dc) % CORES
            ref = r1.at[g, src, :, :, :, pl.ds(0, main)]
            pltpu.make_async_copy(ref, ref, p1r.at[g, n]).wait()
        for d in (1, 3, 2):
            second(g, LINES[0], d).start()

    for copy in hints:
        copy.wait_recv()
    moved = []
    for g in everyone:
        axis = RETURNS[g][1]
        s2[g, me[axis]] = (s1[0, :, :, me[1]], s1[1, :, me[0]], s1[2, :, :, me[2]])[g]
        for d in (1, 3, 2):
            moved.append(remote(lane(s1, g, (me[axis] + d) % RING, slice(None)), s2.at[g, me[axis]],
                                q2s.at[g, d], q2r.at[g, d], shifted(axis, d)))
            moved[-1].start()

    for copy in later:
        copy.wait_recv()
    def rest_of(k3):
        for d in (1, 3, 2):
            if more:
                second_more(k3, d).start()
            for g in everyone:
                if k3 != LINES[0]:
                    second(g, k3, d).start()

    for k3 in LINES[:-1]:
        rest_of(k3)

    for copy in moved:
        copy.wait_recv()

    wanted = lax.broadcasted_iota(jnp.int32, (cap, t), 0).astype(f32)

    def weights(g, h3, src):
        first_axis, axis, third = RETURNS[g]
        ids = info[third, h3, 0:8, :]
        gates = info[third, h3, 8:16, :]
        base = src * STRIDES[axis] + me[third] * STRIDES[third]
        hits, gate = [], []
        for k in range(LINE):
            same = ids == (base + (k // CORES) * STRIDES[first_axis] + k % CORES).astype(f32)
            hits.append(jnp.sum(jnp.where(same, 1.0, 0.0), axis=0, keepdims=True))
            gate.append(jnp.sum(jnp.where(same, gates, 0.0), axis=0, keepdims=True))
        hit = jnp.concatenate(hits, axis=0)
        rank = jnp.dot(hit.astype(bf16), upper[...], preferred_element_type=f32)
        slot = jnp.where((hit > 0.5) & (rank < cap + 0.5), rank - 1.0, -1.0)
        for k in range(LINE):
            scale = jnp.sum(jnp.where(eye, s2[g, src, k, h3], 0.0), axis=1, keepdims=True)
            w = jnp.where(slot[k:k + 1, :] == wanted, gate[k], 0.0) * scale
            a = w.astype(bf16)
            w = w - a.astype(f32)
            b = w.astype(bf16)
            w = w - b.astype(f32)
            at = pl.ds(k * cap, cap)
            wt[at, pl.ds(0, t)] = a
            wt[at, pl.ds(t, t)] = b
            wt[at, pl.ds(2 * t, t)] = w.astype(bf16)

    def line(index, _):
        k3 = 2 - index + 3 * (index // 2) - 2 * (index // 3)

        def plane(turn, _):
            d = turn + turn // 2 - 2 * (turn // 3)

            def fetch(g):
                third = RETURNS[g][2]
                src = (me[RETURNS[g][1]] - d) % RING
                return pltpu.make_async_copy(r2.at[g, (me[third] + k3) % RING, src, :, :, pl.ds(0, width[g])],
                                             db.at[g, :, :, pl.ds(0, width[g])], dsem.at[g])

            for g in everyone:
                _, axis, third = RETURNS[g]
                h3 = (me[third] + k3) % RING

                @pl.when(turn == 0)
                def _():
                    at = pl.ds(0, width[g])
                    if g == 1:
                        db[g, :, :, at] = r1[g, :, me[axis], h3, :, at]
                    else:
                        db[g, :, :, at] = r1[g, :, h3, me[axis], :, at]
                    acc[g, index] = jnp.zeros(acc.shape[2:], f32)

                @pl.when(turn > 0)
                def _():
                    second(g, k3, d).wait_recv()
                    if more and g == 0:
                        second_more(k3, d).wait_recv()
                    fetch(g).start()

            for g in everyone:
                _, axis, third = RETURNS[g]
                weights(g, (me[third] + k3) % RING, (me[axis] - d) % RING)

                @pl.when(turn > 0)
                def _():
                    fetch(g).wait()

                def piece(at, size):
                    q = db[g, :, :, at].reshape(rows, size).astype(f32)
                    high = q.astype(bf16)
                    low = (q - high.astype(f32)).astype(bf16)
                    dims = (((0,), (0,)), ((), ()))
                    p = (lax.dot_general(wt[...], high, dims, preferred_element_type=f32)
                         + lax.dot_general(wt[...], low, dims, preferred_element_type=f32))
                    acc[g, index, :, at] += p[0:t] + p[t:2 * t] + p[2 * t:]

                begin = 0
                while begin < width[g]:
                    size = min(WIDE, width[g] - begin)
                    piece(pl.ds(begin, size), size)
                    begin += size

                @pl.when((turn == RING - 1) & (index == 0))
                def _():
                    for way in range(2):
                        opposite(g, way).start()

                @pl.when((turn == RING - 1) & (index == 2))
                def _():
                    for way in range(2):
                        opposite(g, way).wait_recv()
                        rows_of = pl.ds(way * (t // 2), t // 2)
                        at = pl.ds(0, width[g])
                        acc[g, 1 + way, rows_of, at] += part[g, way, :, at]
                    for way in range(2):
                        home(g, way).start()
            return 0

        lax.fori_loop(0, RING, plane, 0)

        @pl.when(index == 0)
        def _():
            rest_of(LINES[-1])
        return 0

    def opposite(g, way):
        at = pl.ds(0, width[g])
        return remote(acc.at[g, 0, pl.ds(way * (t // 2), t // 2), at], part.at[g, way, :, at],
                      hs.at[g, way], hr.at[g, way], shifted(RETURNS[g][2], LINES[1 + way]))

    def home(g, way):
        at = pl.ds(0, width[g])
        return remote(acc.at[g, 1 + way, :, at], planes.at[g, way, :, at],
                      p3s.at[g, way], p3r.at[g, way], shifted(RETURNS[g][2], LINES[1 + way]))

    lax.fori_loop(0, RING, line, 0)

    xload.wait()
    for g in reversed(everyone):
        for way in range(2):
            home(g, way).wait_recv()

        def finish(n, _):
            at = pl.ds(pl.multiple_of(n * 128, 128), 128)
            to = pl.ds(pl.multiple_of(col0[g] + n * 128, 128), 128)
            total = acc[g, RING - 1, :, at] + planes[g, 0, :, at] + planes[g, 1, :, at]
            y_ref[:, to] = (xv[:, to].astype(f32) + total).astype(bf16)
            return 0

        lax.fori_loop(0, width[g] // 128, finish, 0)

    for copy in hints + moved + later:
        copy.wait_send()

    def last(step, _):
        each(first(step), lambda copy: copy.wait_send())
        return 0

    lax.fori_loop(RING * RING - SLOTS, RING * RING, last, 0)
    for g in everyone:
        for k3 in range(RING):
            for d in (1, 3, 2):
                second(g, k3, d).wait_send()
                if more and g == 0:
                    second_more(k3, d).wait_send()
        for way in range(2):
            opposite(g, way).wait_send()
            home(g, way).wait_send()


def layer_kernel(t, cap, groups, ids_ref, gates_ref, x_ref, w1_ref, w3_ref, w2_ref, y_ref, rx_ref, r2,
                 w1, w3, w2, idv, gatev, info, upper, ready, small_sem, wsem, load_sem, gsend, grecv, rsend, rrecv, self_sem,
                 isend, irecv, xload_sem, *sems):
    hd, ff = w1.shape
    n = len(groups)
    wide = max(w for _, w in groups)
    more = max(wide - min(w for _, w in groups), 128)
    small = [pltpu.make_async_copy(a, b, small_sem.at[k]) for k, (a, b) in enumerate(((ids_ref, idv), (gates_ref, gatev)))]
    weight_loads = [pltpu.make_async_copy(a, b, wsem.at[k])
                    for k, (a, b) in enumerate(((w1_ref, w1), (w3_ref, w3), (w2_ref, w2)))]
    for load in small:
        load.start()
    for load in small:
        load.wait()

    def there(got, out, pick):
        dispatch_part(t, cap, groups, x_ref, rx_ref, idv, gatev, upper, info, load_sem, gsend, grecv, rsend, rrecv, self_sem,
                      isend, irecv, weight_loads, got, out, pick)

    pl.run_scoped(there,
                  pltpu.VMEM((n, RING, RING, t + IDROWS, wide), bf16),
                  pltpu.VMEM((n, RING, LINE, RING, cap, wide), bf16),
                  pltpu.VMEM((LINE * cap, t), bf16))

    def back(*scratch):
        experts_part(t, cap, groups, x_ref, rx_ref, y_ref, r2, w1, w3, w2, info, upper, ready, weight_loads, xload_sem, sems,
                     *scratch)

    pl.run_scoped(back,
                  pltpu.VMEM((2, RING, CORES, cap, hd), bf16),
                  pltpu.VMEM((LINE * cap, ff), bf16),
                  pltpu.VMEM((LINE * cap, hd), f32),
                  pltpu.VMEM((LINE * cap, 128), f32),
                  pltpu.VMEM((SLOTS, RING, CORES, cap, hd), i16),
                  pltpu.VMEM((RING, RING, RING, CORES, cap, more), i16),
                  pltpu.VMEM((RING, RING, RING, CORES, 1, 128), f32),
                  pltpu.VMEM((n, LINE, RING, RING, cap, wide), i16),
                  pltpu.VMEM((n, LINE, RING, RING, 1, 128), f32),
                  pltpu.VMEM((n, RING, LINE, RING, 1, 128), f32),
                  pltpu.VMEM((n, RING, t, wide), f32),
                  pltpu.VMEM((n, 2, t // 2, wide), f32),
                  pltpu.VMEM((n, 2, t, wide), f32),
                  pltpu.VMEM((n, LINE, cap, wide), i16),
                  pltpu.VMEM((LINE * cap, 3 * t), bf16),
                  pltpu.VMEM((t, hd), bf16))


def layer(x, ids, gates, w1, w3, w2, cap):
    t, hd = x.shape
    ff = w1.shape[1]
    groups = column_groups(hd, 128)
    wide = max(w for _, w in groups)
    n = len(groups)
    dma = pltpu.SemaphoreType.DMA
    anywhere = pl.BlockSpec(memory_space=pl.ANY)
    y, _, _ = pl.pallas_call(
        functools.partial(layer_kernel, t, cap, groups),
        out_shape=(jax.ShapeDtypeStruct((t, hd), bf16),
                   jax.ShapeDtypeStruct((RING, RING, RING, CORES, cap, hd), bf16),
                   jax.ShapeDtypeStruct((n, RING, RING, LINE, cap, wide), i16)),
        in_specs=[anywhere] * 6,
        out_specs=(pl.BlockSpec(memory_space=pltpu.VMEM), anywhere, anywhere),
        scratch_shapes=[
            pltpu.VMEM((hd, ff), bf16), pltpu.VMEM((hd, ff), bf16), pltpu.VMEM((ff, hd), bf16),
            pltpu.VMEM((IDROWS, t), jnp.int32), pltpu.VMEM((IDROWS, t), f32),
            pltpu.VMEM((3, RING, 2 * IDROWS, t), f32),
            pltpu.VMEM((t, t), bf16),
            pltpu.SemaphoreType.REGULAR,
            dma((2,)), dma((3,)), dma((n,)),
            dma((n, 4 + 4 * RING)), dma((n, 4 + 4 * RING)), dma((n, RING, LINE)), dma((n, RING, LINE)), dma((n, RING)),
            dma((3, RING)), dma((3, RING)), dma,
            dma((2,)), dma((SLOTS, LINE + 4)), dma((n, LINE)), dma((n, LINE)), dma((n, LINE)),
            dma((n, RING, RING)), dma((n, RING, RING)), dma((n, RING)), dma((n, RING)),
            dma((n, 2)), dma((n, 2)), dma((n, 2)), dma((n, 2)), dma((LINE,)), dma((LINE,)),
            dma((RING, RING)), dma((RING, RING)), dma((n,)),
        ],
        compiler_params=pltpu.CompilerParams(collective_id=0, has_side_effects=True, vmem_limit_bytes=67043328),
        name="layer",
    )(ids.T, gates.T, x, w1, w3, w2)
    return y


def solution(mesh):
    nd = mesh.shape["ey"] * mesh.shape["ex"]
    tok = P(("dp", "ey", "ex"), None)
    wsp = P(("ey", "ex"), None, None)

    def local(x, ids, gates, w1, w3, w2):
        t = x.shape[0]
        cap = min(t, CAPF * t * ids.shape[1] // nd)
        return layer(x, ids, gates, w1[0], w3[0], w2[0], cap)

    return jax.shard_map(local, mesh=mesh, in_specs=(tok, tok, tok, wsp, wsp, wsp),
                         out_specs=tok, check_vma=False)
```

```python
import functools

import jax
import jax.numpy as jnp
from jax import lax
from jax.experimental import pallas as pl
from jax.experimental.pallas import tpu as pltpu
from jax.sharding import PartitionSpec as P

CAPF = 2
FULL = 32000.0
RING = 4
CORES = 2
IDROWS = 8
ORDERS = ((0, 1, 2), (2, 0, 1), (1, 2, 0))
LINE = RING * CORES
STRIDES = (RING * RING * CORES, RING * CORES, CORES)
RETURNS = ((2, 1, 0), (1, 0, 2), (0, 2, 1))
TILE = 256
LINES = (2, 1, 3, 0)
WIDE = 512
PIECE = 256
SLOTS = 5
MESH = pl.DeviceIdType.MESH
PEERS = [(axis, by, dc) for axis in range(3) for by in range(1, RING) for dc in range(CORES)] + [(0, 0, 1)]
bf16, i16, f32 = jnp.bfloat16, jnp.int16, jnp.float32


def column_groups(hd, tile):
    tiles = hd // tile
    first = -(-tiles // 3)
    second = -(-(tiles - first) // 2)
    widths = [first * tile, second * tile, (tiles - first - second) * tile]
    starts = [0, widths[0], widths[0] + widths[1]]
    return list(zip(starts, widths))


def dispatch_part(t, cap, groups, x_ref, rx_ref, idv, gatev, upper, info, load_sem, gsend, grecv, rsend, rrecv, self_sem,
                  isend, irecv, weight_loads, got, out, pick):
    ey, ex, dp = lax.axis_index("ey"), lax.axis_index("ex"), lax.axis_index("dp")
    me = [ey // RING, ey % RING, ex // CORES]
    core = ex % CORES
    rows = t + IDROWS
    split = (rows // 2 + 7) // 8 * 8

    def device(coords, c):
        return (dp, coords[0] * RING + coords[1], coords[2] * CORES + c)

    def shifted(axis, by, c=None):
        coords = list(me)
        coords[axis] = (coords[axis] + by) % RING
        return device(coords, core if c is None else c)

    loads = [pltpu.make_async_copy(x_ref.at[:, pl.ds(start, width)], got.at[g, 0, 0, pl.ds(0, t), pl.ds(0, width)],
                                   load_sem.at[g]) for g, (start, width) in enumerate(groups)]
    for load in loads:
        load.start()

    barrier = pltpu.get_barrier_semaphore()
    for axis, by, dc in PEERS:
        pl.semaphore_signal(barrier, inc=1, device_id=shifted(axis, by, (core + dc) % CORES), device_id_type=MESH)
    row = lax.broadcasted_iota(jnp.int32, (t, t), 0)
    col = lax.broadcasted_iota(jnp.int32, (t, t), 1)
    upper[...] = jnp.where(row <= col, 1.0, 0.0).astype(bf16)
    ids = idv[...].astype(f32)
    for g in range(len(groups)):
        got[g, 0, 0, pl.ds(t, IDROWS), pl.ds(0, t)] = ids.astype(bf16)
    for axis in range(3):
        info[axis, me[axis], 0:8, :] = ids
        info[axis, me[axis], 8:16, :] = gatev[...]
    pl.semaphore_wait(barrier, len(PEERS))
    for load in loads:
        load.wait()

    def hop(g, index, block, to, axis, by, part=None):
        width = groups[g][1]
        at = pl.ds(0, rows) if part is None else part
        copy = pltpu.make_async_remote_copy(
            src_ref=got.at[g, block[0], block[1], at, pl.ds(0, width)],
            dst_ref=got.at[g, to[0], to[1], at, pl.ds(0, width)],
            send_sem=gsend.at[g, index], recv_sem=grecv.at[g, index],
            device_id=shifted(axis, by), device_id_type=MESH)
        copy.start()
        hops[g, index] = copy

    hops = {}
    low, high = pl.ds(0, split), pl.ds(split, rows - split)

    def first(g):
        p = ORDERS[g][0]
        hop(g, 0, (0, 0), (3, 0), p, 1)
        hop(g, 1, (0, 0), (1, 0), p, 3)

    def second(g, i):
        q = ORDERS[g][1]
        hop(g, 4 + 4 * i, (i, 0), (i, 3), q, 1)
        hop(g, 5 + 4 * i, (i, 0), (i, 1), q, 3)

    def second_on(g, i):
        q = ORDERS[g][1]
        hops[g, 4 + 4 * i].wait_recv()
        hop(g, 6 + 4 * i, (i, 3), (i, 2), q, 1, low)
        hops[g, 5 + 4 * i].wait_recv()
        hop(g, 7 + 4 * i, (i, 1), (i, 2), q, 3, high)

    everyone = range(len(groups))
    for g in everyone:
        first(g)
        second(g, 0)
    for load in weight_loads:
        load.start()
    told = []
    for axis in range(3):
        for by in range(1, RING):
            told.append(pltpu.make_async_remote_copy(
                src_ref=info.at[axis, me[axis]], dst_ref=info.at[axis, me[axis]], send_sem=isend.at[axis, by],
                recv_sem=irecv.at[axis, by], device_id=shifted(axis, by), device_id_type=MESH))
            told[-1].start()

    for g in everyone:
        p = ORDERS[g][0]
        hops[g, 0].wait_recv()
        hop(g, 2, (3, 0), (2, 0), p, 1, low)
        second(g, 3)
        hops[g, 1].wait_recv()
        hop(g, 3, (1, 0), (2, 0), p, 3, high)
        second(g, 1)
    for g in everyone:
        second_on(g, 0)
    for g in everyone:
        hops[g, 2].wait_recv()
        hops[g, 3].wait_recv()
        second(g, 2)

    def choose(g, j):
        p, _, r = ORDERS[g]
        width = groups[g][1]
        stride = (RING * RING * CORES, RING * CORES, CORES)[r]
        base = ey * (RING * CORES) + ex - core - me[r] * stride

        def one(i, _):
            ids = got[g, i, j, pl.ds(t, IDROWS), pl.ds(0, t)].astype(f32)
            lines = []
            for k in range(RING * CORES):
                expert = (base + (k // CORES) * stride + k % CORES).astype(f32)
                lines.append(jnp.sum(jnp.where(ids == expert, 1.0, 0.0), axis=0, keepdims=True))
            hit = jnp.concatenate(lines, axis=0)
            rank = jnp.dot(hit.astype(bf16), upper[...], preferred_element_type=f32)
            slot = jnp.where((hit > 0.5) & (rank < cap + 0.5), rank - 1.0, -1.0)
            wanted = lax.broadcasted_iota(jnp.int32, (cap, t), 0).astype(f32)
            for k in range(RING * CORES):
                pick[pl.ds(k * cap, cap), :] = jnp.where(slot[k:k + 1, :] == wanted, 1.0, 0.0).astype(bf16)
            place = (me[p] + i) % RING

            def tile(n, _):
                at = pl.ds(pl.multiple_of(n * 128, 128), 128)
                val = jnp.dot(pick[...], got[g, i, j, pl.ds(0, t), at], preferred_element_type=f32).astype(bf16)
                for k in range(RING * CORES):
                    out[g, j, k, place, :, at] = val[k * cap:(k + 1) * cap]
                return 0

            return lax.fori_loop(0, width // 128, tile, 0)

        lax.fori_loop(0, RING, one, 0)

    def place_in(ref, g, j):
        start, width = groups[g]
        p, q, r = ORDERS[g]
        at = [None, None, None]
        at[p] = slice(None)
        at[q] = (me[q] + j) % RING
        at[r] = me[r]
        return ref.at[at[0], at[1], at[2], core, :, pl.ds(start, width)]

    sends, keeps = [], []

    def exchange(g, j):
        _, _, r = ORDERS[g]
        width = groups[g][1]
        for dr in range(RING):
            for dc in range(CORES):
                to, c = (me[r] + dr) % RING, (core + dc) % CORES
                src = out.at[g, j, to * CORES + c, :, :, pl.ds(0, width)]
                if dr == 0 and dc == 0:
                    copy = pltpu.make_async_copy(src, place_in(rx_ref, g, j), self_sem.at[g, j])
                    keeps.append(copy)
                else:
                    n = dr * CORES + dc
                    copy = pltpu.make_async_remote_copy(
                        src_ref=src, dst_ref=place_in(rx_ref, g, j),
                        send_sem=rsend.at[g, j, n], recv_sem=rrecv.at[g, j, n],
                        device_id=shifted(r, dr, c), device_id_type=MESH)
                    sends.append(copy)
                copy.start()

    for g in everyone:
        choose(g, 0)
        exchange(g, 0)
    for i in (3, 1):
        for g in everyone:
            second_on(g, i)
    for g in everyone:
        second_on(g, 2)
    for j in (3, 1):
        for g in everyone:
            choose(g, j)
            exchange(g, j)
    for g in everyone:
        for i in range(RING):
            hops[g, 6 + 4 * i].wait_recv()
            hops[g, 7 + 4 * i].wait_recv()
        choose(g, 2)
        exchange(g, 2)

    for copy in sends:
        copy.wait_recv()
    for copy in keeps:
        copy.wait()
    for copy in hops.values():
        copy.wait_send()
    for copy in sends + told:
        copy.wait_send()
    for copy in told:
        copy.wait_recv()


def experts_part(t, cap, groups, x_ref, rx_ref, y_ref, r2, w1, w3, w2, info, upper, ready, weight_loads, xload_sem, sems,
                 xb, hh, res, top, ob, rest, so, r1, s1, s2, acc, part, planes, db, wt, xv):
    xsem, p1s, p1r, q1s, q1r, p2s, p2r, q2s, q2r, p3s, p3r, hs, hr, e1s, e1r, e2s, e2r, dsem = sems
    ey, ex, dp = lax.axis_index("ey"), lax.axis_index("ex"), lax.axis_index("dp")
    me = [ey // RING, ey % RING, ex // CORES]
    core = ex % CORES
    rows = LINE * cap
    hd, ff = w1.shape
    everyone = range(len(groups))
    col0 = [start for start, _ in groups]
    width = [w for _, w in groups]
    main = min(width)
    more = width[0] - main
    own = [me[RETURNS[g][0]] * CORES + core for g in everyone]

    def shifted(axis, by, c=None):
        coords = list(me)
        coords[axis] = (coords[axis] + by) % RING
        return (dp, coords[0] * RING + coords[1], coords[2] * CORES + (core if c is None else c))

    def remote(src, dst, send, recv, to):
        return pltpu.make_async_remote_copy(src_ref=src, dst_ref=dst, send_sem=send, recv_sem=recv,
                                            device_id=to, device_id_type=MESH)

    def homes(step):
        left = RING * RING - 1 - step
        return (left + left // RING) % RING, left % RING

    def tile_load(step):
        dz, dy = homes(step)
        return pltpu.make_async_copy(rx_ref.at[(me[0] + dz) % RING, (me[1] + dy) % RING], xb.at[step % 2], xsem.at[step % 2])

    tile_load(0).start()

    for axis, by, dc in PEERS:
        pl.semaphore_signal(ready, inc=1, device_id=shifted(axis, by, (core + dc) % CORES), device_id_type=MESH)
    xload = pltpu.make_async_copy(x_ref, xv, xload_sem)
    xload.start()
    for load in weight_loads:
        load.wait()

    def first(step):
        dz, dy = homes(step)
        zh, yh = (me[0] + dz) % RING, (me[1] + dy) % RING
        slot = step % SLOTS
        found = []
        for n in range(1, LINE):
            d, dc = n // CORES, n % CORES
            c = (core + dc) % CORES
            found.append((None, remote(
                ob.at[slot, (me[2] + d) % RING, c, :, pl.ds(col0[0], main)],
                r1.at[0, own[0], zh, yh, :, pl.ds(0, main)],
                p1s.at[slot, n], p1r.at[0, n], shifted(2, d, c))))
        for g, axis, d, lead in ((1, 1, dy, zh), (2, 0, dz, yh)):
            for dc in range(CORES):
                c = (core + dc) % CORES
                found.append((None if dc else d != 0, remote(
                    ob.at[slot, :, c, :, pl.ds(col0[g], width[g])],
                    r1.at[g, own[g], lead, :, :, pl.ds(0, width[g])],
                    p1s.at[slot, LINE + 2 * (g - 1) + dc], p1r.at[g, d * CORES + dc], shifted(axis, d, c))))
        return found

    def each(found, act):
        for whether, copy in found:
            if whether is None:
                act(copy)
            else:
                @pl.when(whether)
                def _():
                    act(copy)

    eye = lax.broadcasted_iota(jnp.int32, (cap, 128), 0) == lax.broadcasted_iota(jnp.int32, (cap, 128), 1)

    def code(step, begin, end):
        slot = step % SLOTS
        for n in range(begin, end):
            at = pl.ds(n * 128, 128)
            v = jnp.round(res[:, at] * top[...]).astype(jnp.int32).astype(i16)
            ob[slot, :, :, :, at] = v.reshape(RING, CORES, cap, 128)

    def room(step):
        @pl.when(step >= SLOTS)
        def _():
            each(first(step - SLOTS), lambda copy: copy.wait_send())

    def leave(step):
        each(first(step), lambda copy: copy.start())
        dz, dy = homes(step)
        zh, yh = (me[0] + dz) % RING, (me[1] + dy) % RING
        slot = step % SLOTS
        r1[0, own[0], zh, yh, :, pl.ds(0, width[0])] = ob[slot, me[2], core, :, pl.ds(col0[0], width[0])]
        if more:
            rest[zh, yh] = ob[slot, :, :, :, pl.ds(col0[0] + main, more)]
        for g, d, lead in ((1, dy, zh), (2, dz, yh)):
            @pl.when(d == 0)
            def _():
                for xh in range(RING):
                    r1[g, own[g], lead, xh, :, pl.ds(0, width[g])] = ob[slot, xh, core, :, pl.ds(col0[g], width[g])]

    def tile(step, _):
        dz, dy = homes(step)
        zh, yh = (me[0] + dz) % RING, (me[1] + dy) % RING

        @pl.when(step + 1 < RING * RING)
        def _():
            tile_load(step + 1).start()

        room(step - 1)
        tile_load(step).wait()
        ups, codes = ff // TILE, hd // 128
        for n in range(ups):
            at = pl.ds(n * TILE, TILE)
            xt = xb[step % 2].reshape(rows, hd)
            a1 = jnp.dot(xt, w1[:, at], preferred_element_type=f32)
            a3 = jnp.dot(xt, w3[:, at], preferred_element_type=f32)
            hh[:, at] = (a1 * (1.0 / (1.0 + jnp.exp(-a1))) * a3).astype(bf16)
            code(step - 1, codes * n // ups, codes * (n + 1) // ups)

        @pl.when(step == 1)
        def _():
            pl.semaphore_wait(ready, len(PEERS))

        @pl.when(step > 0)
        def _():
            leave(step - 1)

        most = jnp.zeros((rows, 128), f32)
        for n in range(hd // WIDE):
            o = jnp.dot(hh[...], w2[:, n * WIDE:(n + 1) * WIDE], preferred_element_type=f32)
            res[:, n * WIDE:(n + 1) * WIDE] = o
            o = jnp.abs(o)
            for k in range(WIDE // 128):
                most = jnp.maximum(most, o[:, k * 128:(k + 1) * 128])
        peak = jnp.maximum(jnp.max(most, axis=1, keepdims=True), 1e-30)
        top[...] = jnp.broadcast_to(FULL / peak, top.shape)
        for k in range(LINE):
            part = jnp.where(eye, peak[k * cap:(k + 1) * cap], 0.0)
            so[zh, yh, k // CORES, k % CORES] = jnp.sum(part, axis=0, keepdims=True) * (1.0 / FULL)
        return 0

    steps = RING * RING
    lax.fori_loop(0, steps, tile, 0)
    room(steps - 1)
    code(steps - 1, 0, hd // 128)
    leave(steps - 1)

    def scales(g, coord, c):
        return (so.at[:, :, coord, c], so.at[:, coord, :, c], so.at[coord, :, :, c])[g]

    hints = []
    for g in everyone:
        axis = RETURNS[g][0]
        s1[g, own[g]] = (so[:, :, me[2], core], so[:, me[1], :, core], so[me[0], :, :, core])[g]
        for n in range(1, LINE):
            d, dc = n // CORES, n % CORES
            c = (core + dc) % CORES
            hints.append(remote(scales(g, (me[axis] + d) % RING, c), s1.at[g, own[g]],
                                q1s.at[g, n], q1r.at[g, n], shifted(axis, d, c)))
            hints[-1].start()

    later = []
    if more:
        for n in range(1, LINE):
            d, dc = n // CORES, n % CORES
            c = (core + dc) % CORES
            later.append(remote(rest.at[:, :, (me[2] + d) % RING, c], r1.at[0, own[0], :, :, :, pl.ds(main, more)],
                                e1s.at[n], e1r.at[n], shifted(2, d, c)))
            later[-1].start()

    def lane(ref, g, h2, h3):
        return (ref.at[0, :, h3, h2], ref.at[1, :, h2, h3], ref.at[2, :, h3, h2])[g]

    def second(g, k3, d):
        _, axis, third = RETURNS[g]
        h3 = (me[third] + k3) % RING
        at = pl.ds(0, main)
        src = (r1.at[0, :, h3, (me[axis] + d) % RING, :, at] if g == 0 else
               r1.at[1, :, (me[axis] + d) % RING, h3, :, at] if g == 1 else
               r1.at[2, :, h3, (me[axis] + d) % RING, :, at])
        return remote(src, r2.at[g, h3, me[axis], :, :, at], p2s.at[g, k3, d], p2r.at[g, k3, d], shifted(axis, d))

    def second_more(k3, d):
        _, axis, third = RETURNS[0]
        h3 = (me[third] + k3) % RING
        at = pl.ds(main, more)
        return remote(r1.at[0, :, h3, (me[axis] + d) % RING, :, at], r2.at[0, h3, me[axis], :, :, at],
                      e2s.at[k3, d], e2r.at[k3, d], shifted(axis, d))

    for g in everyone:
        axis = RETURNS[g][0]
        for n in range(1, LINE):
            d, dc = n // CORES, n % CORES
            src = (me[axis] - d) % RING * CORES + (core + dc) % CORES
            ref = r1.at[g, src, :, :, :, pl.ds(0, main)]
            pltpu.make_async_copy(ref, ref, p1r.at[g, n]).wait()
        for d in (1, 3, 2):
            second(g, LINES[0], d).start()

    for copy in hints:
        copy.wait_recv()
    moved = []
    for g in everyone:
        axis = RETURNS[g][1]
        s2[g, me[axis]] = (s1[0, :, :, me[1]], s1[1, :, me[0]], s1[2, :, :, me[2]])[g]
        for d in (1, 3, 2):
            moved.append(remote(lane(s1, g, (me[axis] + d) % RING, slice(None)), s2.at[g, me[axis]],
                                q2s.at[g, d], q2r.at[g, d], shifted(axis, d)))
            moved[-1].start()

    for copy in later:
        copy.wait_recv()
    def rest_of(k3):
        for d in (1, 3, 2):
            if more:
                second_more(k3, d).start()
            for g in everyone:
                if k3 != LINES[0]:
                    second(g, k3, d).start()

    for k3 in LINES[:-1]:
        rest_of(k3)

    for copy in moved:
        copy.wait_recv()

    wanted = lax.broadcasted_iota(jnp.int32, (cap, t), 0).astype(f32)

    def weights(g, h3, src):
        first_axis, axis, third = RETURNS[g]
        base = src * STRIDES[axis] + me[third] * STRIDES[third]
        found = {}

        def begin():
            ids = info[third, h3, 0:8, :]
            gates = info[third, h3, 8:16, :]
            hits, gate = [], []
            for k in range(LINE):
                same = ids == (base + (k // CORES) * STRIDES[first_axis] + k % CORES).astype(f32)
                hits.append(jnp.sum(jnp.where(same, 1.0, 0.0), axis=0, keepdims=True))
                gate.append(jnp.sum(jnp.where(same, gates, 0.0), axis=0, keepdims=True))
            hit = jnp.concatenate(hits, axis=0)
            rank = jnp.dot(hit.astype(bf16), upper[...], preferred_element_type=f32)
            found["slot"] = jnp.where((hit > 0.5) & (rank < cap + 0.5), rank - 1.0, -1.0)
            found["gate"] = gate

        def expert(k):
            scale = jnp.sum(jnp.where(eye, s2[g, src, k, h3], 0.0), axis=1, keepdims=True)
            w = jnp.where(found["slot"][k:k + 1, :] == wanted, found["gate"][k], 0.0) * scale
            for p in range(3):
                a = w.astype(bf16)
                wt[g, pl.ds(p * rows + k * cap, cap), :] = a
                w = w - a.astype(f32)

        return [begin] + [functools.partial(expert, k) for k in range(LINE)]

    def line(index, _):
        k3 = 2 - index + 3 * (index // 2) - 2 * (index // 3)

        def plane(turn, _):
            d = turn + turn // 2 - 2 * (turn // 3)

            def fetch(g):
                third = RETURNS[g][2]
                src = (me[RETURNS[g][1]] - d) % RING
                return pltpu.make_async_copy(r2.at[g, (me[third] + k3) % RING, src, :, :, pl.ds(0, width[g])],
                                             db.at[g, :, :, pl.ds(0, width[g])], dsem.at[g])

            for g in everyone:
                _, axis, third = RETURNS[g]
                h3 = (me[third] + k3) % RING

                @pl.when(turn == 0)
                def _():
                    at = pl.ds(0, width[g])
                    if g == 1:
                        db[g, :, :, at] = r1[g, :, me[axis], h3, :, at]
                    else:
                        db[g, :, :, at] = r1[g, :, h3, me[axis], :, at]
                    acc[g, index] = jnp.zeros(acc.shape[2:], f32)

                @pl.when(turn > 0)
                def _():
                    second(g, k3, d).wait_recv()
                    if more and g == 0:
                        second_more(k3, d).wait_recv()
                    fetch(g).start()

            @pl.when(turn > 0)
            def _():
                for g in everyone:
                    fetch(g).wait()

            def piece(g, begin, size):
                at = pl.ds(begin, size)
                q = db[g, :, :, at].reshape(rows, size).astype(f32)
                high = q.astype(bf16)
                low = (q - high.astype(f32)).astype(bf16)
                dims = (((0,), (0,)), ((), ()))
                p = (lax.dot_general(wt[g], jnp.concatenate([high] * 3, axis=0), dims, preferred_element_type=f32)
                     + lax.dot_general(wt[g], jnp.concatenate([low] * 3, axis=0), dims, preferred_element_type=f32))
                acc[g, index, :, at] += p

            def steps_of(g):
                _, axis, third = RETURNS[g]
                return weights(g, (me[third] + k3) % RING, (me[axis] - d) % RING)

            for act in steps_of(0):
                act()
            for g in everyone:
                products = [functools.partial(piece, g, begin, min(PIECE, width[g] - begin))
                            for begin in range(0, width[g], PIECE)]
                others = steps_of(g + 1) if g + 1 < len(groups) else []
                for k, act in enumerate(products):
                    act()
                    for other in others[len(others) * k // len(products):len(others) * (k + 1) // len(products)]:
                        other()

            for g in everyone:
                @pl.when((turn == RING - 1) & (index == 0))
                def _():
                    for way in range(2):
                        opposite(g, way).start()

                @pl.when((turn == RING - 1) & (index == 2))
                def _():
                    for way in range(2):
                        opposite(g, way).wait_recv()
                        rows_of = pl.ds(way * (t // 2), t // 2)
                        at = pl.ds(0, width[g])
                        acc[g, 1 + way, rows_of, at] += part[g, way, :, at]
                    for way in range(2):
                        home(g, way).start()
            return 0

        lax.fori_loop(0, RING, plane, 0)

        @pl.when(index == 0)
        def _():
            rest_of(LINES[-1])
        return 0

    def opposite(g, way):
        at = pl.ds(0, width[g])
        return remote(acc.at[g, 0, pl.ds(way * (t // 2), t // 2), at], part.at[g, way, :, at],
                      hs.at[g, way], hr.at[g, way], shifted(RETURNS[g][2], LINES[1 + way]))

    def home(g, way):
        at = pl.ds(0, width[g])
        return remote(acc.at[g, 1 + way, :, at], planes.at[g, way, :, at],
                      p3s.at[g, way], p3r.at[g, way], shifted(RETURNS[g][2], LINES[1 + way]))

    lax.fori_loop(0, RING, line, 0)

    xload.wait()
    for g in reversed(everyone):
        for way in range(2):
            home(g, way).wait_recv()

        def finish(n, _):
            at = pl.ds(pl.multiple_of(n * 128, 128), 128)
            to = pl.ds(pl.multiple_of(col0[g] + n * 128, 128), 128)
            total = acc[g, RING - 1, :, at] + planes[g, 0, :, at] + planes[g, 1, :, at]
            y_ref[:, to] = (xv[:, to].astype(f32) + total).astype(bf16)
            return 0

        lax.fori_loop(0, width[g] // 128, finish, 0)

    for copy in hints + moved + later:
        copy.wait_send()

    def last(step, _):
        each(first(step), lambda copy: copy.wait_send())
        return 0

    lax.fori_loop(RING * RING - SLOTS, RING * RING, last, 0)
    for g in everyone:
        for k3 in range(RING):
            for d in (1, 3, 2):
                second(g, k3, d).wait_send()
                if more and g == 0:
                    second_more(k3, d).wait_send()
        for way in range(2):
            opposite(g, way).wait_send()
            home(g, way).wait_send()


def layer_kernel(t, cap, groups, ids_ref, gates_ref, x_ref, w1_ref, w3_ref, w2_ref, y_ref, rx_ref, r2,
                 w1, w3, w2, idv, gatev, info, upper, ready, small_sem, wsem, load_sem, gsend, grecv, rsend, rrecv, self_sem,
                 isend, irecv, xload_sem, *sems):
    hd, ff = w1.shape
    n = len(groups)
    wide = max(w for _, w in groups)
    more = max(wide - min(w for _, w in groups), 128)
    small = [pltpu.make_async_copy(a, b, small_sem.at[k]) for k, (a, b) in enumerate(((ids_ref, idv), (gates_ref, gatev)))]
    weight_loads = [pltpu.make_async_copy(a, b, wsem.at[k])
                    for k, (a, b) in enumerate(((w1_ref, w1), (w3_ref, w3), (w2_ref, w2)))]
    for load in small:
        load.start()
    for load in small:
        load.wait()

    def there(got, out, pick):
        dispatch_part(t, cap, groups, x_ref, rx_ref, idv, gatev, upper, info, load_sem, gsend, grecv, rsend, rrecv, self_sem,
                      isend, irecv, weight_loads, got, out, pick)

    pl.run_scoped(there,
                  pltpu.VMEM((n, RING, RING, t + IDROWS, wide), bf16),
                  pltpu.VMEM((n, RING, LINE, RING, cap, wide), bf16),
                  pltpu.VMEM((LINE * cap, t), bf16))

    def back(*scratch):
        experts_part(t, cap, groups, x_ref, rx_ref, y_ref, r2, w1, w3, w2, info, upper, ready, weight_loads, xload_sem, sems,
                     *scratch)

    pl.run_scoped(back,
                  pltpu.VMEM((2, RING, CORES, cap, hd), bf16),
                  pltpu.VMEM((LINE * cap, ff), bf16),
                  pltpu.VMEM((LINE * cap, hd), f32),
                  pltpu.VMEM((LINE * cap, 128), f32),
                  pltpu.VMEM((SLOTS, RING, CORES, cap, hd), i16),
                  pltpu.VMEM((RING, RING, RING, CORES, cap, more), i16),
                  pltpu.VMEM((RING, RING, RING, CORES, 1, 128), f32),
                  pltpu.VMEM((n, LINE, RING, RING, cap, wide), i16),
                  pltpu.VMEM((n, LINE, RING, RING, 1, 128), f32),
                  pltpu.VMEM((n, RING, LINE, RING, 1, 128), f32),
                  pltpu.VMEM((n, RING, t, wide), f32),
                  pltpu.VMEM((n, 2, t // 2, wide), f32),
                  pltpu.VMEM((n, 2, t, wide), f32),
                  pltpu.VMEM((n, LINE, cap, wide), i16),
                  pltpu.VMEM((n, 3 * LINE * cap, t), bf16),
                  pltpu.VMEM((t, hd), bf16))


def layer(x, ids, gates, w1, w3, w2, cap):
    t, hd = x.shape
    ff = w1.shape[1]
    groups = column_groups(hd, 128)
    wide = max(w for _, w in groups)
    n = len(groups)
    dma = pltpu.SemaphoreType.DMA
    anywhere = pl.BlockSpec(memory_space=pl.ANY)
    y, _, _ = pl.pallas_call(
        functools.partial(layer_kernel, t, cap, groups),
        out_shape=(jax.ShapeDtypeStruct((t, hd), bf16),
                   jax.ShapeDtypeStruct((RING, RING, RING, CORES, cap, hd), bf16),
                   jax.ShapeDtypeStruct((n, RING, RING, LINE, cap, wide), i16)),
        in_specs=[anywhere] * 6,
        out_specs=(pl.BlockSpec(memory_space=pltpu.VMEM), anywhere, anywhere),
        scratch_shapes=[
            pltpu.VMEM((hd, ff), bf16), pltpu.VMEM((hd, ff), bf16), pltpu.VMEM((ff, hd), bf16),
            pltpu.VMEM((IDROWS, t), jnp.int32), pltpu.VMEM((IDROWS, t), f32),
            pltpu.VMEM((3, RING, 2 * IDROWS, t), f32),
            pltpu.VMEM((t, t), bf16),
            pltpu.SemaphoreType.REGULAR,
            dma((2,)), dma((3,)), dma((n,)),
            dma((n, 4 + 4 * RING)), dma((n, 4 + 4 * RING)), dma((n, RING, LINE)), dma((n, RING, LINE)), dma((n, RING)),
            dma((3, RING)), dma((3, RING)), dma,
            dma((2,)), dma((SLOTS, LINE + 4)), dma((n, LINE)), dma((n, LINE)), dma((n, LINE)),
            dma((n, RING, RING)), dma((n, RING, RING)), dma((n, RING)), dma((n, RING)),
            dma((n, 2)), dma((n, 2)), dma((n, 2)), dma((n, 2)), dma((LINE,)), dma((LINE,)),
            dma((RING, RING)), dma((RING, RING)), dma((n,)),
        ],
        compiler_params=pltpu.CompilerParams(collective_id=0, has_side_effects=True, vmem_limit_bytes=67043328),
        name="layer",
    )(ids.T, gates.T, x, w1, w3, w2)
    return y


def solution(mesh):
    nd = mesh.shape["ey"] * mesh.shape["ex"]
    tok = P(("dp", "ey", "ex"), None)
    wsp = P(("ey", "ex"), None, None)

    def local(x, ids, gates, w1, w3, w2):
        t = x.shape[0]
        cap = min(t, CAPF * t * ids.shape[1] // nd)
        return layer(x, ids, gates, w1[0], w3[0], w2[0], cap)

    return jax.shard_map(local, mesh=mesh, in_specs=(tok, tok, tok, wsp, wsp, wsp),
                         out_specs=tok, check_vma=False)
```

```python
import functools

import jax
import jax.numpy as jnp
from jax import lax
from jax.experimental import pallas as pl
from jax.experimental.pallas import tpu as pltpu
from jax.sharding import PartitionSpec as P

CAPF = 2
FULL = 32000.0
RING = 4
CORES = 2
IDROWS = 8
ORDERS = ((0, 1, 2), (2, 0, 1), (1, 2, 0))
LINE = RING * CORES
STRIDES = (RING * RING * CORES, RING * CORES, CORES)
RETURNS = ((2, 1, 0), (1, 0, 2), (0, 2, 1))
TILE = 256
LINES = (2, 1, 3, 0)
WIDE = 512
PIECE = 256
SLOTS = 5
MESH = pl.DeviceIdType.MESH
PEERS = [(axis, by, dc) for axis in range(3) for by in range(1, RING) for dc in range(CORES)] + [(0, 0, 1)]
bf16, i16, f32 = jnp.bfloat16, jnp.int16, jnp.float32


def column_groups(hd, tile):
    tiles = hd // tile
    first = -(-tiles // 3)
    second = -(-(tiles - first) // 2)
    widths = [first * tile, second * tile, (tiles - first - second) * tile]
    starts = [0, widths[0], widths[0] + widths[1]]
    return list(zip(starts, widths))


EARLY = 2


def homes(step):
    turn, k = step // RING, step % RING
    dy = (1 + 2 * k - 3 * (k // 2)) % RING
    return (dy + 2 - turn + 3 * (turn // 2) - 2 * (turn // 3)) % RING, dy


def tile_load(step, me, rx_ref, xb, xsem):
    dz, dy = homes(step)
    return pltpu.make_async_copy(rx_ref.at[(me[0] + dz) % RING, (me[1] + dy) % RING], xb.at[step % 2], xsem.at[step % 2])


def diagonal(cap):
    return lax.broadcasted_iota(jnp.int32, (cap, 128), 0) == lax.broadcasted_iota(jnp.int32, (cap, 128), 1)


def code(step, begin, end, res, top, ob):
    slot = step % SLOTS
    cap = ob.shape[3]
    for n in range(begin, end):
        at = pl.ds(n * 128, 128)
        v = jnp.round(res[:, at] * top[...]).astype(jnp.int32).astype(i16)
        ob[slot, :, :, :, at] = v.reshape(RING, CORES, cap, 128)


def up(step, w1, w3, xb, hh, res, top, ob):
    hd, ff = w1.shape
    rows = hh.shape[0]
    ups, codes = ff // TILE, hd // 128
    for n in range(ups):
        at = pl.ds(n * TILE, TILE)
        xt = xb[step % 2].reshape(rows, hd)
        a1 = jnp.dot(xt, w1[:, at], preferred_element_type=f32)
        a3 = jnp.dot(xt, w3[:, at], preferred_element_type=f32)
        hh[:, at] = (a1 * (1.0 / (1.0 + jnp.exp(-a1))) * a3).astype(bf16)
        code(step - 1, codes * n // ups, codes * (n + 1) // ups, res, top, ob)


def down(step, me, w2, hh, res, top, so):
    ff, hd = w2.shape
    rows = hh.shape[0]
    cap = rows // LINE
    dz, dy = homes(step)
    zh, yh = (me[0] + dz) % RING, (me[1] + dy) % RING
    most = jnp.zeros((rows, 128), f32)
    for n in range(hd // WIDE):
        o = jnp.dot(hh[...], w2[:, n * WIDE:(n + 1) * WIDE], preferred_element_type=f32)
        res[:, n * WIDE:(n + 1) * WIDE] = o
        o = jnp.abs(o)
        for k in range(WIDE // 128):
            most = jnp.maximum(most, o[:, k * 128:(k + 1) * 128])
    peak = jnp.maximum(jnp.max(most, axis=1, keepdims=True), 1e-30)
    top[...] = jnp.broadcast_to(FULL / peak, top.shape)
    for k in range(LINE):
        part = jnp.where(diagonal(cap), peak[k * cap:(k + 1) * cap], 0.0)
        so[zh, yh, k // CORES, k % CORES] = jnp.sum(part, axis=0, keepdims=True) * (1.0 / FULL)


def dispatch_part(t, cap, groups, x_ref, rx_ref, idv, gatev, upper, info, load_sem, gsend, grecv, rsend, rrecv, self_sem,
                  isend, irecv, weight_loads, xsem, w1, w3, w2, xb, hh, res, top, ob, so, got, out, pick):
    ey, ex, dp = lax.axis_index("ey"), lax.axis_index("ex"), lax.axis_index("dp")
    me = [ey // RING, ey % RING, ex // CORES]
    core = ex % CORES
    rows = t + IDROWS
    split = (rows // 2 + 7) // 8 * 8

    def device(coords, c):
        return (dp, coords[0] * RING + coords[1], coords[2] * CORES + c)

    def shifted(axis, by, c=None):
        coords = list(me)
        coords[axis] = (coords[axis] + by) % RING
        return device(coords, core if c is None else c)

    loads = [pltpu.make_async_copy(x_ref.at[:, pl.ds(start, width)], got.at[g, 0, 0, pl.ds(0, t), pl.ds(0, width)],
                                   load_sem.at[g]) for g, (start, width) in enumerate(groups)]
    for load in loads:
        load.start()

    barrier = pltpu.get_barrier_semaphore()
    for axis, by, dc in PEERS:
        pl.semaphore_signal(barrier, inc=1, device_id=shifted(axis, by, (core + dc) % CORES), device_id_type=MESH)
    row = lax.broadcasted_iota(jnp.int32, (t, t), 0)
    col = lax.broadcasted_iota(jnp.int32, (t, t), 1)
    upper[...] = jnp.where(row <= col, 1.0, 0.0).astype(bf16)
    ids = idv[...].astype(f32)
    for g in range(len(groups)):
        got[g, 0, 0, pl.ds(t, IDROWS), pl.ds(0, t)] = ids.astype(bf16)
    for axis in range(3):
        info[axis, me[axis], 0:8, :] = ids
        info[axis, me[axis], 8:16, :] = gatev[...]
    pl.semaphore_wait(barrier, len(PEERS))
    for load in loads:
        load.wait()

    def hop(g, index, block, to, axis, by, part=None):
        width = groups[g][1]
        at = pl.ds(0, rows) if part is None else part
        copy = pltpu.make_async_remote_copy(
            src_ref=got.at[g, block[0], block[1], at, pl.ds(0, width)],
            dst_ref=got.at[g, to[0], to[1], at, pl.ds(0, width)],
            send_sem=gsend.at[g, index], recv_sem=grecv.at[g, index],
            device_id=shifted(axis, by), device_id_type=MESH)
        copy.start()
        hops[g, index] = copy

    hops = {}
    low, high = pl.ds(0, split), pl.ds(split, rows - split)

    def first(g):
        p = ORDERS[g][0]
        hop(g, 0, (0, 0), (3, 0), p, 1)
        hop(g, 1, (0, 0), (1, 0), p, 3)

    def second(g, i):
        q = ORDERS[g][1]
        hop(g, 4 + 4 * i, (i, 0), (i, 3), q, 1)
        hop(g, 5 + 4 * i, (i, 0), (i, 1), q, 3)

    def second_on(g, i):
        q = ORDERS[g][1]
        hops[g, 4 + 4 * i].wait_recv()
        hop(g, 6 + 4 * i, (i, 3), (i, 2), q, 1, low)
        hops[g, 5 + 4 * i].wait_recv()
        hop(g, 7 + 4 * i, (i, 1), (i, 2), q, 3, high)

    everyone = range(len(groups))
    for g in everyone:
        first(g)
        second(g, 0)
    for load in weight_loads:
        load.start()
    told = []
    for axis in range(3):
        for by in range(1, RING):
            told.append(pltpu.make_async_remote_copy(
                src_ref=info.at[axis, me[axis]], dst_ref=info.at[axis, me[axis]], send_sem=isend.at[axis, by],
                recv_sem=irecv.at[axis, by], device_id=shifted(axis, by), device_id_type=MESH))
            told[-1].start()

    for g in everyone:
        p = ORDERS[g][0]
        hops[g, 0].wait_recv()
        hop(g, 2, (3, 0), (2, 0), p, 1, low)
        second(g, 3)
        hops[g, 1].wait_recv()
        hop(g, 3, (1, 0), (2, 0), p, 3, high)
        second(g, 1)
    for g in everyone:
        second_on(g, 0)
    for g in everyone:
        hops[g, 2].wait_recv()
        hops[g, 3].wait_recv()
        second(g, 2)

    def choose(g, j):
        p, _, r = ORDERS[g]
        width = groups[g][1]
        stride = (RING * RING * CORES, RING * CORES, CORES)[r]
        base = ey * (RING * CORES) + ex - core - me[r] * stride

        def one(i, _):
            ids = got[g, i, j, pl.ds(t, IDROWS), pl.ds(0, t)].astype(f32)
            lines = []
            for k in range(RING * CORES):
                expert = (base + (k // CORES) * stride + k % CORES).astype(f32)
                lines.append(jnp.sum(jnp.where(ids == expert, 1.0, 0.0), axis=0, keepdims=True))
            hit = jnp.concatenate(lines, axis=0)
            rank = jnp.dot(hit.astype(bf16), upper[...], preferred_element_type=f32)
            slot = jnp.where((hit > 0.5) & (rank < cap + 0.5), rank - 1.0, -1.0)
            wanted = lax.broadcasted_iota(jnp.int32, (cap, t), 0).astype(f32)
            for k in range(RING * CORES):
                pick[pl.ds(k * cap, cap), :] = jnp.where(slot[k:k + 1, :] == wanted, 1.0, 0.0).astype(bf16)
            place = (me[p] + i) % RING

            def tile(n, _):
                at = pl.ds(pl.multiple_of(n * 128, 128), 128)
                val = jnp.dot(pick[...], got[g, i, j, pl.ds(0, t), at], preferred_element_type=f32).astype(bf16)
                for k in range(RING * CORES):
                    out[g, j, k, place, :, at] = val[k * cap:(k + 1) * cap]
                return 0

            return lax.fori_loop(0, width // 128, tile, 0)

        lax.fori_loop(0, RING, one, 0)

    def place_in(ref, g, j):
        start, width = groups[g]
        p, q, r = ORDERS[g]
        at = [None, None, None]
        at[p] = slice(None)
        at[q] = (me[q] + j) % RING
        at[r] = me[r]
        return ref.at[at[0], at[1], at[2], core, :, pl.ds(start, width)]

    sends = {}

    def exchange(g, j):
        _, _, r = ORDERS[g]
        width = groups[g][1]
        for dr in range(RING):
            for dc in range(CORES):
                to, c = (me[r] + dr) % RING, (core + dc) % CORES
                src = out.at[g, j, to * CORES + c, :, :, pl.ds(0, width)]
                if dr == 0 and dc == 0:
                    copy = pltpu.make_async_copy(src, place_in(rx_ref, g, j), self_sem.at[g, j])
                else:
                    n = dr * CORES + dc
                    copy = pltpu.make_async_remote_copy(
                        src_ref=src, dst_ref=place_in(rx_ref, g, j),
                        send_sem=rsend.at[g, j, n], recv_sem=rrecv.at[g, j, n],
                        device_id=shifted(r, dr, c), device_id_type=MESH)
                sends.setdefault((g, j), []).append(copy)
                copy.start()

    for g in everyone:
        choose(g, 0)
        exchange(g, 0)
    for i in (3, 1):
        for g in everyone:
            second_on(g, i)
    for g in everyone:
        second_on(g, 2)
    for j in (3, 1):
        for g in everyone:
            choose(g, j)
            exchange(g, j)
    for g in (2, 0, 1):
        for i in range(RING):
            hops[g, 6 + 4 * i].wait_recv()
            hops[g, 7 + 4 * i].wait_recv()
        choose(g, 2)
        exchange(g, 2)

    def arrived(which):
        for each in which:
            for copy in sends[each][1:]:
                copy.wait_recv()
            sends[each][0].wait()

    last = [(0, 2), (1, 2)]
    arrived([each for each in sends if each not in last])
    for load in weight_loads:
        load.wait()
    tile_load(0, me, rx_ref, xb, xsem).start()

    def tile(step, _):
        @pl.when(step + 1 < EARLY)
        def _():
            tile_load(step + 1, me, rx_ref, xb, xsem).start()

        tile_load(step, me, rx_ref, xb, xsem).wait()
        up(step, w1, w3, xb, hh, res, top, ob)
        down(step, me, w2, hh, res, top, so)
        return 0

    lax.fori_loop(0, EARLY, tile, 0)

    arrived(last)
    for copy in list(hops.values()) + told + [copy for each in sends.values() for copy in each[1:]]:
        copy.wait_send()
    for copy in told:
        copy.wait_recv()


def experts_part(t, cap, groups, x_ref, rx_ref, y_ref, r2, w1, w3, w2, info, upper, ready, ysem, xsem, sems,
                 xb, hh, res, top, ob, so, yv, rest, r1, s1, s2, acc, part, planes, db, wt, xv):
    p1s, p1r, q1s, q1r, p2s, p2r, q2s, q2r, p3s, p3r, hs, hr, e1s, e1r, e2s, e2r, dsem = sems
    ey, ex, dp = lax.axis_index("ey"), lax.axis_index("ex"), lax.axis_index("dp")
    me = [ey // RING, ey % RING, ex // CORES]
    core = ex % CORES
    rows = LINE * cap
    hd, ff = w1.shape
    everyone = range(len(groups))
    col0 = [start for start, _ in groups]
    width = [w for _, w in groups]
    main = min(width)
    more = width[0] - main
    own = [me[RETURNS[g][0]] * CORES + core for g in everyone]

    def shifted(axis, by, c=None):
        coords = list(me)
        coords[axis] = (coords[axis] + by) % RING
        return (dp, coords[0] * RING + coords[1], coords[2] * CORES + (core if c is None else c))

    def remote(src, dst, send, recv, to):
        return pltpu.make_async_remote_copy(src_ref=src, dst_ref=dst, send_sem=send, recv_sem=recv,
                                            device_id=to, device_id_type=MESH)

    for axis, by, dc in PEERS:
        pl.semaphore_signal(ready, inc=1, device_id=shifted(axis, by, (core + dc) % CORES), device_id_type=MESH)
    tile_load(EARLY, me, rx_ref, xb, xsem).start()
    xload = pltpu.make_async_copy(x_ref, xv, ysem.at[len(groups)])
    xload.start()

    def first(step):
        dz, dy = homes(step)
        zh, yh = (me[0] + dz) % RING, (me[1] + dy) % RING
        slot = step % SLOTS
        found = []
        for n in range(1, LINE):
            d, dc = n // CORES, n % CORES
            c = (core + dc) % CORES
            found.append((None, remote(
                ob.at[slot, (me[2] + d) % RING, c, :, pl.ds(col0[0], main)],
                r1.at[0, own[0], zh, yh, :, pl.ds(0, main)],
                p1s.at[slot, n], p1r.at[0, n], shifted(2, d, c))))
        for g, axis, d, lead in ((1, 1, dy, zh), (2, 0, dz, yh)):
            for dc in range(CORES):
                c = (core + dc) % CORES
                found.append((None if dc else d != 0, remote(
                    ob.at[slot, :, c, :, pl.ds(col0[g], width[g])],
                    r1.at[g, own[g], lead, :, :, pl.ds(0, width[g])],
                    p1s.at[slot, LINE + 2 * (g - 1) + dc], p1r.at[g, d * CORES + dc], shifted(axis, d, c))))
        return found

    def each(found, act):
        for whether, copy in found:
            if whether is None:
                act(copy)
            else:
                @pl.when(whether)
                def _():
                    act(copy)

    eye = diagonal(cap)

    def room(step):
        @pl.when(step >= SLOTS)
        def _():
            each(first(step - SLOTS), lambda copy: copy.wait_send())

    def leave(step):
        each(first(step), lambda copy: copy.start())
        dz, dy = homes(step)
        zh, yh = (me[0] + dz) % RING, (me[1] + dy) % RING
        slot = step % SLOTS
        r1[0, own[0], zh, yh, :, pl.ds(0, width[0])] = ob[slot, me[2], core, :, pl.ds(col0[0], width[0])]
        if more:
            rest[zh, yh] = ob[slot, :, :, :, pl.ds(col0[0] + main, more)]
        for g, d, lead in ((1, dy, zh), (2, dz, yh)):
            @pl.when(d == 0)
            def _():
                for xh in range(RING):
                    r1[g, own[g], lead, xh, :, pl.ds(0, width[g])] = ob[slot, xh, core, :, pl.ds(col0[g], width[g])]

    def tile(step, _):
        @pl.when(step + 1 < RING * RING)
        def _():
            tile_load(step + 1, me, rx_ref, xb, xsem).start()

        room(step - 1)
        tile_load(step, me, rx_ref, xb, xsem).wait()
        up(step, w1, w3, xb, hh, res, top, ob)
        leave(step - 1)
        down(step, me, w2, hh, res, top, so)
        return 0

    steps = RING * RING
    pl.semaphore_wait(ready, len(PEERS))

    def leave_early(step, _):
        leave(step)
        return 0

    lax.fori_loop(0, EARLY - 1, leave_early, 0)
    lax.fori_loop(EARLY, steps, tile, 0)
    room(steps - 1)
    code(steps - 1, 0, hd // 128, res, top, ob)
    leave(steps - 1)

    def scales(g, coord, c):
        return (so.at[:, :, coord, c], so.at[:, coord, :, c], so.at[coord, :, :, c])[g]

    hints = []
    for g in everyone:
        axis = RETURNS[g][0]
        s1[g, own[g]] = (so[:, :, me[2], core], so[:, me[1], :, core], so[me[0], :, :, core])[g]
        for n in range(1, LINE):
            d, dc = n // CORES, n % CORES
            c = (core + dc) % CORES
            hints.append(remote(scales(g, (me[axis] + d) % RING, c), s1.at[g, own[g]],
                                q1s.at[g, n], q1r.at[g, n], shifted(axis, d, c)))
            hints[-1].start()

    later = []
    if more:
        for n in range(1, LINE):
            d, dc = n // CORES, n % CORES
            c = (core + dc) % CORES
            later.append(remote(rest.at[:, :, (me[2] + d) % RING, c], r1.at[0, own[0], :, :, :, pl.ds(main, more)],
                                e1s.at[n], e1r.at[n], shifted(2, d, c)))
            later[-1].start()

    def lane(ref, g, h2, h3):
        return (ref.at[0, :, h3, h2], ref.at[1, :, h2, h3], ref.at[2, :, h3, h2])[g]

    def second(g, k3, d):
        _, axis, third = RETURNS[g]
        h3 = (me[third] + k3) % RING
        at = pl.ds(0, main)
        src = (r1.at[0, :, h3, (me[axis] + d) % RING, :, at] if g == 0 else
               r1.at[1, :, (me[axis] + d) % RING, h3, :, at] if g == 1 else
               r1.at[2, :, h3, (me[axis] + d) % RING, :, at])
        return remote(src, r2.at[g, h3, me[axis], :, :, at], p2s.at[g, k3, d], p2r.at[g, k3, d], shifted(axis, d))

    def second_more(k3, d):
        _, axis, third = RETURNS[0]
        h3 = (me[third] + k3) % RING
        at = pl.ds(main, more)
        return remote(r1.at[0, :, h3, (me[axis] + d) % RING, :, at], r2.at[0, h3, me[axis], :, :, at],
                      e2s.at[k3, d], e2r.at[k3, d], shifted(axis, d))

    for g in everyone:
        axis = RETURNS[g][0]
        for n in range(1, LINE):
            d, dc = n // CORES, n % CORES
            src = (me[axis] - d) % RING * CORES + (core + dc) % CORES
            ref = r1.at[g, src, :, :, :, pl.ds(0, main)]
            pltpu.make_async_copy(ref, ref, p1r.at[g, n]).wait()
        for d in (1, 3, 2):
            second(g, LINES[0], d).start()

    for copy in hints:
        copy.wait_recv()
    moved = []
    for g in everyone:
        axis = RETURNS[g][1]
        s2[g, me[axis]] = (s1[0, :, :, me[1]], s1[1, :, me[0]], s1[2, :, :, me[2]])[g]
        for d in (1, 3, 2):
            moved.append(remote(lane(s1, g, (me[axis] + d) % RING, slice(None)), s2.at[g, me[axis]],
                                q2s.at[g, d], q2r.at[g, d], shifted(axis, d)))
            moved[-1].start()

    for copy in later:
        copy.wait_recv()
    def rest_of(k3):
        for d in (1, 3, 2):
            if more:
                second_more(k3, d).start()
            for g in everyone:
                if k3 != LINES[0]:
                    second(g, k3, d).start()

    for k3 in LINES[:-1]:
        rest_of(k3)

    for copy in moved:
        copy.wait_recv()

    wanted = lax.broadcasted_iota(jnp.int32, (cap, t), 0).astype(f32)

    def weights(g, h3, src):
        first_axis, axis, third = RETURNS[g]
        base = src * STRIDES[axis] + me[third] * STRIDES[third]
        found = {}

        def begin():
            ids = info[third, h3, 0:8, :]
            gates = info[third, h3, 8:16, :]
            hits, gate = [], []
            for k in range(LINE):
                same = ids == (base + (k // CORES) * STRIDES[first_axis] + k % CORES).astype(f32)
                hits.append(jnp.sum(jnp.where(same, 1.0, 0.0), axis=0, keepdims=True))
                gate.append(jnp.sum(jnp.where(same, gates, 0.0), axis=0, keepdims=True))
            hit = jnp.concatenate(hits, axis=0)
            rank = jnp.dot(hit.astype(bf16), upper[...], preferred_element_type=f32)
            found["slot"] = jnp.where((hit > 0.5) & (rank < cap + 0.5), rank - 1.0, -1.0)
            found["gate"] = gate

        def expert(k):
            scale = jnp.sum(jnp.where(eye, s2[g, src, k, h3], 0.0), axis=1, keepdims=True)
            w = jnp.where(found["slot"][k:k + 1, :] == wanted, found["gate"][k], 0.0) * scale
            for p in range(3):
                a = w.astype(bf16)
                wt[g, pl.ds(p * rows + k * cap, cap), :] = a
                w = w - a.astype(f32)

        return [begin] + [functools.partial(expert, k) for k in range(LINE)]

    def line(index, _):
        k3 = 2 - index + 3 * (index // 2) - 2 * (index // 3)

        def plane(turn, _):
            d = turn + turn // 2 - 2 * (turn // 3)

            def fetch(g):
                third = RETURNS[g][2]
                src = (me[RETURNS[g][1]] - d) % RING
                return pltpu.make_async_copy(r2.at[g, (me[third] + k3) % RING, src, :, :, pl.ds(0, width[g])],
                                             db.at[g, :, :, pl.ds(0, width[g])], dsem.at[g])

            for g in everyone:
                _, axis, third = RETURNS[g]
                h3 = (me[third] + k3) % RING

                @pl.when(turn == 0)
                def _():
                    at = pl.ds(0, width[g])
                    if g == 1:
                        db[g, :, :, at] = r1[g, :, me[axis], h3, :, at]
                    else:
                        db[g, :, :, at] = r1[g, :, h3, me[axis], :, at]
                    acc[g, index] = jnp.zeros(acc.shape[2:], f32)

                @pl.when(turn > 0)
                def _():
                    second(g, k3, d).wait_recv()
                    if more and g == 0:
                        second_more(k3, d).wait_recv()
                    fetch(g).start()

            @pl.when(turn > 0)
            def _():
                for g in everyone:
                    fetch(g).wait()

            def piece(g, begin, size):
                at = pl.ds(begin, size)
                q = db[g, :, :, at].reshape(rows, size).astype(f32)
                high = q.astype(bf16)
                low = (q - high.astype(f32)).astype(bf16)
                dims = (((0,), (0,)), ((), ()))
                p = (lax.dot_general(wt[g], jnp.concatenate([high] * 3, axis=0), dims, preferred_element_type=f32)
                     + lax.dot_general(wt[g], jnp.concatenate([low] * 3, axis=0), dims, preferred_element_type=f32))
                acc[g, index, :, at] += p

            def steps_of(g):
                _, axis, third = RETURNS[g]
                return weights(g, (me[third] + k3) % RING, (me[axis] - d) % RING)

            for act in steps_of(0):
                act()
            for g in everyone:
                products = [functools.partial(piece, g, begin, min(PIECE, width[g] - begin))
                            for begin in range(0, width[g], PIECE)]
                others = steps_of(g + 1) if g + 1 < len(groups) else []
                for k, act in enumerate(products):
                    act()
                    for other in others[len(others) * k // len(products):len(others) * (k + 1) // len(products)]:
                        other()

            for g in everyone:
                @pl.when((turn == RING - 1) & (index == 0))
                def _():
                    for way in range(2):
                        opposite(g, way).start()

                @pl.when((turn == RING - 1) & (index == 2))
                def _():
                    for way in range(2):
                        opposite(g, way).wait_recv()
                        rows_of = pl.ds(way * (t // 2), t // 2)
                        at = pl.ds(0, width[g])
                        acc[g, 1 + way, rows_of, at] += part[g, way, :, at]
                    for way in range(2):
                        home(g, way).start()
            return 0

        lax.fori_loop(0, RING, plane, 0)

        @pl.when(index == 0)
        def _():
            rest_of(LINES[-1])
        return 0

    def opposite(g, way):
        at = pl.ds(0, width[g])
        return remote(acc.at[g, 0, pl.ds(way * (t // 2), t // 2), at], part.at[g, way, :, at],
                      hs.at[g, way], hr.at[g, way], shifted(RETURNS[g][2], LINES[1 + way]))

    def home(g, way):
        at = pl.ds(0, width[g])
        return remote(acc.at[g, 1 + way, :, at], planes.at[g, way, :, at],
                      p3s.at[g, way], p3r.at[g, way], shifted(RETURNS[g][2], LINES[1 + way]))

    lax.fori_loop(0, RING, line, 0)

    for copy in hints + moved + later:
        copy.wait_send()

    def last(step, _):
        each(first(step), lambda copy: copy.wait_send())
        return 0

    lax.fori_loop(RING * RING - SLOTS, RING * RING, last, 0)
    for g in everyone:
        for k3 in range(RING):
            for d in (1, 3, 2):
                second(g, k3, d).wait_send()
                if more and g == 0:
                    second_more(k3, d).wait_send()
        for way in range(2):
            opposite(g, way).wait_send()

    xload.wait()
    stores = []
    for g in reversed(everyone):
        for way in range(2):
            home(g, way).wait_recv()

        def finish(n, _):
            at = pl.ds(pl.multiple_of(n * 128, 128), 128)
            to = pl.ds(pl.multiple_of(col0[g] + n * 128, 128), 128)
            total = acc[g, RING - 1, :, at] + planes[g, 0, :, at] + planes[g, 1, :, at]
            yv[:, to] = (xv[:, to].astype(f32) + total).astype(bf16)
            return 0

        lax.fori_loop(0, width[g] // 128, finish, 0)
        at = pl.ds(col0[g], width[g])
        stores.append(pltpu.make_async_copy(yv.at[:, at], y_ref.at[:, at], ysem.at[g]))
        stores[-1].start()

    for g in everyone:
        for way in range(2):
            home(g, way).wait_send()
    for store in stores:
        store.wait()


def layer_kernel(t, cap, groups, ids_ref, gates_ref, x_ref, w1_ref, w3_ref, w2_ref, y_ref, rx_ref, r2,
                 w1, w3, w2, idv, gatev, info, upper, xb, hh, res, top, ob, so, yv, ready, small_sem, wsem, load_sem,
                 gsend, grecv, rsend, rrecv, self_sem, isend, irecv, ysem, xsem, *sems):
    hd = w1.shape[0]
    n = len(groups)
    wide = max(w for _, w in groups)
    more = max(wide - min(w for _, w in groups), 128)
    small = [pltpu.make_async_copy(a, b, small_sem.at[k]) for k, (a, b) in enumerate(((ids_ref, idv), (gates_ref, gatev)))]
    weight_loads = [pltpu.make_async_copy(a, b, wsem.at[k])
                    for k, (a, b) in enumerate(((w1_ref, w1), (w3_ref, w3), (w2_ref, w2)))]
    for load in small:
        load.start()
    for load in small:
        load.wait()

    def there(got, out, pick):
        dispatch_part(t, cap, groups, x_ref, rx_ref, idv, gatev, upper, info, load_sem, gsend, grecv, rsend, rrecv, self_sem,
                      isend, irecv, weight_loads, xsem, w1, w3, w2, xb, hh, res, top, ob, so, got, out, pick)

    pl.run_scoped(there,
                  pltpu.VMEM((n, RING, RING, t + IDROWS, wide), bf16),
                  pltpu.VMEM((n, RING, LINE, RING, cap, wide), bf16),
                  pltpu.VMEM((LINE * cap, t), bf16))

    def back(*scratch):
        experts_part(t, cap, groups, x_ref, rx_ref, y_ref, r2, w1, w3, w2, info, upper, ready, ysem, xsem, sems,
                     xb, hh, res, top, ob, so, yv, *scratch)

    pl.run_scoped(back,
                  pltpu.VMEM((RING, RING, RING, CORES, cap, more), i16),
                  pltpu.VMEM((n, LINE, RING, RING, cap, wide), i16),
                  pltpu.VMEM((n, LINE, RING, RING, 1, 128), f32),
                  pltpu.VMEM((n, RING, LINE, RING, 1, 128), f32),
                  pltpu.VMEM((n, RING, t, wide), f32),
                  pltpu.VMEM((n, 2, t // 2, wide), f32),
                  pltpu.VMEM((n, 2, t, wide), f32),
                  pltpu.VMEM((n, LINE, cap, wide), i16),
                  pltpu.VMEM((n, 3 * LINE * cap, t), bf16),
                  pltpu.VMEM((t, hd), bf16))


def layer(x, ids, gates, w1, w3, w2, cap):
    t, hd = x.shape
    ff = w1.shape[1]
    groups = column_groups(hd, 128)
    wide = max(w for _, w in groups)
    n = len(groups)
    dma = pltpu.SemaphoreType.DMA
    anywhere = pl.BlockSpec(memory_space=pl.ANY)
    y, _, _ = pl.pallas_call(
        functools.partial(layer_kernel, t, cap, groups),
        out_shape=(jax.ShapeDtypeStruct((t, hd), bf16),
                   jax.ShapeDtypeStruct((RING, RING, RING, CORES, cap, hd), bf16),
                   jax.ShapeDtypeStruct((n, RING, RING, LINE, cap, wide), i16)),
        in_specs=[anywhere] * 6,
        out_specs=(anywhere,) * 3,
        scratch_shapes=[
            pltpu.VMEM((hd, ff), bf16), pltpu.VMEM((hd, ff), bf16), pltpu.VMEM((ff, hd), bf16),
            pltpu.VMEM((IDROWS, t), jnp.int32), pltpu.VMEM((IDROWS, t), f32),
            pltpu.VMEM((3, RING, 2 * IDROWS, t), f32),
            pltpu.VMEM((t, t), bf16),
            pltpu.VMEM((2, RING, CORES, cap, hd), bf16),
            pltpu.VMEM((LINE * cap, ff), bf16),
            pltpu.VMEM((LINE * cap, hd), f32),
            pltpu.VMEM((LINE * cap, 128), f32),
            pltpu.VMEM((SLOTS, RING, CORES, cap, hd), i16),
            pltpu.VMEM((RING, RING, RING, CORES, 1, 128), f32),
            pltpu.VMEM((t, hd), bf16),
            pltpu.SemaphoreType.REGULAR,
            dma((2,)), dma((3,)), dma((n,)),
            dma((n, 4 + 4 * RING)), dma((n, 4 + 4 * RING)), dma((n, RING, LINE)), dma((n, RING, LINE)), dma((n, RING)),
            dma((3, RING)), dma((3, RING)), dma((n + 1,)), dma((2,)),
            dma((SLOTS, LINE + 4)), dma((n, LINE)), dma((n, LINE)), dma((n, LINE)),
            dma((n, RING, RING)), dma((n, RING, RING)), dma((n, RING)), dma((n, RING)),
            dma((n, 2)), dma((n, 2)), dma((n, 2)), dma((n, 2)), dma((LINE,)), dma((LINE,)),
            dma((RING, RING)), dma((RING, RING)), dma((n,)),
        ],
        compiler_params=pltpu.CompilerParams(collective_id=0, has_side_effects=True, vmem_limit_bytes=67043328),
        name="layer",
    )(ids.T, gates.T, x, w1, w3, w2)
    return y


def solution(mesh):
    nd = mesh.shape["ey"] * mesh.shape["ex"]
    tok = P(("dp", "ey", "ex"), None)
    wsp = P(("ey", "ex"), None, None)

    def local(x, ids, gates, w1, w3, w2):
        t = x.shape[0]
        cap = min(t, CAPF * t * ids.shape[1] // nd)
        return layer(x, ids, gates, w1[0], w3[0], w2[0], cap)

    return jax.shard_map(local, mesh=mesh, in_specs=(tok, tok, tok, wsp, wsp, wsp),
                         out_specs=tok, check_vma=False)
```

```python
import functools

import jax
import jax.numpy as jnp
from jax import lax
from jax.experimental import pallas as pl
from jax.experimental.pallas import tpu as pltpu
from jax.sharding import PartitionSpec as P

CAPF = 2
FULL = 32000.0
RING = 4
CORES = 2
IDROWS = 8
ORDERS = ((0, 1, 2), (2, 0, 1), (1, 2, 0))
LINE = RING * CORES
STRIDES = (RING * RING * CORES, RING * CORES, CORES)
RETURNS = ((2, 1, 0), (1, 0, 2), (0, 2, 1))
TILE = 256
LINES = (2, 1, 3, 0)
WIDE = 512
PIECE = 256
SLOTS = 5
MESH = pl.DeviceIdType.MESH
PEERS = [(axis, by, dc) for axis in range(3) for by in range(1, RING) for dc in range(CORES)] + [(0, 0, 1)]
bf16, i16, f32 = jnp.bfloat16, jnp.int16, jnp.float32


def column_groups(hd, tile):
    tiles = hd // tile
    first = -(-tiles // 3)
    second = -(-(tiles - first) // 2)
    widths = [first * tile, second * tile, (tiles - first - second) * tile]
    starts = [0, widths[0], widths[0] + widths[1]]
    return list(zip(starts, widths))


EARLY = 2


def homes(step):
    turn, k = step // RING, step % RING
    dy = (1 + 2 * k - 3 * (k // 2)) % RING
    return (dy + 2 - turn + 3 * (turn // 2) - 2 * (turn // 3)) % RING, dy


def tile_load(step, me, rx_ref, xb, xsem):
    dz, dy = homes(step)
    return pltpu.make_async_copy(rx_ref.at[(me[0] + dz) % RING, (me[1] + dy) % RING], xb.at[step % 2], xsem.at[step % 2])


def diagonal(cap):
    return lax.broadcasted_iota(jnp.int32, (cap, 128), 0) == lax.broadcasted_iota(jnp.int32, (cap, 128), 1)


def code(step, begin, end, res, top, ob):
    slot = step % SLOTS
    cap = ob.shape[3]
    for n in range(begin, end):
        at = pl.ds(n * 128, 128)
        v = jnp.round(res[:, at] * top[...]).astype(jnp.int32).astype(i16)
        ob[slot, :, :, :, at] = v.reshape(RING, CORES, cap, 128)


def up(step, w1, w3, xb, hh, res, top, ob):
    hd, ff = w1.shape
    rows = hh.shape[0]
    ups, codes = ff // TILE, hd // 128
    for n in range(ups):
        at = pl.ds(n * TILE, TILE)
        xt = xb[step % 2].reshape(rows, hd)
        a1 = jnp.dot(xt, w1[:, at], preferred_element_type=f32)
        a3 = jnp.dot(xt, w3[:, at], preferred_element_type=f32)
        hh[:, at] = (a1 * (1.0 / (1.0 + jnp.exp(-a1))) * a3).astype(bf16)
        code(step - 1, codes * n // ups, codes * (n + 1) // ups, res, top, ob)


def down(step, me, w2, hh, res, top, so):
    ff, hd = w2.shape
    rows = hh.shape[0]
    cap = rows // LINE
    dz, dy = homes(step)
    zh, yh = (me[0] + dz) % RING, (me[1] + dy) % RING
    most = jnp.zeros((rows, 128), f32)
    for n in range(hd // WIDE):
        o = jnp.dot(hh[...], w2[:, n * WIDE:(n + 1) * WIDE], preferred_element_type=f32)
        res[:, n * WIDE:(n + 1) * WIDE] = o
        o = jnp.abs(o)
        for k in range(WIDE // 128):
            most = jnp.maximum(most, o[:, k * 128:(k + 1) * 128])
    peak = jnp.maximum(jnp.max(most, axis=1, keepdims=True), 1e-30)
    top[...] = jnp.broadcast_to(FULL / peak, top.shape)
    for k in range(LINE):
        part = jnp.where(diagonal(cap), peak[k * cap:(k + 1) * cap], 0.0)
        so[zh, yh, k // CORES, k % CORES] = jnp.sum(part, axis=0, keepdims=True) * (1.0 / FULL)


def dispatch_part(t, cap, groups, x_ref, rx_ref, small, idv, gatev, upper, info, load_sem, gsend, grecv, rsend, rrecv, self_sem,
                  isend, irecv, weight_loads, xsem, w1, w3, w2, xb, hh, res, top, ob, so, got, out, pick):
    ey, ex, dp = lax.axis_index("ey"), lax.axis_index("ex"), lax.axis_index("dp")
    me = [ey // RING, ey % RING, ex // CORES]
    core = ex % CORES
    rows = t + IDROWS
    split = (rows // 2 + 7) // 8 * 8

    def device(coords, c):
        return (dp, coords[0] * RING + coords[1], coords[2] * CORES + c)

    def shifted(axis, by, c=None):
        coords = list(me)
        coords[axis] = (coords[axis] + by) % RING
        return device(coords, core if c is None else c)

    loads = [pltpu.make_async_copy(x_ref.at[:, pl.ds(start, width)], got.at[g, 0, 0, pl.ds(0, t), pl.ds(0, width)],
                                   load_sem.at[g]) for g, (start, width) in enumerate(groups)]

    barrier = pltpu.get_barrier_semaphore()
    for axis, by, dc in PEERS:
        pl.semaphore_signal(barrier, inc=1, device_id=shifted(axis, by, (core + dc) % CORES), device_id_type=MESH)
    for load in small + loads:
        load.start()
    row = lax.broadcasted_iota(jnp.int32, (t, t), 0)
    col = lax.broadcasted_iota(jnp.int32, (t, t), 1)
    upper[...] = jnp.where(row <= col, 1.0, 0.0).astype(bf16)
    for load in small:
        load.wait()
    ids = idv[...].astype(f32)
    for g in range(len(groups)):
        got[g, 0, 0, pl.ds(t, IDROWS), pl.ds(0, t)] = ids.astype(bf16)
    for axis in range(3):
        info[axis, me[axis], 0:8, :] = ids
        info[axis, me[axis], 8:16, :] = gatev[...]
    pl.semaphore_wait(barrier, len(PEERS))
    for load in loads:
        load.wait()

    def hop(g, index, block, to, axis, by, part=None):
        width = groups[g][1]
        at = pl.ds(0, rows) if part is None else part
        copy = pltpu.make_async_remote_copy(
            src_ref=got.at[g, block[0], block[1], at, pl.ds(0, width)],
            dst_ref=got.at[g, to[0], to[1], at, pl.ds(0, width)],
            send_sem=gsend.at[g, index], recv_sem=grecv.at[g, index],
            device_id=shifted(axis, by), device_id_type=MESH)
        copy.start()
        hops[g, index] = copy

    hops = {}
    low, high = pl.ds(0, split), pl.ds(split, rows - split)

    def first(g):
        p = ORDERS[g][0]
        hop(g, 0, (0, 0), (3, 0), p, 1)
        hop(g, 1, (0, 0), (1, 0), p, 3)

    def second(g, i):
        q = ORDERS[g][1]
        hop(g, 4 + 4 * i, (i, 0), (i, 3), q, 1)
        hop(g, 5 + 4 * i, (i, 0), (i, 1), q, 3)

    def second_on(g, i):
        q = ORDERS[g][1]
        hops[g, 4 + 4 * i].wait_recv()
        hop(g, 6 + 4 * i, (i, 3), (i, 2), q, 1, low)
        hops[g, 5 + 4 * i].wait_recv()
        hop(g, 7 + 4 * i, (i, 1), (i, 2), q, 3, high)

    everyone = range(len(groups))
    for g in everyone:
        first(g)
        second(g, 0)
    for g in everyone:
        p = ORDERS[g][0]
        hops[g, 0].wait_recv()
        hop(g, 2, (3, 0), (2, 0), p, 1, low)
        second(g, 3)
        hops[g, 1].wait_recv()
        hop(g, 3, (1, 0), (2, 0), p, 3, high)
        second(g, 1)
    for g in everyone:
        second_on(g, 0)
    for g in everyone:
        hops[g, 2].wait_recv()
        hops[g, 3].wait_recv()
        second(g, 2)

    def choose(g, j):
        p, _, r = ORDERS[g]
        width = groups[g][1]
        stride = (RING * RING * CORES, RING * CORES, CORES)[r]
        base = ey * (RING * CORES) + ex - core - me[r] * stride

        def one(i, _):
            ids = got[g, i, j, pl.ds(t, IDROWS), pl.ds(0, t)].astype(f32)
            lines = []
            for k in range(RING * CORES):
                expert = (base + (k // CORES) * stride + k % CORES).astype(f32)
                lines.append(jnp.sum(jnp.where(ids == expert, 1.0, 0.0), axis=0, keepdims=True))
            hit = jnp.concatenate(lines, axis=0)
            rank = jnp.dot(hit.astype(bf16), upper[...], preferred_element_type=f32)
            slot = jnp.where((hit > 0.5) & (rank < cap + 0.5), rank - 1.0, -1.0)
            wanted = lax.broadcasted_iota(jnp.int32, (cap, t), 0).astype(f32)
            for k in range(RING * CORES):
                pick[pl.ds(k * cap, cap), :] = jnp.where(slot[k:k + 1, :] == wanted, 1.0, 0.0).astype(bf16)
            place = (me[p] + i) % RING

            def tile(n, _):
                at = pl.ds(pl.multiple_of(n * 128, 128), 128)
                val = jnp.dot(pick[...], got[g, i, j, pl.ds(0, t), at], preferred_element_type=f32).astype(bf16)
                for k in range(RING * CORES):
                    out[g, j, k, place, :, at] = val[k * cap:(k + 1) * cap]
                return 0

            return lax.fori_loop(0, width // 128, tile, 0)

        lax.fori_loop(0, RING, one, 0)

    def place_in(ref, g, j):
        start, width = groups[g]
        p, q, r = ORDERS[g]
        at = [None, None, None]
        at[p] = slice(None)
        at[q] = (me[q] + j) % RING
        at[r] = me[r]
        return ref.at[at[0], at[1], at[2], core, :, pl.ds(start, width)]

    sends = {}

    def exchange(g, j):
        _, _, r = ORDERS[g]
        width = groups[g][1]
        for dr in range(RING):
            for dc in range(CORES):
                to, c = (me[r] + dr) % RING, (core + dc) % CORES
                src = out.at[g, j, to * CORES + c, :, :, pl.ds(0, width)]
                if dr == 0 and dc == 0:
                    copy = pltpu.make_async_copy(src, place_in(rx_ref, g, j), self_sem.at[g, j])
                else:
                    n = dr * CORES + dc
                    copy = pltpu.make_async_remote_copy(
                        src_ref=src, dst_ref=place_in(rx_ref, g, j),
                        send_sem=rsend.at[g, j, n], recv_sem=rrecv.at[g, j, n],
                        device_id=shifted(r, dr, c), device_id_type=MESH)
                sends.setdefault((g, j), []).append(copy)
                copy.start()

    for g in everyone:
        choose(g, 0)
        exchange(g, 0)
    for load in weight_loads:
        load.start()
    told = []
    for axis in range(3):
        for by in range(1, RING):
            told.append(pltpu.make_async_remote_copy(
                src_ref=info.at[axis, me[axis]], dst_ref=info.at[axis, me[axis]], send_sem=isend.at[axis, by],
                recv_sem=irecv.at[axis, by], device_id=shifted(axis, by), device_id_type=MESH))
            told[-1].start()
    for i in (3, 1):
        for g in everyone:
            second_on(g, i)
    for g in everyone:
        second_on(g, 2)
    for j in (3, 1):
        for g in everyone:
            choose(g, j)
            exchange(g, j)
    for g in (2, 0, 1):
        for i in range(RING):
            hops[g, 6 + 4 * i].wait_recv()
            hops[g, 7 + 4 * i].wait_recv()
        choose(g, 2)
        exchange(g, 2)

    def arrived(which):
        for each in which:
            for copy in sends[each][1:]:
                copy.wait_recv()
            sends[each][0].wait()

    last = [(0, 2), (1, 2)]
    arrived([each for each in sends if each not in last])
    for load in weight_loads:
        load.wait()
    tile_load(0, me, rx_ref, xb, xsem).start()

    def tile(step, _):
        @pl.when(step + 1 < EARLY)
        def _():
            tile_load(step + 1, me, rx_ref, xb, xsem).start()

        tile_load(step, me, rx_ref, xb, xsem).wait()
        up(step, w1, w3, xb, hh, res, top, ob)
        down(step, me, w2, hh, res, top, so)
        return 0

    lax.fori_loop(0, EARLY, tile, 0)

    arrived(last)
    for copy in list(hops.values()) + told + [copy for each in sends.values() for copy in each[1:]]:
        copy.wait_send()
    for copy in told:
        copy.wait_recv()


def experts_part(t, cap, groups, x_ref, rx_ref, y_ref, r2, w1, w3, w2, info, upper, ready, ysem, xsem, sems,
                 xb, hh, res, top, ob, so, yv, rest, r1, s1, s2, acc, part, planes, db, wt, xv):
    p1s, p1r, q1s, q1r, p2s, p2r, q2s, q2r, p3s, p3r, hs, hr, e1s, e1r, e2s, e2r, dsem = sems
    ey, ex, dp = lax.axis_index("ey"), lax.axis_index("ex"), lax.axis_index("dp")
    me = [ey // RING, ey % RING, ex // CORES]
    core = ex % CORES
    rows = LINE * cap
    hd, ff = w1.shape
    everyone = range(len(groups))
    col0 = [start for start, _ in groups]
    width = [w for _, w in groups]
    main = min(width)
    more = width[0] - main
    own = [me[RETURNS[g][0]] * CORES + core for g in everyone]

    def shifted(axis, by, c=None):
        coords = list(me)
        coords[axis] = (coords[axis] + by) % RING
        return (dp, coords[0] * RING + coords[1], coords[2] * CORES + (core if c is None else c))

    def remote(src, dst, send, recv, to):
        return pltpu.make_async_remote_copy(src_ref=src, dst_ref=dst, send_sem=send, recv_sem=recv,
                                            device_id=to, device_id_type=MESH)

    for axis, by, dc in PEERS:
        pl.semaphore_signal(ready, inc=1, device_id=shifted(axis, by, (core + dc) % CORES), device_id_type=MESH)
    tile_load(EARLY, me, rx_ref, xb, xsem).start()
    xload = pltpu.make_async_copy(x_ref, xv, ysem.at[len(groups)])
    xload.start()

    def first(step):
        dz, dy = homes(step)
        zh, yh = (me[0] + dz) % RING, (me[1] + dy) % RING
        slot = step % SLOTS
        found = []
        for n in range(1, LINE):
            d, dc = n // CORES, n % CORES
            c = (core + dc) % CORES
            found.append((None, remote(
                ob.at[slot, (me[2] + d) % RING, c, :, pl.ds(col0[0], main)],
                r1.at[0, own[0], zh, yh, :, pl.ds(0, main)],
                p1s.at[slot, n], p1r.at[0, n], shifted(2, d, c))))
        for g, axis, d, lead in ((1, 1, dy, zh), (2, 0, dz, yh)):
            for dc in range(CORES):
                c = (core + dc) % CORES
                found.append((None if dc else d != 0, remote(
                    ob.at[slot, :, c, :, pl.ds(col0[g], width[g])],
                    r1.at[g, own[g], lead, :, :, pl.ds(0, width[g])],
                    p1s.at[slot, LINE + 2 * (g - 1) + dc], p1r.at[g, d * CORES + dc], shifted(axis, d, c))))
        return found

    def each(found, act):
        for whether, copy in found:
            if whether is None:
                act(copy)
            else:
                @pl.when(whether)
                def _():
                    act(copy)

    eye = diagonal(cap)

    def room(step):
        @pl.when(step >= SLOTS)
        def _():
            each(first(step - SLOTS), lambda copy: copy.wait_send())

    def leave(step):
        each(first(step), lambda copy: copy.start())
        dz, dy = homes(step)
        zh, yh = (me[0] + dz) % RING, (me[1] + dy) % RING
        slot = step % SLOTS
        r1[0, own[0], zh, yh, :, pl.ds(0, width[0])] = ob[slot, me[2], core, :, pl.ds(col0[0], width[0])]
        if more:
            rest[zh, yh] = ob[slot, :, :, :, pl.ds(col0[0] + main, more)]
        for g, d, lead in ((1, dy, zh), (2, dz, yh)):
            @pl.when(d == 0)
            def _():
                for xh in range(RING):
                    r1[g, own[g], lead, xh, :, pl.ds(0, width[g])] = ob[slot, xh, core, :, pl.ds(col0[g], width[g])]

    def tile(step, _):
        @pl.when(step + 1 < RING * RING)
        def _():
            tile_load(step + 1, me, rx_ref, xb, xsem).start()

        room(step - 1)
        tile_load(step, me, rx_ref, xb, xsem).wait()
        up(step, w1, w3, xb, hh, res, top, ob)
        leave(step - 1)
        down(step, me, w2, hh, res, top, so)
        return 0

    steps = RING * RING
    pl.semaphore_wait(ready, len(PEERS))

    def leave_early(step, _):
        leave(step)
        return 0

    lax.fori_loop(0, EARLY - 1, leave_early, 0)
    lax.fori_loop(EARLY, steps, tile, 0)
    room(steps - 1)
    code(steps - 1, 0, hd // 128, res, top, ob)
    leave(steps - 1)

    def scales(g, coord, c):
        return (so.at[:, :, coord, c], so.at[:, coord, :, c], so.at[coord, :, :, c])[g]

    hints = []
    for g in everyone:
        axis = RETURNS[g][0]
        s1[g, own[g]] = (so[:, :, me[2], core], so[:, me[1], :, core], so[me[0], :, :, core])[g]
        for n in range(1, LINE):
            d, dc = n // CORES, n % CORES
            c = (core + dc) % CORES
            hints.append(remote(scales(g, (me[axis] + d) % RING, c), s1.at[g, own[g]],
                                q1s.at[g, n], q1r.at[g, n], shifted(axis, d, c)))
            hints[-1].start()

    later = []
    if more:
        for n in range(1, LINE):
            d, dc = n // CORES, n % CORES
            c = (core + dc) % CORES
            later.append(remote(rest.at[:, :, (me[2] + d) % RING, c], r1.at[0, own[0], :, :, :, pl.ds(main, more)],
                                e1s.at[n], e1r.at[n], shifted(2, d, c)))
            later[-1].start()

    def lane(ref, g, h2, h3):
        return (ref.at[0, :, h3, h2], ref.at[1, :, h2, h3], ref.at[2, :, h3, h2])[g]

    def second(g, k3, d):
        _, axis, third = RETURNS[g]
        h3 = (me[third] + k3) % RING
        at = pl.ds(0, main)
        src = (r1.at[0, :, h3, (me[axis] + d) % RING, :, at] if g == 0 else
               r1.at[1, :, (me[axis] + d) % RING, h3, :, at] if g == 1 else
               r1.at[2, :, h3, (me[axis] + d) % RING, :, at])
        return remote(src, r2.at[g, h3, me[axis], :, :, at], p2s.at[g, k3, d], p2r.at[g, k3, d], shifted(axis, d))

    def second_more(k3, d):
        _, axis, third = RETURNS[0]
        h3 = (me[third] + k3) % RING
        at = pl.ds(main, more)
        return remote(r1.at[0, :, h3, (me[axis] + d) % RING, :, at], r2.at[0, h3, me[axis], :, :, at],
                      e2s.at[k3, d], e2r.at[k3, d], shifted(axis, d))

    for g in everyone:
        axis = RETURNS[g][0]
        for n in range(1, LINE):
            d, dc = n // CORES, n % CORES
            src = (me[axis] - d) % RING * CORES + (core + dc) % CORES
            ref = r1.at[g, src, :, :, :, pl.ds(0, main)]
            pltpu.make_async_copy(ref, ref, p1r.at[g, n]).wait()
        for d in (1, 3, 2):
            second(g, LINES[0], d).start()

    for copy in hints:
        copy.wait_recv()
    moved = []
    for g in everyone:
        axis = RETURNS[g][1]
        s2[g, me[axis]] = (s1[0, :, :, me[1]], s1[1, :, me[0]], s1[2, :, :, me[2]])[g]
        for d in (1, 3, 2):
            moved.append(remote(lane(s1, g, (me[axis] + d) % RING, slice(None)), s2.at[g, me[axis]],
                                q2s.at[g, d], q2r.at[g, d], shifted(axis, d)))
            moved[-1].start()

    for copy in later:
        copy.wait_recv()
    def rest_of(k3):
        for d in (1, 3, 2):
            if more:
                second_more(k3, d).start()
            for g in everyone:
                if k3 != LINES[0]:
                    second(g, k3, d).start()

    for k3 in LINES[:-1]:
        rest_of(k3)

    for copy in moved:
        copy.wait_recv()

    wanted = lax.broadcasted_iota(jnp.int32, (cap, t), 0).astype(f32)

    def weights(g, h3, src):
        first_axis, axis, third = RETURNS[g]
        base = src * STRIDES[axis] + me[third] * STRIDES[third]
        found = {}

        def begin():
            ids = info[third, h3, 0:8, :]
            gates = info[third, h3, 8:16, :]
            hits, gate = [], []
            for k in range(LINE):
                same = ids == (base + (k // CORES) * STRIDES[first_axis] + k % CORES).astype(f32)
                hits.append(jnp.sum(jnp.where(same, 1.0, 0.0), axis=0, keepdims=True))
                gate.append(jnp.sum(jnp.where(same, gates, 0.0), axis=0, keepdims=True))
            hit = jnp.concatenate(hits, axis=0)
            rank = jnp.dot(hit.astype(bf16), upper[...], preferred_element_type=f32)
            found["slot"] = jnp.where((hit > 0.5) & (rank < cap + 0.5), rank - 1.0, -1.0)
            found["gate"] = gate

        def expert(k):
            scale = jnp.sum(jnp.where(eye, s2[g, src, k, h3], 0.0), axis=1, keepdims=True)
            w = jnp.where(found["slot"][k:k + 1, :] == wanted, found["gate"][k], 0.0) * scale
            for p in range(3):
                a = w.astype(bf16)
                wt[g, pl.ds(p * rows + k * cap, cap), :] = a
                w = w - a.astype(f32)

        return [begin] + [functools.partial(expert, k) for k in range(LINE)]

    def line(index, _):
        k3 = 2 - index + 3 * (index // 2) - 2 * (index // 3)

        def plane(turn, _):
            d = turn + turn // 2 - 2 * (turn // 3)

            def fetch(g):
                third = RETURNS[g][2]
                src = (me[RETURNS[g][1]] - d) % RING
                return pltpu.make_async_copy(r2.at[g, (me[third] + k3) % RING, src, :, :, pl.ds(0, width[g])],
                                             db.at[g, :, :, pl.ds(0, width[g])], dsem.at[g])

            for g in everyone:
                _, axis, third = RETURNS[g]
                h3 = (me[third] + k3) % RING

                @pl.when(turn == 0)
                def _():
                    at = pl.ds(0, width[g])
                    if g == 1:
                        db[g, :, :, at] = r1[g, :, me[axis], h3, :, at]
                    else:
                        db[g, :, :, at] = r1[g, :, h3, me[axis], :, at]
                    acc[g, index] = jnp.zeros(acc.shape[2:], f32)

                @pl.when(turn > 0)
                def _():
                    second(g, k3, d).wait_recv()
                    if more and g == 0:
                        second_more(k3, d).wait_recv()
                    fetch(g).start()

            @pl.when(turn > 0)
            def _():
                for g in everyone:
                    fetch(g).wait()

            def piece(g, begin, size):
                at = pl.ds(begin, size)
                q = db[g, :, :, at].reshape(rows, size).astype(f32)
                high = q.astype(bf16)
                low = (q - high.astype(f32)).astype(bf16)
                dims = (((0,), (0,)), ((), ()))
                p = (lax.dot_general(wt[g], jnp.concatenate([high] * 3, axis=0), dims, preferred_element_type=f32)
                     + lax.dot_general(wt[g], jnp.concatenate([low] * 3, axis=0), dims, preferred_element_type=f32))
                acc[g, index, :, at] += p

            def steps_of(g):
                _, axis, third = RETURNS[g]
                return weights(g, (me[third] + k3) % RING, (me[axis] - d) % RING)

            for act in steps_of(0):
                act()
            for g in everyone:
                products = [functools.partial(piece, g, begin, min(PIECE, width[g] - begin))
                            for begin in range(0, width[g], PIECE)]
                others = steps_of(g + 1) if g + 1 < len(groups) else []
                for k, act in enumerate(products):
                    act()
                    for other in others[len(others) * k // len(products):len(others) * (k + 1) // len(products)]:
                        other()

            for g in everyone:
                @pl.when((turn == RING - 1) & (index == 0))
                def _():
                    for way in range(2):
                        opposite(g, way).start()

                @pl.when((turn == RING - 1) & (index == 2))
                def _():
                    for way in range(2):
                        opposite(g, way).wait_recv()
                        rows_of = pl.ds(way * (t // 2), t // 2)
                        at = pl.ds(0, width[g])
                        acc[g, 1 + way, rows_of, at] += part[g, way, :, at]
                    for way in range(2):
                        home(g, way).start()
            return 0

        lax.fori_loop(0, RING, plane, 0)

        @pl.when(index == 0)
        def _():
            rest_of(LINES[-1])
        return 0

    def opposite(g, way):
        at = pl.ds(0, width[g])
        return remote(acc.at[g, 0, pl.ds(way * (t // 2), t // 2), at], part.at[g, way, :, at],
                      hs.at[g, way], hr.at[g, way], shifted(RETURNS[g][2], LINES[1 + way]))

    def home(g, way):
        at = pl.ds(0, width[g])
        return remote(acc.at[g, 1 + way, :, at], planes.at[g, way, :, at],
                      p3s.at[g, way], p3r.at[g, way], shifted(RETURNS[g][2], LINES[1 + way]))

    lax.fori_loop(0, RING, line, 0)

    for copy in hints + moved + later:
        copy.wait_send()

    def last(step, _):
        each(first(step), lambda copy: copy.wait_send())
        return 0

    lax.fori_loop(RING * RING - SLOTS, RING * RING, last, 0)
    for g in everyone:
        for k3 in range(RING):
            for d in (1, 3, 2):
                second(g, k3, d).wait_send()
                if more and g == 0:
                    second_more(k3, d).wait_send()
        for way in range(2):
            opposite(g, way).wait_send()

    xload.wait()
    stores = []
    for g in reversed(everyone):
        for way in range(2):
            home(g, way).wait_recv()

        def finish(n, _):
            at = pl.ds(pl.multiple_of(n * 128, 128), 128)
            to = pl.ds(pl.multiple_of(col0[g] + n * 128, 128), 128)
            total = acc[g, RING - 1, :, at] + planes[g, 0, :, at] + planes[g, 1, :, at]
            yv[:, to] = (xv[:, to].astype(f32) + total).astype(bf16)
            return 0

        lax.fori_loop(0, width[g] // 128, finish, 0)
        at = pl.ds(col0[g], width[g])
        stores.append(pltpu.make_async_copy(yv.at[:, at], y_ref.at[:, at], ysem.at[g]))
        stores[-1].start()

    for g in everyone:
        for way in range(2):
            home(g, way).wait_send()
    for store in stores:
        store.wait()


def layer_kernel(t, cap, groups, ids_ref, gates_ref, x_ref, w1_ref, w3_ref, w2_ref, y_ref, rx_ref, r2,
                 w1, w3, w2, idv, gatev, info, upper, xb, hh, res, top, ob, so, yv, ready, small_sem, wsem, load_sem,
                 gsend, grecv, rsend, rrecv, self_sem, isend, irecv, ysem, xsem, *sems):
    hd = w1.shape[0]
    n = len(groups)
    wide = max(w for _, w in groups)
    more = max(wide - min(w for _, w in groups), 128)
    small = [pltpu.make_async_copy(a, b, small_sem.at[k]) for k, (a, b) in enumerate(((ids_ref, idv), (gates_ref, gatev)))]
    weight_loads = [pltpu.make_async_copy(a, b, wsem.at[k])
                    for k, (a, b) in enumerate(((w1_ref, w1), (w3_ref, w3), (w2_ref, w2)))]

    def there(got, out, pick):
        dispatch_part(t, cap, groups, x_ref, rx_ref, small, idv, gatev, upper, info, load_sem, gsend, grecv, rsend, rrecv, self_sem,
                      isend, irecv, weight_loads, xsem, w1, w3, w2, xb, hh, res, top, ob, so, got, out, pick)

    pl.run_scoped(there,
                  pltpu.VMEM((n, RING, RING, t + IDROWS, wide), bf16),
                  pltpu.VMEM((n, RING, LINE, RING, cap, wide), bf16),
                  pltpu.VMEM((LINE * cap, t), bf16))

    def back(*scratch):
        experts_part(t, cap, groups, x_ref, rx_ref, y_ref, r2, w1, w3, w2, info, upper, ready, ysem, xsem, sems,
                     xb, hh, res, top, ob, so, yv, *scratch)

    pl.run_scoped(back,
                  pltpu.VMEM((RING, RING, RING, CORES, cap, more), i16),
                  pltpu.VMEM((n, LINE, RING, RING, cap, wide), i16),
                  pltpu.VMEM((n, LINE, RING, RING, 1, 128), f32),
                  pltpu.VMEM((n, RING, LINE, RING, 1, 128), f32),
                  pltpu.VMEM((n, RING, t, wide), f32),
                  pltpu.VMEM((n, 2, t // 2, wide), f32),
                  pltpu.VMEM((n, 2, t, wide), f32),
                  pltpu.VMEM((n, LINE, cap, wide), i16),
                  pltpu.VMEM((n, 3 * LINE * cap, t), bf16),
                  pltpu.VMEM((t, hd), bf16))


def layer(x, ids, gates, w1, w3, w2, cap):
    t, hd = x.shape
    ff = w1.shape[1]
    groups = column_groups(hd, 128)
    wide = max(w for _, w in groups)
    n = len(groups)
    dma = pltpu.SemaphoreType.DMA
    anywhere = pl.BlockSpec(memory_space=pl.ANY)
    y, _, _ = pl.pallas_call(
        functools.partial(layer_kernel, t, cap, groups),
        out_shape=(jax.ShapeDtypeStruct((t, hd), bf16),
                   jax.ShapeDtypeStruct((RING, RING, RING, CORES, cap, hd), bf16),
                   jax.ShapeDtypeStruct((n, RING, RING, LINE, cap, wide), i16)),
        in_specs=[anywhere] * 6,
        out_specs=(anywhere,) * 3,
        scratch_shapes=[
            pltpu.VMEM((hd, ff), bf16), pltpu.VMEM((hd, ff), bf16), pltpu.VMEM((ff, hd), bf16),
            pltpu.VMEM((IDROWS, t), jnp.int32), pltpu.VMEM((IDROWS, t), f32),
            pltpu.VMEM((3, RING, 2 * IDROWS, t), f32),
            pltpu.VMEM((t, t), bf16),
            pltpu.VMEM((2, RING, CORES, cap, hd), bf16),
            pltpu.VMEM((LINE * cap, ff), bf16),
            pltpu.VMEM((LINE * cap, hd), f32),
            pltpu.VMEM((LINE * cap, 128), f32),
            pltpu.VMEM((SLOTS, RING, CORES, cap, hd), i16),
            pltpu.VMEM((RING, RING, RING, CORES, 1, 128), f32),
            pltpu.VMEM((t, hd), bf16),
            pltpu.SemaphoreType.REGULAR,
            dma((2,)), dma((3,)), dma((n,)),
            dma((n, 4 + 4 * RING)), dma((n, 4 + 4 * RING)), dma((n, RING, LINE)), dma((n, RING, LINE)), dma((n, RING)),
            dma((3, RING)), dma((3, RING)), dma((n + 1,)), dma((2,)),
            dma((SLOTS, LINE + 4)), dma((n, LINE)), dma((n, LINE)), dma((n, LINE)),
            dma((n, RING, RING)), dma((n, RING, RING)), dma((n, RING)), dma((n, RING)),
            dma((n, 2)), dma((n, 2)), dma((n, 2)), dma((n, 2)), dma((LINE,)), dma((LINE,)),
            dma((RING, RING)), dma((RING, RING)), dma((n,)),
        ],
        compiler_params=pltpu.CompilerParams(collective_id=0, has_side_effects=True, vmem_limit_bytes=67043328),
        name="layer",
    )(ids.T, gates.T, x, w1, w3, w2)
    return y


def solution(mesh):
    nd = mesh.shape["ey"] * mesh.shape["ex"]
    tok = P(("dp", "ey", "ex"), None)
    wsp = P(("ey", "ex"), None, None)

    def local(x, ids, gates, w1, w3, w2):
        t = x.shape[0]
        cap = min(t, CAPF * t * ids.shape[1] // nd)
        return layer(x, ids, gates, w1[0], w3[0], w2[0], cap)

    return jax.shard_map(local, mesh=mesh, in_specs=(tok, tok, tok, wsp, wsp, wsp),
                         out_specs=tok, check_vma=False)
```

```python
import functools

import jax
import jax.numpy as jnp
from jax import lax
from jax.experimental import pallas as pl
from jax.experimental.pallas import tpu as pltpu
from jax.sharding import PartitionSpec as P

CAPF = 2
FULL = 32000.0
RING = 4
CORES = 2
IDROWS = 8
ORDERS = ((0, 1, 2), (2, 0, 1), (1, 2, 0))
LINE = RING * CORES
STRIDES = (RING * RING * CORES, RING * CORES, CORES)
RETURNS = ((2, 1, 0), (1, 0, 2), (0, 2, 1))
TILE = 256
LINES = (2, 1, 3, 0)
WIDE = 512
PIECE = 256
SLOTS = 5
MESH = pl.DeviceIdType.MESH
PEERS = [(axis, by, dc) for axis in range(3) for by in range(1, RING) for dc in range(CORES)] + [(0, 0, 1)]
bf16, i16, f32 = jnp.bfloat16, jnp.int16, jnp.float32


def column_groups(hd, tile):
    tiles = hd // tile
    first = -(-tiles // 3)
    second = -(-(tiles - first) // 2)
    widths = [first * tile, second * tile, (tiles - first - second) * tile]
    starts = [0, widths[0], widths[0] + widths[1]]
    return list(zip(starts, widths))


EARLY = 2


def homes(step):
    turn, k = step // RING, step % RING
    dy = (1 + 2 * k - 3 * (k // 2)) % RING
    return (dy + 2 - turn + 3 * (turn // 2) - 2 * (turn // 3)) % RING, dy


def tile_load(step, me, rx_ref, xb, xsem):
    dz, dy = homes(step)
    return pltpu.make_async_copy(rx_ref.at[(me[0] + dz) % RING, (me[1] + dy) % RING], xb.at[step % 2], xsem.at[step % 2])


def diagonal(cap):
    return lax.broadcasted_iota(jnp.int32, (cap, 128), 0) == lax.broadcasted_iota(jnp.int32, (cap, 128), 1)


def code(step, begin, end, res, top, ob):
    slot = step % SLOTS
    cap = ob.shape[3]
    for n in range(begin, end):
        at = pl.ds(n * 128, 128)
        v = jnp.round(res[:, at] * top[...]).astype(jnp.int32).astype(i16)
        ob[slot, :, :, :, at] = v.reshape(RING, CORES, cap, 128)


def up(step, w1, w3, xb, hh, res, top, ob):
    hd, ff = w1.shape
    rows = hh.shape[0]
    ups, codes = ff // TILE, hd // 128
    for n in range(ups):
        at = pl.ds(n * TILE, TILE)
        xt = xb[step % 2].reshape(rows, hd)
        a1 = jnp.dot(xt, w1[:, at], preferred_element_type=f32)
        a3 = jnp.dot(xt, w3[:, at], preferred_element_type=f32)
        hh[:, at] = (a1 * (1.0 / (1.0 + jnp.exp(-a1))) * a3).astype(bf16)
        code(step - 1, codes * n // ups, codes * (n + 1) // ups, res, top, ob)


def down(step, me, w2, hh, res, top, so):
    ff, hd = w2.shape
    rows = hh.shape[0]
    cap = rows // LINE
    dz, dy = homes(step)
    zh, yh = (me[0] + dz) % RING, (me[1] + dy) % RING
    most = jnp.zeros((rows, 128), f32)
    for n in range(hd // WIDE):
        o = jnp.dot(hh[...], w2[:, n * WIDE:(n + 1) * WIDE], preferred_element_type=f32)
        res[:, n * WIDE:(n + 1) * WIDE] = o
        o = jnp.abs(o)
        for k in range(WIDE // 128):
            most = jnp.maximum(most, o[:, k * 128:(k + 1) * 128])
    peak = jnp.maximum(jnp.max(most, axis=1, keepdims=True), 1e-30)
    top[...] = jnp.broadcast_to(FULL / peak, top.shape)
    for k in range(LINE):
        part = jnp.where(diagonal(cap), peak[k * cap:(k + 1) * cap], 0.0)
        so[zh, yh, k // CORES, k % CORES] = jnp.sum(part, axis=0, keepdims=True) * (1.0 / FULL)


def dispatch_part(t, cap, groups, x_ref, rx_ref, small, idv, gatev, upper, info, load_sem, gsend, grecv, rsend, rrecv, self_sem,
                  isend, irecv, weight_loads, xsem, w1, w3, w2, xb, hh, res, top, ob, so, got, out, pick):
    ey, ex, dp = lax.axis_index("ey"), lax.axis_index("ex"), lax.axis_index("dp")
    me = [ey // RING, ey % RING, ex // CORES]
    core = ex % CORES
    rows = t + IDROWS
    split = (rows // 2 + 7) // 8 * 8

    def device(coords, c):
        return (dp, coords[0] * RING + coords[1], coords[2] * CORES + c)

    def shifted(axis, by, c=None):
        coords = list(me)
        coords[axis] = (coords[axis] + by) % RING
        return device(coords, core if c is None else c)

    loads = [pltpu.make_async_copy(x_ref.at[:, pl.ds(start, width)], got.at[g, 0, 0, pl.ds(0, t), pl.ds(0, width)],
                                   load_sem.at[g]) for g, (start, width) in enumerate(groups)]

    barrier = pltpu.get_barrier_semaphore()
    for axis, by, dc in PEERS:
        pl.semaphore_signal(barrier, inc=1, device_id=shifted(axis, by, (core + dc) % CORES), device_id_type=MESH)
    for load in small + loads:
        load.start()
    row = lax.broadcasted_iota(jnp.int32, (t, t), 0)
    col = lax.broadcasted_iota(jnp.int32, (t, t), 1)
    upper[...] = jnp.where(row <= col, 1.0, 0.0).astype(bf16)
    for load in small:
        load.wait()
    ids = idv[...].astype(f32)
    for g in range(len(groups)):
        got[g, 0, 0, pl.ds(t, IDROWS), pl.ds(0, t)] = ids.astype(bf16)
    for axis in range(3):
        info[axis, me[axis], 0:8, :] = ids
        info[axis, me[axis], 8:16, :] = gatev[...]
    pl.semaphore_wait(barrier, len(PEERS))
    for load in loads:
        load.wait()

    def hop(g, index, block, to, axis, by, part=None):
        width = groups[g][1]
        at = pl.ds(0, rows) if part is None else part
        copy = pltpu.make_async_remote_copy(
            src_ref=got.at[g, block[0], block[1], at, pl.ds(0, width)],
            dst_ref=got.at[g, to[0], to[1], at, pl.ds(0, width)],
            send_sem=gsend.at[g, index], recv_sem=grecv.at[g, index],
            device_id=shifted(axis, by), device_id_type=MESH)
        copy.start()
        hops[g, index] = copy

    hops = {}
    low, high = pl.ds(0, split), pl.ds(split, rows - split)

    def first(g):
        p = ORDERS[g][0]
        hop(g, 0, (0, 0), (3, 0), p, 1)
        hop(g, 1, (0, 0), (1, 0), p, 3)

    def second(g, i):
        q = ORDERS[g][1]
        hop(g, 4 + 4 * i, (i, 0), (i, 3), q, 1)
        hop(g, 5 + 4 * i, (i, 0), (i, 1), q, 3)

    def second_on(g, i):
        q = ORDERS[g][1]
        hops[g, 4 + 4 * i].wait_recv()
        hop(g, 6 + 4 * i, (i, 3), (i, 2), q, 1, low)
        hops[g, 5 + 4 * i].wait_recv()
        hop(g, 7 + 4 * i, (i, 1), (i, 2), q, 3, high)

    def choose(g, j):
        p, _, r = ORDERS[g]
        width = groups[g][1]
        stride = (RING * RING * CORES, RING * CORES, CORES)[r]
        base = ey * (RING * CORES) + ex - core - me[r] * stride

        def one(i, _):
            ids = got[g, i, j, pl.ds(t, IDROWS), pl.ds(0, t)].astype(f32)
            lines = []
            for k in range(RING * CORES):
                expert = (base + (k // CORES) * stride + k % CORES).astype(f32)
                lines.append(jnp.sum(jnp.where(ids == expert, 1.0, 0.0), axis=0, keepdims=True))
            hit = jnp.concatenate(lines, axis=0)
            rank = jnp.dot(hit.astype(bf16), upper[...], preferred_element_type=f32)
            slot = jnp.where((hit > 0.5) & (rank < cap + 0.5), rank - 1.0, -1.0)
            wanted = lax.broadcasted_iota(jnp.int32, (cap, t), 0).astype(f32)
            for k in range(RING * CORES):
                pick[pl.ds(k * cap, cap), :] = jnp.where(slot[k:k + 1, :] == wanted, 1.0, 0.0).astype(bf16)
            place = (me[p] + i) % RING

            def tile(n, _):
                at = pl.ds(pl.multiple_of(n * 128, 128), 128)
                val = jnp.dot(pick[...], got[g, i, j, pl.ds(0, t), at], preferred_element_type=f32).astype(bf16)
                for k in range(RING * CORES):
                    out[g, j, k, place, :, at] = val[k * cap:(k + 1) * cap]
                return 0

            return lax.fori_loop(0, width // 128, tile, 0)

        lax.fori_loop(0, RING, one, 0)

    def place_in(ref, g, j):
        start, width = groups[g]
        p, q, r = ORDERS[g]
        at = [None, None, None]
        at[p] = slice(None)
        at[q] = (me[q] + j) % RING
        at[r] = me[r]
        return ref.at[at[0], at[1], at[2], core, :, pl.ds(start, width)]

    sends = {}

    def exchange(g, j):
        _, _, r = ORDERS[g]
        width = groups[g][1]
        for dr in range(RING):
            for dc in range(CORES):
                to, c = (me[r] + dr) % RING, (core + dc) % CORES
                src = out.at[g, j, to * CORES + c, :, :, pl.ds(0, width)]
                if dr == 0 and dc == 0:
                    copy = pltpu.make_async_copy(src, place_in(rx_ref, g, j), self_sem.at[g, j])
                else:
                    n = dr * CORES + dc
                    copy = pltpu.make_async_remote_copy(
                        src_ref=src, dst_ref=place_in(rx_ref, g, j),
                        send_sem=rsend.at[g, j, n], recv_sem=rrecv.at[g, j, n],
                        device_id=shifted(r, dr, c), device_id_type=MESH)
                sends.setdefault((g, j), []).append(copy)
                copy.start()

    everyone = range(len(groups))
    for g in everyone:
        first(g)
        second(g, 0)
    for g in everyone:
        p = ORDERS[g][0]
        hops[g, 0].wait_recv()
        hop(g, 2, (3, 0), (2, 0), p, 1, low)
        second(g, 3)
        hops[g, 1].wait_recv()
        hop(g, 3, (1, 0), (2, 0), p, 3, high)
        second(g, 1)
    for g in everyone:
        second_on(g, 0)
    for g in everyone:
        hops[g, 2].wait_recv()
        hops[g, 3].wait_recv()
        second(g, 2)
        choose(g, 0)
        exchange(g, 0)

    for load in weight_loads:
        load.start()
    told = []
    for axis in range(3):
        for by in range(1, RING):
            told.append(pltpu.make_async_remote_copy(
                src_ref=info.at[axis, me[axis]], dst_ref=info.at[axis, me[axis]], send_sem=isend.at[axis, by],
                recv_sem=irecv.at[axis, by], device_id=shifted(axis, by), device_id_type=MESH))
            told[-1].start()
    for i in (3, 1):
        for g in everyone:
            second_on(g, i)
    for g in everyone:
        second_on(g, 2)
    for j in (3, 1):
        for g in everyone:
            choose(g, j)
            exchange(g, j)
    for g in (2, 0, 1):
        for i in range(RING):
            hops[g, 6 + 4 * i].wait_recv()
            hops[g, 7 + 4 * i].wait_recv()
        choose(g, 2)
        exchange(g, 2)

    def arrived(which):
        for each in which:
            for copy in sends[each][1:]:
                copy.wait_recv()
            sends[each][0].wait()

    last = [(0, 2), (1, 2)]
    arrived([each for each in sends if each not in last])
    for load in weight_loads:
        load.wait()
    tile_load(0, me, rx_ref, xb, xsem).start()

    def tile(step, _):
        @pl.when(step + 1 < EARLY)
        def _():
            tile_load(step + 1, me, rx_ref, xb, xsem).start()

        tile_load(step, me, rx_ref, xb, xsem).wait()
        up(step, w1, w3, xb, hh, res, top, ob)
        down(step, me, w2, hh, res, top, so)
        return 0

    lax.fori_loop(0, EARLY, tile, 0)

    arrived(last)
    for copy in list(hops.values()) + told + [copy for each in sends.values() for copy in each[1:]]:
        copy.wait_send()
    for copy in told:
        copy.wait_recv()


def experts_part(t, cap, groups, x_ref, rx_ref, y_ref, r2, w1, w3, w2, info, upper, ready, ysem, xsem, sems,
                 xb, hh, res, top, ob, so, yv, rest, r1, s1, s2, acc, part, planes, db, wt, xv):
    p1s, p1r, q1s, q1r, p2s, p2r, q2s, q2r, p3s, p3r, hs, hr, e1s, e1r, e2s, e2r, dsem = sems
    ey, ex, dp = lax.axis_index("ey"), lax.axis_index("ex"), lax.axis_index("dp")
    me = [ey // RING, ey % RING, ex // CORES]
    core = ex % CORES
    rows = LINE * cap
    hd, ff = w1.shape
    everyone = range(len(groups))
    col0 = [start for start, _ in groups]
    width = [w for _, w in groups]
    main = min(width)
    more = width[0] - main
    own = [me[RETURNS[g][0]] * CORES + core for g in everyone]

    def shifted(axis, by, c=None):
        coords = list(me)
        coords[axis] = (coords[axis] + by) % RING
        return (dp, coords[0] * RING + coords[1], coords[2] * CORES + (core if c is None else c))

    def remote(src, dst, send, recv, to):
        return pltpu.make_async_remote_copy(src_ref=src, dst_ref=dst, send_sem=send, recv_sem=recv,
                                            device_id=to, device_id_type=MESH)

    for axis, by, dc in PEERS:
        pl.semaphore_signal(ready, inc=1, device_id=shifted(axis, by, (core + dc) % CORES), device_id_type=MESH)
    tile_load(EARLY, me, rx_ref, xb, xsem).start()
    xload = pltpu.make_async_copy(x_ref, xv, ysem.at[len(groups)])
    xload.start()

    def first(step):
        dz, dy = homes(step)
        zh, yh = (me[0] + dz) % RING, (me[1] + dy) % RING
        slot = step % SLOTS
        found = []
        for n in range(1, LINE):
            d, dc = n // CORES, n % CORES
            c = (core + dc) % CORES
            found.append((None, remote(
                ob.at[slot, (me[2] + d) % RING, c, :, pl.ds(col0[0], main)],
                r1.at[0, own[0], zh, yh, :, pl.ds(0, main)],
                p1s.at[slot, n], p1r.at[0, n], shifted(2, d, c))))
        for g, axis, d, lead in ((1, 1, dy, zh), (2, 0, dz, yh)):
            for dc in range(CORES):
                c = (core + dc) % CORES
                found.append((None if dc else d != 0, remote(
                    ob.at[slot, :, c, :, pl.ds(col0[g], width[g])],
                    r1.at[g, own[g], lead, :, :, pl.ds(0, width[g])],
                    p1s.at[slot, LINE + 2 * (g - 1) + dc], p1r.at[g, d * CORES + dc], shifted(axis, d, c))))
        return found

    def each(found, act):
        for whether, copy in found:
            if whether is None:
                act(copy)
            else:
                @pl.when(whether)
                def _():
                    act(copy)

    eye = diagonal(cap)

    def room(step):
        @pl.when(step >= SLOTS)
        def _():
            each(first(step - SLOTS), lambda copy: copy.wait_send())

    def leave(step):
        each(first(step), lambda copy: copy.start())
        dz, dy = homes(step)
        zh, yh = (me[0] + dz) % RING, (me[1] + dy) % RING
        slot = step % SLOTS
        r1[0, own[0], zh, yh, :, pl.ds(0, width[0])] = ob[slot, me[2], core, :, pl.ds(col0[0], width[0])]
        if more:
            rest[zh, yh] = ob[slot, :, :, :, pl.ds(col0[0] + main, more)]
        for g, d, lead in ((1, dy, zh), (2, dz, yh)):
            @pl.when(d == 0)
            def _():
                for xh in range(RING):
                    r1[g, own[g], lead, xh, :, pl.ds(0, width[g])] = ob[slot, xh, core, :, pl.ds(col0[g], width[g])]

    def tile(step, _):
        @pl.when(step + 1 < RING * RING)
        def _():
            tile_load(step + 1, me, rx_ref, xb, xsem).start()

        room(step - 1)
        tile_load(step, me, rx_ref, xb, xsem).wait()
        up(step, w1, w3, xb, hh, res, top, ob)
        leave(step - 1)
        down(step, me, w2, hh, res, top, so)
        return 0

    steps = RING * RING
    pl.semaphore_wait(ready, len(PEERS))

    def leave_early(step, _):
        leave(step)
        return 0

    lax.fori_loop(0, EARLY - 1, leave_early, 0)
    lax.fori_loop(EARLY, steps, tile, 0)
    room(steps - 1)
    code(steps - 1, 0, hd // 128, res, top, ob)
    leave(steps - 1)

    def scales(g, coord, c):
        return (so.at[:, :, coord, c], so.at[:, coord, :, c], so.at[coord, :, :, c])[g]

    hints = []
    for g in everyone:
        axis = RETURNS[g][0]
        s1[g, own[g]] = (so[:, :, me[2], core], so[:, me[1], :, core], so[me[0], :, :, core])[g]
        for n in range(1, LINE):
            d, dc = n // CORES, n % CORES
            c = (core + dc) % CORES
            hints.append(remote(scales(g, (me[axis] + d) % RING, c), s1.at[g, own[g]],
                                q1s.at[g, n], q1r.at[g, n], shifted(axis, d, c)))
            hints[-1].start()

    later = []
    if more:
        for n in range(1, LINE):
            d, dc = n // CORES, n % CORES
            c = (core + dc) % CORES
            later.append(remote(rest.at[:, :, (me[2] + d) % RING, c], r1.at[0, own[0], :, :, :, pl.ds(main, more)],
                                e1s.at[n], e1r.at[n], shifted(2, d, c)))
            later[-1].start()

    def lane(ref, g, h2, h3):
        return (ref.at[0, :, h3, h2], ref.at[1, :, h2, h3], ref.at[2, :, h3, h2])[g]

    def second(g, k3, d):
        _, axis, third = RETURNS[g]
        h3 = (me[third] + k3) % RING
        at = pl.ds(0, main)
        src = (r1.at[0, :, h3, (me[axis] + d) % RING, :, at] if g == 0 else
               r1.at[1, :, (me[axis] + d) % RING, h3, :, at] if g == 1 else
               r1.at[2, :, h3, (me[axis] + d) % RING, :, at])
        return remote(src, r2.at[g, h3, me[axis], :, :, at], p2s.at[g, k3, d], p2r.at[g, k3, d], shifted(axis, d))

    def second_more(k3, d):
        _, axis, third = RETURNS[0]
        h3 = (me[third] + k3) % RING
        at = pl.ds(main, more)
        return remote(r1.at[0, :, h3, (me[axis] + d) % RING, :, at], r2.at[0, h3, me[axis], :, :, at],
                      e2s.at[k3, d], e2r.at[k3, d], shifted(axis, d))

    for g in (1, 2, 0):
        axis = RETURNS[g][0]
        for n in range(1, LINE):
            d, dc = n // CORES, n % CORES
            src = (me[axis] - d) % RING * CORES + (core + dc) % CORES
            ref = r1.at[g, src, :, :, :, pl.ds(0, main)]
            pltpu.make_async_copy(ref, ref, p1r.at[g, n]).wait()
        for d in (1, 3, 2):
            second(g, LINES[0], d).start()

    for copy in hints:
        copy.wait_recv()
    moved = []
    for g in everyone:
        axis = RETURNS[g][1]
        s2[g, me[axis]] = (s1[0, :, :, me[1]], s1[1, :, me[0]], s1[2, :, :, me[2]])[g]
        for d in (1, 3, 2):
            moved.append(remote(lane(s1, g, (me[axis] + d) % RING, slice(None)), s2.at[g, me[axis]],
                                q2s.at[g, d], q2r.at[g, d], shifted(axis, d)))
            moved[-1].start()

    for copy in later:
        copy.wait_recv()
    def rest_of(k3):
        for d in (1, 3, 2):
            if more:
                second_more(k3, d).start()
            for g in everyone:
                if k3 != LINES[0]:
                    second(g, k3, d).start()

    for k3 in LINES[:-1]:
        rest_of(k3)

    for copy in moved:
        copy.wait_recv()

    wanted = lax.broadcasted_iota(jnp.int32, (cap, t), 0).astype(f32)

    def weights(g, h3, src):
        first_axis, axis, third = RETURNS[g]
        base = src * STRIDES[axis] + me[third] * STRIDES[third]
        found = {}

        def begin():
            ids = info[third, h3, 0:8, :]
            gates = info[third, h3, 8:16, :]
            hits, gate = [], []
            for k in range(LINE):
                same = ids == (base + (k // CORES) * STRIDES[first_axis] + k % CORES).astype(f32)
                hits.append(jnp.sum(jnp.where(same, 1.0, 0.0), axis=0, keepdims=True))
                gate.append(jnp.sum(jnp.where(same, gates, 0.0), axis=0, keepdims=True))
            hit = jnp.concatenate(hits, axis=0)
            rank = jnp.dot(hit.astype(bf16), upper[...], preferred_element_type=f32)
            found["slot"] = jnp.where((hit > 0.5) & (rank < cap + 0.5), rank - 1.0, -1.0)
            found["gate"] = gate

        def expert(k):
            scale = jnp.sum(jnp.where(eye, s2[g, src, k, h3], 0.0), axis=1, keepdims=True)
            w = jnp.where(found["slot"][k:k + 1, :] == wanted, found["gate"][k], 0.0) * scale
            for p in range(3):
                a = w.astype(bf16)
                wt[g, pl.ds(p * rows + k * cap, cap), :] = a
                w = w - a.astype(f32)

        return [begin] + [functools.partial(expert, k) for k in range(LINE)]

    def line(index, _):
        k3 = 2 - index + 3 * (index // 2) - 2 * (index // 3)

        def plane(turn, _):
            d = turn + turn // 2 - 2 * (turn // 3)

            def fetch(g):
                third = RETURNS[g][2]
                src = (me[RETURNS[g][1]] - d) % RING
                return pltpu.make_async_copy(r2.at[g, (me[third] + k3) % RING, src, :, :, pl.ds(0, width[g])],
                                             db.at[g, :, :, pl.ds(0, width[g])], dsem.at[g])

            for g in everyone:
                _, axis, third = RETURNS[g]
                h3 = (me[third] + k3) % RING

                @pl.when(turn == 0)
                def _():
                    at = pl.ds(0, width[g])
                    if g == 1:
                        db[g, :, :, at] = r1[g, :, me[axis], h3, :, at]
                    else:
                        db[g, :, :, at] = r1[g, :, h3, me[axis], :, at]
                    acc[g, index] = jnp.zeros(acc.shape[2:], f32)

                @pl.when(turn > 0)
                def _():
                    second(g, k3, d).wait_recv()
                    if more and g == 0:
                        second_more(k3, d).wait_recv()
                    fetch(g).start()

            @pl.when(turn > 0)
            def _():
                for g in everyone:
                    fetch(g).wait()

            def piece(g, begin, size):
                at = pl.ds(begin, size)
                q = db[g, :, :, at].reshape(rows, size).astype(f32)
                high = q.astype(bf16)
                low = (q - high.astype(f32)).astype(bf16)
                dims = (((0,), (0,)), ((), ()))
                p = (lax.dot_general(wt[g], jnp.concatenate([high] * 3, axis=0), dims, preferred_element_type=f32)
                     + lax.dot_general(wt[g], jnp.concatenate([low] * 3, axis=0), dims, preferred_element_type=f32))
                acc[g, index, :, at] += p

            def steps_of(g):
                _, axis, third = RETURNS[g]
                return weights(g, (me[third] + k3) % RING, (me[axis] - d) % RING)

            for act in steps_of(0):
                act()
            for g in everyone:
                products = [functools.partial(piece, g, begin, min(PIECE, width[g] - begin))
                            for begin in range(0, width[g], PIECE)]
                others = steps_of(g + 1) if g + 1 < len(groups) else []
                for k, act in enumerate(products):
                    act()
                    for other in others[len(others) * k // len(products):len(others) * (k + 1) // len(products)]:
                        other()

            for g in everyone:
                @pl.when((turn == RING - 1) & (index == 0))
                def _():
                    for way in range(2):
                        opposite(g, way).start()

                @pl.when((turn == RING - 1) & (index == 2))
                def _():
                    for way in range(2):
                        opposite(g, way).wait_recv()
                        rows_of = pl.ds(way * (t // 2), t // 2)
                        at = pl.ds(0, width[g])
                        acc[g, 1 + way, rows_of, at] += part[g, way, :, at]
                    for way in range(2):
                        home(g, way).start()
            return 0

        lax.fori_loop(0, RING, plane, 0)

        @pl.when(index == 0)
        def _():
            rest_of(LINES[-1])
        return 0

    def opposite(g, way):
        at = pl.ds(0, width[g])
        return remote(acc.at[g, 0, pl.ds(way * (t // 2), t // 2), at], part.at[g, way, :, at],
                      hs.at[g, way], hr.at[g, way], shifted(RETURNS[g][2], LINES[1 + way]))

    def home(g, way):
        at = pl.ds(0, width[g])
        return remote(acc.at[g, 1 + way, :, at], planes.at[g, way, :, at],
                      p3s.at[g, way], p3r.at[g, way], shifted(RETURNS[g][2], LINES[1 + way]))

    lax.fori_loop(0, RING, line, 0)

    for copy in hints + moved + later:
        copy.wait_send()

    def last(step, _):
        each(first(step), lambda copy: copy.wait_send())
        return 0

    lax.fori_loop(RING * RING - SLOTS, RING * RING, last, 0)
    for g in everyone:
        for k3 in range(RING):
            for d in (1, 3, 2):
                second(g, k3, d).wait_send()
                if more and g == 0:
                    second_more(k3, d).wait_send()
        for way in range(2):
            opposite(g, way).wait_send()

    xload.wait()
    stores = []
    for g in reversed(everyone):
        for way in range(2):
            home(g, way).wait_recv()

        def finish(n, _):
            at = pl.ds(pl.multiple_of(n * 128, 128), 128)
            to = pl.ds(pl.multiple_of(col0[g] + n * 128, 128), 128)
            total = acc[g, RING - 1, :, at] + planes[g, 0, :, at] + planes[g, 1, :, at]
            yv[:, to] = (xv[:, to].astype(f32) + total).astype(bf16)
            return 0

        lax.fori_loop(0, width[g] // 128, finish, 0)
        at = pl.ds(col0[g], width[g])
        stores.append(pltpu.make_async_copy(yv.at[:, at], y_ref.at[:, at], ysem.at[g]))
        stores[-1].start()

    for g in everyone:
        for way in range(2):
            home(g, way).wait_send()
    for store in stores:
        store.wait()


def layer_kernel(t, cap, groups, ids_ref, gates_ref, x_ref, w1_ref, w3_ref, w2_ref, y_ref, rx_ref, r2,
                 w1, w3, w2, idv, gatev, info, upper, xb, hh, res, top, ob, so, yv, ready, small_sem, wsem, load_sem,
                 gsend, grecv, rsend, rrecv, self_sem, isend, irecv, ysem, xsem, *sems):
    hd = w1.shape[0]
    n = len(groups)
    wide = max(w for _, w in groups)
    more = max(wide - min(w for _, w in groups), 128)
    small = [pltpu.make_async_copy(a, b, small_sem.at[k]) for k, (a, b) in enumerate(((ids_ref, idv), (gates_ref, gatev)))]
    weight_loads = [pltpu.make_async_copy(a, b, wsem.at[k])
                    for k, (a, b) in enumerate(((w1_ref, w1), (w3_ref, w3), (w2_ref, w2)))]

    def there(got, out, pick):
        dispatch_part(t, cap, groups, x_ref, rx_ref, small, idv, gatev, upper, info, load_sem, gsend, grecv, rsend, rrecv, self_sem,
                      isend, irecv, weight_loads, xsem, w1, w3, w2, xb, hh, res, top, ob, so, got, out, pick)

    pl.run_scoped(there,
                  pltpu.VMEM((n, RING, RING, t + IDROWS, wide), bf16),
                  pltpu.VMEM((n, RING, LINE, RING, cap, wide), bf16),
                  pltpu.VMEM((LINE * cap, t), bf16))

    def back(*scratch):
        experts_part(t, cap, groups, x_ref, rx_ref, y_ref, r2, w1, w3, w2, info, upper, ready, ysem, xsem, sems,
                     xb, hh, res, top, ob, so, yv, *scratch)

    pl.run_scoped(back,
                  pltpu.VMEM((RING, RING, RING, CORES, cap, more), i16),
                  pltpu.VMEM((n, LINE, RING, RING, cap, wide), i16),
                  pltpu.VMEM((n, LINE, RING, RING, 1, 128), f32),
                  pltpu.VMEM((n, RING, LINE, RING, 1, 128), f32),
                  pltpu.VMEM((n, RING, t, wide), f32),
                  pltpu.VMEM((n, 2, t // 2, wide), f32),
                  pltpu.VMEM((n, 2, t, wide), f32),
                  pltpu.VMEM((n, LINE, cap, wide), i16),
                  pltpu.VMEM((n, 3 * LINE * cap, t), bf16),
                  pltpu.VMEM((t, hd), bf16))


def layer(x, ids, gates, w1, w3, w2, cap):
    t, hd = x.shape
    ff = w1.shape[1]
    groups = column_groups(hd, 128)
    wide = max(w for _, w in groups)
    n = len(groups)
    dma = pltpu.SemaphoreType.DMA
    anywhere = pl.BlockSpec(memory_space=pl.ANY)
    y, _, _ = pl.pallas_call(
        functools.partial(layer_kernel, t, cap, groups),
        out_shape=(jax.ShapeDtypeStruct((t, hd), bf16),
                   jax.ShapeDtypeStruct((RING, RING, RING, CORES, cap, hd), bf16),
                   jax.ShapeDtypeStruct((n, RING, RING, LINE, cap, wide), i16)),
        in_specs=[anywhere] * 6,
        out_specs=(anywhere,) * 3,
        scratch_shapes=[
            pltpu.VMEM((hd, ff), bf16), pltpu.VMEM((hd, ff), bf16), pltpu.VMEM((ff, hd), bf16),
            pltpu.VMEM((IDROWS, t), jnp.int32), pltpu.VMEM((IDROWS, t), f32),
            pltpu.VMEM((3, RING, 2 * IDROWS, t), f32),
            pltpu.VMEM((t, t), bf16),
            pltpu.VMEM((2, RING, CORES, cap, hd), bf16),
            pltpu.VMEM((LINE * cap, ff), bf16),
            pltpu.VMEM((LINE * cap, hd), f32),
            pltpu.VMEM((LINE * cap, 128), f32),
            pltpu.VMEM((SLOTS, RING, CORES, cap, hd), i16),
            pltpu.VMEM((RING, RING, RING, CORES, 1, 128), f32),
            pltpu.VMEM((t, hd), bf16),
            pltpu.SemaphoreType.REGULAR,
            dma((2,)), dma((3,)), dma((n,)),
            dma((n, 4 + 4 * RING)), dma((n, 4 + 4 * RING)), dma((n, RING, LINE)), dma((n, RING, LINE)), dma((n, RING)),
            dma((3, RING)), dma((3, RING)), dma((n + 1,)), dma((2,)),
            dma((SLOTS, LINE + 4)), dma((n, LINE)), dma((n, LINE)), dma((n, LINE)),
            dma((n, RING, RING)), dma((n, RING, RING)), dma((n, RING)), dma((n, RING)),
            dma((n, 2)), dma((n, 2)), dma((n, 2)), dma((n, 2)), dma((LINE,)), dma((LINE,)),
            dma((RING, RING)), dma((RING, RING)), dma((n,)),
        ],
        compiler_params=pltpu.CompilerParams(collective_id=0, has_side_effects=True, vmem_limit_bytes=67043328),
        name="layer",
    )(ids.T, gates.T, x, w1, w3, w2)
    return y


def solution(mesh):
    nd = mesh.shape["ey"] * mesh.shape["ex"]
    tok = P(("dp", "ey", "ex"), None)
    wsp = P(("ey", "ex"), None, None)

    def local(x, ids, gates, w1, w3, w2):
        t = x.shape[0]
        cap = min(t, CAPF * t * ids.shape[1] // nd)
        return layer(x, ids, gates, w1[0], w3[0], w2[0], cap)

    return jax.shard_map(local, mesh=mesh, in_specs=(tok, tok, tok, wsp, wsp, wsp),
                         out_specs=tok, check_vma=False)
```

```python
import functools

import jax
import jax.numpy as jnp
from jax import lax
from jax.experimental import pallas as pl
from jax.experimental.pallas import tpu as pltpu
from jax.sharding import PartitionSpec as P

CAPF = 2
FULL = 32000.0
RING = 4
CORES = 2
IDROWS = 8
ORDERS = ((0, 1, 2), (2, 0, 1), (1, 2, 0))
LINE = RING * CORES
STRIDES = (RING * RING * CORES, RING * CORES, CORES)
RETURNS = ((2, 1, 0), (1, 0, 2), (0, 2, 1))
TILE = 256
LINES = (2, 1, 3, 0)
WIDE = 512
PIECE = 256
SLOTS = 5
MESH = pl.DeviceIdType.MESH
PEERS = [(axis, by, dc) for axis in range(3) for by in range(1, RING) for dc in range(CORES)] + [(0, 0, 1)]
bf16, i16, f32 = jnp.bfloat16, jnp.int16, jnp.float32


def column_groups(hd, tile):
    tiles = hd // tile
    first = -(-tiles // 3)
    second = -(-(tiles - first) // 2)
    widths = [first * tile, second * tile, (tiles - first - second) * tile]
    starts = [0, widths[0], widths[0] + widths[1]]
    return list(zip(starts, widths))


EARLY = 2


def homes(step):
    turn, k = step // RING, step % RING
    dy = (1 + 2 * k - 3 * (k // 2)) % RING
    return (dy + 2 - turn + 3 * (turn // 2) - 2 * (turn // 3)) % RING, dy


def tile_load(step, me, rx_ref, xb, xsem):
    dz, dy = homes(step)
    return pltpu.make_async_copy(rx_ref.at[(me[0] + dz) % RING, (me[1] + dy) % RING], xb.at[step % 2], xsem.at[step % 2])


def diagonal(cap):
    return lax.broadcasted_iota(jnp.int32, (cap, 128), 0) == lax.broadcasted_iota(jnp.int32, (cap, 128), 1)


def code(step, begin, end, res, top, ob):
    slot = step % SLOTS
    cap = ob.shape[3]
    for n in range(begin, end):
        at = pl.ds(n * 128, 128)
        v = jnp.round(res[:, at] * top[...]).astype(jnp.int32).astype(i16)
        ob[slot, :, :, :, at] = v.reshape(RING, CORES, cap, 128)


def up(step, w1, w3, xb, hh, res, top, ob):
    hd, ff = w1.shape
    rows = hh.shape[0]
    ups, codes = ff // TILE, hd // 128
    for n in range(ups):
        at = pl.ds(n * TILE, TILE)
        xt = xb[step % 2].reshape(rows, hd)
        a1 = jnp.dot(xt, w1[:, at], preferred_element_type=f32)
        a3 = jnp.dot(xt, w3[:, at], preferred_element_type=f32)
        hh[:, at] = (a1 * (1.0 / (1.0 + jnp.exp(-a1))) * a3).astype(bf16)
        code(step - 1, codes * n // ups, codes * (n + 1) // ups, res, top, ob)


def down(step, me, w2, hh, res, top, so):
    ff, hd = w2.shape
    rows = hh.shape[0]
    cap = rows // LINE
    dz, dy = homes(step)
    zh, yh = (me[0] + dz) % RING, (me[1] + dy) % RING
    most = jnp.zeros((rows, 128), f32)
    for n in range(hd // WIDE):
        o = jnp.dot(hh[...], w2[:, n * WIDE:(n + 1) * WIDE], preferred_element_type=f32)
        res[:, n * WIDE:(n + 1) * WIDE] = o
        o = jnp.abs(o)
        for k in range(WIDE // 128):
            most = jnp.maximum(most, o[:, k * 128:(k + 1) * 128])
    peak = jnp.maximum(jnp.max(most, axis=1, keepdims=True), 1e-30)
    top[...] = jnp.broadcast_to(FULL / peak, top.shape)
    for k in range(LINE):
        part = jnp.where(diagonal(cap), peak[k * cap:(k + 1) * cap], 0.0)
        so[zh, yh, k // CORES, k % CORES] = jnp.sum(part, axis=0, keepdims=True) * (1.0 / FULL)


def dispatch_part(t, cap, groups, x_ref, rx_ref, small, idv, gatev, upper, info, load_sem, gsend, grecv, rsend, rrecv, self_sem,
                  isend, irecv, weight_loads, xsem, w1, w3, w2, xb, hh, res, top, ob, so, got, out, pick):
    ey, ex, dp = lax.axis_index("ey"), lax.axis_index("ex"), lax.axis_index("dp")
    me = [ey // RING, ey % RING, ex // CORES]
    core = ex % CORES
    rows = t + IDROWS
    split = (rows // 2 + 7) // 8 * 8

    def device(coords, c):
        return (dp, coords[0] * RING + coords[1], coords[2] * CORES + c)

    def shifted(axis, by, c=None):
        coords = list(me)
        coords[axis] = (coords[axis] + by) % RING
        return device(coords, core if c is None else c)

    loads = [pltpu.make_async_copy(x_ref.at[:, pl.ds(start, width)], got.at[g, 0, 0, pl.ds(0, t), pl.ds(0, width)],
                                   load_sem.at[g]) for g, (start, width) in enumerate(groups)]

    barrier = pltpu.get_barrier_semaphore()
    for axis, by, dc in PEERS:
        pl.semaphore_signal(barrier, inc=1, device_id=shifted(axis, by, (core + dc) % CORES), device_id_type=MESH)
    for load in small + loads:
        load.start()
    row = lax.broadcasted_iota(jnp.int32, (t, t), 0)
    col = lax.broadcasted_iota(jnp.int32, (t, t), 1)
    upper[...] = jnp.where(row <= col, 1.0, 0.0).astype(bf16)
    for load in small:
        load.wait()
    ids = idv[...].astype(f32)
    for g in range(len(groups)):
        got[g, 0, 0, pl.ds(t, IDROWS), pl.ds(0, t)] = ids.astype(bf16)
    for axis in range(3):
        info[axis, me[axis], 0:8, :] = ids
        info[axis, me[axis], 8:16, :] = gatev[...]
    pl.semaphore_wait(barrier, len(PEERS))
    for load in loads:
        load.wait()

    def hop(g, index, block, to, axis, by, part=None):
        width = groups[g][1]
        at = pl.ds(0, rows) if part is None else part
        copy = pltpu.make_async_remote_copy(
            src_ref=got.at[g, block[0], block[1], at, pl.ds(0, width)],
            dst_ref=got.at[g, to[0], to[1], at, pl.ds(0, width)],
            send_sem=gsend.at[g, index], recv_sem=grecv.at[g, index],
            device_id=shifted(axis, by), device_id_type=MESH)
        copy.start()
        hops[g, index] = copy

    hops = {}
    low, high = pl.ds(0, split), pl.ds(split, rows - split)

    def first(g):
        p = ORDERS[g][0]
        hop(g, 0, (0, 0), (3, 0), p, 1)
        hop(g, 1, (0, 0), (1, 0), p, 3)

    def second(g, i):
        q = ORDERS[g][1]
        hop(g, 4 + 4 * i, (i, 0), (i, 3), q, 1)
        hop(g, 5 + 4 * i, (i, 0), (i, 1), q, 3)

    def second_on(g, i):
        q = ORDERS[g][1]
        hops[g, 4 + 4 * i].wait_recv()
        hop(g, 6 + 4 * i, (i, 3), (i, 2), q, 1, low)
        hops[g, 5 + 4 * i].wait_recv()
        hop(g, 7 + 4 * i, (i, 1), (i, 2), q, 3, high)

    everyone = range(len(groups))
    for g in everyone:
        first(g)
        second(g, 0)
    for g in everyone:
        p = ORDERS[g][0]
        hops[g, 0].wait_recv()
        hop(g, 2, (3, 0), (2, 0), p, 1, low)
        second(g, 3)
        hops[g, 1].wait_recv()
        hop(g, 3, (1, 0), (2, 0), p, 3, high)
        second(g, 1)
    for g in everyone:
        second_on(g, 0)
    for g in everyone:
        hops[g, 2].wait_recv()
        hops[g, 3].wait_recv()
        second(g, 2)

    def choose(g, j):
        p, _, r = ORDERS[g]
        width = groups[g][1]
        stride = (RING * RING * CORES, RING * CORES, CORES)[r]
        base = ey * (RING * CORES) + ex - core - me[r] * stride

        def one(i, _):
            ids = got[g, i, j, pl.ds(t, IDROWS), pl.ds(0, t)].astype(f32)
            lines = []
            for k in range(RING * CORES):
                expert = (base + (k // CORES) * stride + k % CORES).astype(f32)
                lines.append(jnp.sum(jnp.where(ids == expert, 1.0, 0.0), axis=0, keepdims=True))
            hit = jnp.concatenate(lines, axis=0)
            rank = jnp.dot(hit.astype(bf16), upper[...], preferred_element_type=f32)
            slot = jnp.where((hit > 0.5) & (rank < cap + 0.5), rank - 1.0, -1.0)
            wanted = lax.broadcasted_iota(jnp.int32, (cap, t), 0).astype(f32)
            for k in range(RING * CORES):
                pick[pl.ds(k * cap, cap), :] = jnp.where(slot[k:k + 1, :] == wanted, 1.0, 0.0).astype(bf16)
            place = (me[p] + i) % RING

            def tile(n, _):
                at = pl.ds(pl.multiple_of(n * 128, 128), 128)
                val = jnp.dot(pick[...], got[g, i, j, pl.ds(0, t), at], preferred_element_type=f32).astype(bf16)
                for k in range(RING * CORES):
                    out[g, j, k, place, :, at] = val[k * cap:(k + 1) * cap]
                return 0

            return lax.fori_loop(0, width // 128, tile, 0)

        lax.fori_loop(0, RING, one, 0)

    def place_in(ref, g, j):
        start, width = groups[g]
        p, q, r = ORDERS[g]
        at = [None, None, None]
        at[p] = slice(None)
        at[q] = (me[q] + j) % RING
        at[r] = me[r]
        return ref.at[at[0], at[1], at[2], core, :, pl.ds(start, width)]

    sends = {}

    def exchange(g, j):
        _, _, r = ORDERS[g]
        width = groups[g][1]
        for dr in range(RING):
            for dc in range(CORES):
                to, c = (me[r] + dr) % RING, (core + dc) % CORES
                src = out.at[g, j, to * CORES + c, :, :, pl.ds(0, width)]
                if dr == 0 and dc == 0:
                    copy = pltpu.make_async_copy(src, place_in(rx_ref, g, j), self_sem.at[g, j])
                else:
                    n = dr * CORES + dc
                    copy = pltpu.make_async_remote_copy(
                        src_ref=src, dst_ref=place_in(rx_ref, g, j),
                        send_sem=rsend.at[g, j, n], recv_sem=rrecv.at[g, j, n],
                        device_id=shifted(r, dr, c), device_id_type=MESH)
                sends.setdefault((g, j), []).append(copy)
                copy.start()

    for g in everyone:
        choose(g, 0)
        exchange(g, 0)
    for load in weight_loads:
        load.start()
    told = []
    for axis in range(3):
        for by in range(1, RING):
            told.append(pltpu.make_async_remote_copy(
                src_ref=info.at[axis, me[axis]], dst_ref=info.at[axis, me[axis]], send_sem=isend.at[axis, by],
                recv_sem=irecv.at[axis, by], device_id=shifted(axis, by), device_id_type=MESH))
            told[-1].start()
    for i in (3, 1):
        for g in everyone:
            second_on(g, i)
    for g in everyone:
        second_on(g, 2)
    for j in (3, 1):
        for g in everyone:
            choose(g, j)
            exchange(g, j)
    for g in (2, 0, 1):
        for i in range(RING):
            hops[g, 6 + 4 * i].wait_recv()
            hops[g, 7 + 4 * i].wait_recv()
        choose(g, 2)
        exchange(g, 2)

    def arrived(which):
        for each in which:
            for copy in sends[each][1:]:
                copy.wait_recv()
            sends[each][0].wait()

    last = [(0, 2), (1, 2)]
    for copy in list(hops.values()) + told:
        copy.wait_send()
    for copy in told:
        copy.wait_recv()
    arrived([each for each in sends if each not in last])
    for load in weight_loads:
        load.wait()
    tile_load(0, me, rx_ref, xb, xsem).start()

    def tile(step, _):
        @pl.when(step + 1 < EARLY)
        def _():
            tile_load(step + 1, me, rx_ref, xb, xsem).start()

        tile_load(step, me, rx_ref, xb, xsem).wait()
        up(step, w1, w3, xb, hh, res, top, ob)
        down(step, me, w2, hh, res, top, so)
        return 0

    lax.fori_loop(0, EARLY, tile, 0)

    def gone(which):
        for each in which:
            for copy in sends[each][1:]:
                copy.wait_send()

    gone([each for each in sends if each[1] != 2])
    arrived(last)
    gone([each for each in sends if each[1] == 2])


def experts_part(t, cap, groups, x_ref, rx_ref, y_ref, r2, w1, w3, w2, info, upper, ready, ysem, xsem, sems,
                 xb, hh, res, top, ob, so, yv, rest, r1, s1, s2, acc, part, planes, db, wt, xv):
    p1s, p1r, q1s, q1r, p2s, p2r, q2s, q2r, p3s, p3r, hs, hr, e1s, e1r, e2s, e2r, dsem = sems
    ey, ex, dp = lax.axis_index("ey"), lax.axis_index("ex"), lax.axis_index("dp")
    me = [ey // RING, ey % RING, ex // CORES]
    core = ex % CORES
    rows = LINE * cap
    hd, ff = w1.shape
    everyone = range(len(groups))
    col0 = [start for start, _ in groups]
    width = [w for _, w in groups]
    main = min(width)
    more = width[0] - main
    own = [me[RETURNS[g][0]] * CORES + core for g in everyone]

    def shifted(axis, by, c=None):
        coords = list(me)
        coords[axis] = (coords[axis] + by) % RING
        return (dp, coords[0] * RING + coords[1], coords[2] * CORES + (core if c is None else c))

    def remote(src, dst, send, recv, to):
        return pltpu.make_async_remote_copy(src_ref=src, dst_ref=dst, send_sem=send, recv_sem=recv,
                                            device_id=to, device_id_type=MESH)

    for axis, by, dc in PEERS:
        pl.semaphore_signal(ready, inc=1, device_id=shifted(axis, by, (core + dc) % CORES), device_id_type=MESH)
    tile_load(EARLY, me, rx_ref, xb, xsem).start()
    xload = pltpu.make_async_copy(x_ref, xv, ysem.at[len(groups)])
    xload.start()

    def first(step):
        dz, dy = homes(step)
        zh, yh = (me[0] + dz) % RING, (me[1] + dy) % RING
        slot = step % SLOTS
        found = []
        for n in range(1, LINE):
            d, dc = n // CORES, n % CORES
            c = (core + dc) % CORES
            found.append((None, remote(
                ob.at[slot, (me[2] + d) % RING, c, :, pl.ds(col0[0], main)],
                r1.at[0, own[0], zh, yh, :, pl.ds(0, main)],
                p1s.at[slot, n], p1r.at[0, n], shifted(2, d, c))))
        for g, axis, d, lead in ((1, 1, dy, zh), (2, 0, dz, yh)):
            for dc in range(CORES):
                c = (core + dc) % CORES
                found.append((None if dc else d != 0, remote(
                    ob.at[slot, :, c, :, pl.ds(col0[g], width[g])],
                    r1.at[g, own[g], lead, :, :, pl.ds(0, width[g])],
                    p1s.at[slot, LINE + 2 * (g - 1) + dc], p1r.at[g, d * CORES + dc], shifted(axis, d, c))))
        return found

    def each(found, act):
        for whether, copy in found:
            if whether is None:
                act(copy)
            else:
                @pl.when(whether)
                def _():
                    act(copy)

    eye = diagonal(cap)

    def room(step):
        @pl.when(step >= SLOTS)
        def _():
            each(first(step - SLOTS), lambda copy: copy.wait_send())

    def leave(step):
        each(first(step), lambda copy: copy.start())
        dz, dy = homes(step)
        zh, yh = (me[0] + dz) % RING, (me[1] + dy) % RING
        slot = step % SLOTS
        r1[0, own[0], zh, yh, :, pl.ds(0, width[0])] = ob[slot, me[2], core, :, pl.ds(col0[0], width[0])]
        if more:
            rest[zh, yh] = ob[slot, :, :, :, pl.ds(col0[0] + main, more)]
        for g, d, lead in ((1, dy, zh), (2, dz, yh)):
            @pl.when(d == 0)
            def _():
                for xh in range(RING):
                    r1[g, own[g], lead, xh, :, pl.ds(0, width[g])] = ob[slot, xh, core, :, pl.ds(col0[g], width[g])]

    def tile(step, _):
        @pl.when(step + 1 < RING * RING)
        def _():
            tile_load(step + 1, me, rx_ref, xb, xsem).start()

        room(step - 1)
        tile_load(step, me, rx_ref, xb, xsem).wait()
        up(step, w1, w3, xb, hh, res, top, ob)
        leave(step - 1)
        down(step, me, w2, hh, res, top, so)
        return 0

    steps = RING * RING
    pl.semaphore_wait(ready, len(PEERS))

    def leave_early(step, _):
        leave(step)
        return 0

    lax.fori_loop(0, EARLY - 1, leave_early, 0)
    lax.fori_loop(EARLY, steps, tile, 0)
    room(steps - 1)
    code(steps - 1, 0, hd // 128, res, top, ob)
    leave(steps - 1)

    def scales(g, coord, c):
        return (so.at[:, :, coord, c], so.at[:, coord, :, c], so.at[coord, :, :, c])[g]

    hints = []
    for g in everyone:
        axis = RETURNS[g][0]
        s1[g, own[g]] = (so[:, :, me[2], core], so[:, me[1], :, core], so[me[0], :, :, core])[g]
        for n in range(1, LINE):
            d, dc = n // CORES, n % CORES
            c = (core + dc) % CORES
            hints.append(remote(scales(g, (me[axis] + d) % RING, c), s1.at[g, own[g]],
                                q1s.at[g, n], q1r.at[g, n], shifted(axis, d, c)))
            hints[-1].start()

    later = []
    if more:
        for n in range(1, LINE):
            d, dc = n // CORES, n % CORES
            c = (core + dc) % CORES
            later.append(remote(rest.at[:, :, (me[2] + d) % RING, c], r1.at[0, own[0], :, :, :, pl.ds(main, more)],
                                e1s.at[n], e1r.at[n], shifted(2, d, c)))
            later[-1].start()

    def lane(ref, g, h2, h3):
        return (ref.at[0, :, h3, h2], ref.at[1, :, h2, h3], ref.at[2, :, h3, h2])[g]

    def second(g, k3, d):
        _, axis, third = RETURNS[g]
        h3 = (me[third] + k3) % RING
        at = pl.ds(0, main)
        src = (r1.at[0, :, h3, (me[axis] + d) % RING, :, at] if g == 0 else
               r1.at[1, :, (me[axis] + d) % RING, h3, :, at] if g == 1 else
               r1.at[2, :, h3, (me[axis] + d) % RING, :, at])
        return remote(src, r2.at[g, h3, me[axis], :, :, at], p2s.at[g, k3, d], p2r.at[g, k3, d], shifted(axis, d))

    def second_more(k3, d):
        _, axis, third = RETURNS[0]
        h3 = (me[third] + k3) % RING
        at = pl.ds(main, more)
        return remote(r1.at[0, :, h3, (me[axis] + d) % RING, :, at], r2.at[0, h3, me[axis], :, :, at],
                      e2s.at[k3, d], e2r.at[k3, d], shifted(axis, d))

    for g in everyone:
        axis = RETURNS[g][0]
        for n in range(1, LINE):
            d, dc = n // CORES, n % CORES
            src = (me[axis] - d) % RING * CORES + (core + dc) % CORES
            ref = r1.at[g, src, :, :, :, pl.ds(0, main)]
            pltpu.make_async_copy(ref, ref, p1r.at[g, n]).wait()
        for d in (1, 3, 2):
            second(g, LINES[0], d).start()

    for copy in hints:
        copy.wait_recv()
    moved = []
    for g in everyone:
        axis = RETURNS[g][1]
        s2[g, me[axis]] = (s1[0, :, :, me[1]], s1[1, :, me[0]], s1[2, :, :, me[2]])[g]
        for d in (1, 3, 2):
            moved.append(remote(lane(s1, g, (me[axis] + d) % RING, slice(None)), s2.at[g, me[axis]],
                                q2s.at[g, d], q2r.at[g, d], shifted(axis, d)))
            moved[-1].start()

    for copy in later:
        copy.wait_recv()
    def rest_of(k3):
        for d in (1, 3, 2):
            if more:
                second_more(k3, d).start()
            for g in everyone:
                if k3 != LINES[0]:
                    second(g, k3, d).start()

    for k3 in LINES[:-1]:
        rest_of(k3)

    for copy in moved:
        copy.wait_recv()

    wanted = lax.broadcasted_iota(jnp.int32, (cap, t), 0).astype(f32)

    def weights(g, h3, src):
        first_axis, axis, third = RETURNS[g]
        base = src * STRIDES[axis] + me[third] * STRIDES[third]
        found = {}

        def begin():
            ids = info[third, h3, 0:8, :]
            gates = info[third, h3, 8:16, :]
            hits, gate = [], []
            for k in range(LINE):
                same = ids == (base + (k // CORES) * STRIDES[first_axis] + k % CORES).astype(f32)
                hits.append(jnp.sum(jnp.where(same, 1.0, 0.0), axis=0, keepdims=True))
                gate.append(jnp.sum(jnp.where(same, gates, 0.0), axis=0, keepdims=True))
            hit = jnp.concatenate(hits, axis=0)
            rank = jnp.dot(hit.astype(bf16), upper[...], preferred_element_type=f32)
            found["slot"] = jnp.where((hit > 0.5) & (rank < cap + 0.5), rank - 1.0, -1.0)
            found["gate"] = gate

        def expert(k):
            scale = jnp.sum(jnp.where(eye, s2[g, src, k, h3], 0.0), axis=1, keepdims=True)
            w = jnp.where(found["slot"][k:k + 1, :] == wanted, found["gate"][k], 0.0) * scale
            for p in range(3):
                a = w.astype(bf16)
                wt[g, pl.ds(p * rows + k * cap, cap), :] = a
                w = w - a.astype(f32)

        return [begin] + [functools.partial(expert, k) for k in range(LINE)]

    def line(index, _):
        k3 = 2 - index + 3 * (index // 2) - 2 * (index // 3)

        def plane(turn, _):
            d = turn + turn // 2 - 2 * (turn // 3)

            def fetch(g):
                third = RETURNS[g][2]
                src = (me[RETURNS[g][1]] - d) % RING
                return pltpu.make_async_copy(r2.at[g, (me[third] + k3) % RING, src, :, :, pl.ds(0, width[g])],
                                             db.at[g, :, :, pl.ds(0, width[g])], dsem.at[g])

            for g in everyone:
                _, axis, third = RETURNS[g]
                h3 = (me[third] + k3) % RING

                @pl.when(turn == 0)
                def _():
                    at = pl.ds(0, width[g])
                    if g == 1:
                        db[g, :, :, at] = r1[g, :, me[axis], h3, :, at]
                    else:
                        db[g, :, :, at] = r1[g, :, h3, me[axis], :, at]
                    acc[g, index] = jnp.zeros(acc.shape[2:], f32)

                @pl.when(turn > 0)
                def _():
                    second(g, k3, d).wait_recv()
                    if more and g == 0:
                        second_more(k3, d).wait_recv()
                    fetch(g).start()

            @pl.when(turn > 0)
            def _():
                for g in everyone:
                    fetch(g).wait()

            def piece(g, begin, size):
                at = pl.ds(begin, size)
                q = db[g, :, :, at].reshape(rows, size).astype(f32)
                high = q.astype(bf16)
                low = (q - high.astype(f32)).astype(bf16)
                dims = (((0,), (0,)), ((), ()))
                p = (lax.dot_general(wt[g], jnp.concatenate([high] * 3, axis=0), dims, preferred_element_type=f32)
                     + lax.dot_general(wt[g], jnp.concatenate([low] * 3, axis=0), dims, preferred_element_type=f32))
                acc[g, index, :, at] += p

            def steps_of(g):
                _, axis, third = RETURNS[g]
                return weights(g, (me[third] + k3) % RING, (me[axis] - d) % RING)

            for act in steps_of(0):
                act()
            for g in everyone:
                products = [functools.partial(piece, g, begin, min(PIECE, width[g] - begin))
                            for begin in range(0, width[g], PIECE)]
                others = steps_of(g + 1) if g + 1 < len(groups) else []
                for k, act in enumerate(products):
                    act()
                    for other in others[len(others) * k // len(products):len(others) * (k + 1) // len(products)]:
                        other()

            for g in everyone:
                @pl.when((turn == RING - 1) & (index == 0))
                def _():
                    for way in range(2):
                        opposite(g, way).start()

                @pl.when((turn == RING - 1) & (index == 2))
                def _():
                    for way in range(2):
                        opposite(g, way).wait_recv()
                        rows_of = pl.ds(way * (t // 2), t // 2)
                        at = pl.ds(0, width[g])
                        acc[g, 1 + way, rows_of, at] += part[g, way, :, at]
                    for way in range(2):
                        home(g, way).start()
            return 0

        lax.fori_loop(0, RING, plane, 0)

        @pl.when(index == 0)
        def _():
            rest_of(LINES[-1])
        return 0

    def opposite(g, way):
        at = pl.ds(0, width[g])
        return remote(acc.at[g, 0, pl.ds(way * (t // 2), t // 2), at], part.at[g, way, :, at],
                      hs.at[g, way], hr.at[g, way], shifted(RETURNS[g][2], LINES[1 + way]))

    def home(g, way):
        at = pl.ds(0, width[g])
        return remote(acc.at[g, 1 + way, :, at], planes.at[g, way, :, at],
                      p3s.at[g, way], p3r.at[g, way], shifted(RETURNS[g][2], LINES[1 + way]))

    lax.fori_loop(0, RING, line, 0)

    for copy in hints + moved + later:
        copy.wait_send()

    def last(step, _):
        each(first(step), lambda copy: copy.wait_send())
        return 0

    lax.fori_loop(RING * RING - SLOTS, RING * RING, last, 0)
    for g in everyone:
        for k3 in range(RING):
            for d in (1, 3, 2):
                second(g, k3, d).wait_send()
                if more and g == 0:
                    second_more(k3, d).wait_send()
        for way in range(2):
            opposite(g, way).wait_send()

    xload.wait()
    stores = []
    for g in reversed(everyone):
        for way in range(2):
            home(g, way).wait_recv()

        def finish(n, _):
            at = pl.ds(pl.multiple_of(n * 128, 128), 128)
            to = pl.ds(pl.multiple_of(col0[g] + n * 128, 128), 128)
            total = acc[g, RING - 1, :, at] + planes[g, 0, :, at] + planes[g, 1, :, at]
            yv[:, to] = (xv[:, to].astype(f32) + total).astype(bf16)
            return 0

        lax.fori_loop(0, width[g] // 128, finish, 0)
        at = pl.ds(col0[g], width[g])
        stores.append(pltpu.make_async_copy(yv.at[:, at], y_ref.at[:, at], ysem.at[g]))
        stores[-1].start()

    for g in everyone:
        for way in range(2):
            home(g, way).wait_send()
    for store in stores:
        store.wait()


def layer_kernel(t, cap, groups, ids_ref, gates_ref, x_ref, w1_ref, w3_ref, w2_ref, y_ref, rx_ref, r2,
                 w1, w3, w2, idv, gatev, info, upper, xb, hh, res, top, ob, so, yv, ready, small_sem, wsem, load_sem,
                 gsend, grecv, rsend, rrecv, self_sem, isend, irecv, ysem, xsem, *sems):
    hd = w1.shape[0]
    n = len(groups)
    wide = max(w for _, w in groups)
    more = max(wide - min(w for _, w in groups), 128)
    small = [pltpu.make_async_copy(a, b, small_sem.at[k]) for k, (a, b) in enumerate(((ids_ref, idv), (gates_ref, gatev)))]
    weight_loads = [pltpu.make_async_copy(a, b, wsem.at[k])
                    for k, (a, b) in enumerate(((w1_ref, w1), (w3_ref, w3), (w2_ref, w2)))]

    def there(got, out, pick):
        dispatch_part(t, cap, groups, x_ref, rx_ref, small, idv, gatev, upper, info, load_sem, gsend, grecv, rsend, rrecv, self_sem,
                      isend, irecv, weight_loads, xsem, w1, w3, w2, xb, hh, res, top, ob, so, got, out, pick)

    pl.run_scoped(there,
                  pltpu.VMEM((n, RING, RING, t + IDROWS, wide), bf16),
                  pltpu.VMEM((n, RING, LINE, RING, cap, wide), bf16),
                  pltpu.VMEM((LINE * cap, t), bf16))

    def back(*scratch):
        experts_part(t, cap, groups, x_ref, rx_ref, y_ref, r2, w1, w3, w2, info, upper, ready, ysem, xsem, sems,
                     xb, hh, res, top, ob, so, yv, *scratch)

    pl.run_scoped(back,
                  pltpu.VMEM((RING, RING, RING, CORES, cap, more), i16),
                  pltpu.VMEM((n, LINE, RING, RING, cap, wide), i16),
                  pltpu.VMEM((n, LINE, RING, RING, 1, 128), f32),
                  pltpu.VMEM((n, RING, LINE, RING, 1, 128), f32),
                  pltpu.VMEM((n, RING, t, wide), f32),
                  pltpu.VMEM((n, 2, t // 2, wide), f32),
                  pltpu.VMEM((n, 2, t, wide), f32),
                  pltpu.VMEM((n, LINE, cap, wide), i16),
                  pltpu.VMEM((n, 3 * LINE * cap, t), bf16),
                  pltpu.VMEM((t, hd), bf16))


def layer(x, ids, gates, w1, w3, w2, cap):
    t, hd = x.shape
    ff = w1.shape[1]
    groups = column_groups(hd, 128)
    wide = max(w for _, w in groups)
    n = len(groups)
    dma = pltpu.SemaphoreType.DMA
    anywhere = pl.BlockSpec(memory_space=pl.ANY)
    y, _, _ = pl.pallas_call(
        functools.partial(layer_kernel, t, cap, groups),
        out_shape=(jax.ShapeDtypeStruct((t, hd), bf16),
                   jax.ShapeDtypeStruct((RING, RING, RING, CORES, cap, hd), bf16),
                   jax.ShapeDtypeStruct((n, RING, RING, LINE, cap, wide), i16)),
        in_specs=[anywhere] * 6,
        out_specs=(anywhere,) * 3,
        scratch_shapes=[
            pltpu.VMEM((hd, ff), bf16), pltpu.VMEM((hd, ff), bf16), pltpu.VMEM((ff, hd), bf16),
            pltpu.VMEM((IDROWS, t), jnp.int32), pltpu.VMEM((IDROWS, t), f32),
            pltpu.VMEM((3, RING, 2 * IDROWS, t), f32),
            pltpu.VMEM((t, t), bf16),
            pltpu.VMEM((2, RING, CORES, cap, hd), bf16),
            pltpu.VMEM((LINE * cap, ff), bf16),
            pltpu.VMEM((LINE * cap, hd), f32),
            pltpu.VMEM((LINE * cap, 128), f32),
            pltpu.VMEM((SLOTS, RING, CORES, cap, hd), i16),
            pltpu.VMEM((RING, RING, RING, CORES, 1, 128), f32),
            pltpu.VMEM((t, hd), bf16),
            pltpu.SemaphoreType.REGULAR,
            dma((2,)), dma((3,)), dma((n,)),
            dma((n, 4 + 4 * RING)), dma((n, 4 + 4 * RING)), dma((n, RING, LINE)), dma((n, RING, LINE)), dma((n, RING)),
            dma((3, RING)), dma((3, RING)), dma((n + 1,)), dma((2,)),
            dma((SLOTS, LINE + 4)), dma((n, LINE)), dma((n, LINE)), dma((n, LINE)),
            dma((n, RING, RING)), dma((n, RING, RING)), dma((n, RING)), dma((n, RING)),
            dma((n, 2)), dma((n, 2)), dma((n, 2)), dma((n, 2)), dma((LINE,)), dma((LINE,)),
            dma((RING, RING)), dma((RING, RING)), dma((n,)),
        ],
        compiler_params=pltpu.CompilerParams(collective_id=0, has_side_effects=True, vmem_limit_bytes=67043328),
        name="layer",
    )(ids.T, gates.T, x, w1, w3, w2)
    return y


def solution(mesh):
    nd = mesh.shape["ey"] * mesh.shape["ex"]
    tok = P(("dp", "ey", "ex"), None)
    wsp = P(("ey", "ex"), None, None)

    def local(x, ids, gates, w1, w3, w2):
        t = x.shape[0]
        cap = min(t, CAPF * t * ids.shape[1] // nd)
        return layer(x, ids, gates, w1[0], w3[0], w2[0], cap)

    return jax.shard_map(local, mesh=mesh, in_specs=(tok, tok, tok, wsp, wsp, wsp),
                         out_specs=tok, check_vma=False)
```
